32 devices in a mesh: dp: 2 (over x), expert: 16 (over z, y, core).
Axes of the slice: x: 2, y: 2, z: 4, core: 2. Of those that a mesh axis runs over, the one named last changes fastest.
Arguments:
- hidden: bfloat16 [2, 1024, 2, 2048], P('dp', 'expert'), may hold values from -6 to 6
- queries: bfloat16 [2, 1024, 2, 4096], P('dp', 'expert'), may hold values from -45 to 45
- latents: bfloat16 [2, 1024, 2, 512], P('dp', 'expert'), may hold values from -165 to 165
- mem_latents: bfloat16 [2, 32, 2, 512], P('dp'), may hold values from -6 to 6
- lengths: int32 [2, 2], P('dp'), may hold values from 512 to 1024
- ids: int32 [2, 1024, 2, 6], P('dp', 'expert'), may hold values from 0 to 15, all different within a row; in each aligned block of 128 rows (0 to 127, 128 to 255, ..., all dimensions but the last counted through in order) at most 50 rows name the same one
- gates: bfloat16 [2, 1024, 2, 6], P('dp', 'expert'), may hold values from 0.049804688 to 0.5
- norm_gain: bfloat16 [2048], replicated, may hold values from 0.25 to 1.75
- w_uv: bfloat16 [8, 512, 128], P('dp'), may hold values from -0.25 to 0.25
- w_out: bfloat16 [1024, 2048], P('dp'), may hold values from -0.1875 to 0.1875
- w_gate: bfloat16 [16, 2048, 704], P('expert'), may hold values from -0.125 to 0.125
- w_up: bfloat16 [16, 2048, 704], P('expert'), may hold values from -0.125 to 0.125
- w_down: bfloat16 [16, 704, 2048], P('expert'), may hold values from -0.21875 to 0.21875
Outputs:
- layer_out: bfloat16 [2, 1024, 2, 2048], P('dp', 'expert')
The draws below stay inside these ranges and needn't reach their ends.
Inputs may be any that keep to these rules, and one draw needn't show every extreme that they name: `ids`: each row names 6 different experts; the rows of one device (aligned blocks of 128 rows in the order of the leading dimensions) name any one expert at most 50 times, a bound that some block reaches.
All inputs are finite; a program needn't handle non-finite values.
Results may differ from the reference program's by a relative error of at most 0.007.
Values may be sent and summed in bfloat16 or wider, within the bound.
A program may use at most 128 MiB of HBM per device.

```python
import math
import jax
import jax.numpy as jnp
import numpy as np
from jax import lax

D = 2048
HEADS = 8
LAT = 512
VDIM = 128
FF = 704
TOPK = 6
MEM = 32
SEQS = 2
SEG = 1024
TOK_DEV = 128
EXPERTS = 16
CAP = 50
N_DP = 2
N_EXPERT = 16


def draw_latents(key, part):
    entries = jnp.clip(jax.random.normal(jax.random.fold_in(key, 1), (N_DP, SEG, SEQS, LAT), jnp.float32), -6.0, 6.0)
    return entries.astype(jnp.bfloat16)


def draw_queries(key, part):
    full_shape = (N_DP, SEG, SEQS, HEADS, LAT)
    entries = 0.5 * jnp.clip(jax.random.normal(jax.random.fold_in(key, 3), full_shape, jnp.float32), -6.0, 6.0)
    return entries.reshape(N_DP, SEG, SEQS, HEADS * LAT).astype(jnp.bfloat16)


def set_ends(drawn, rng, low, largest):
    spot = [jax.random.randint(jax.random.fold_in(rng, axis), (), 0, length) for axis, length in enumerate(drawn.shape)]
    longest = drawn.shape.index(max(drawn.shape))
    neighbour = spot[:longest] + [(spot[longest] + 1) % drawn.shape[longest]] + spot[longest + 1:]
    return drawn.at[tuple(spot)].set(low).at[tuple(neighbour)].set(largest)


def steps_of(key, extent, shards, least, high):
    level, own = 1.0, jax.random.fold_in(key, 6)
    for dim, parts in shards:
        heights = jnp.exp(jax.random.uniform(jax.random.fold_in(own, dim), (parts,), jnp.float32, least / len(shards), high / len(shards)))
        level = level * jnp.repeat(heights, extent[dim] // parts).reshape([-1 if axis == dim else 1 for axis in range(len(extent))])
    return level


def routed_block(own_key, own, number, rows, number_of, top, most, slope):
    ranking = jax.random.permutation(own_key, number_of)
    crowded, ordinary = portions_of(number_of, rows * top, most, slope, True), portions_of(number_of, rows * top, most, slope, False)
    places = jnp.arange(number_of)

    def named(sizes, offset_by):
        used = int((sizes > 0).sum())
        fixed = max(1, used // 4)
        moved = fixed + (places - fixed + offset_by * (used - fixed)) % max(1, number_of - fixed)
        return jnp.zeros((number_of,), jnp.int32).at[ranking[jnp.where(places < fixed, places, moved)]].set(jnp.asarray(sizes, jnp.int32))

    sizes = jnp.where(number % 4 == 0, named(crowded, number // 4), named(ordinary, number - number // 4 - 1))
    mixed = jax.random.permutation(jax.random.fold_in(own, 3), number_of)
    giver, sink = mixed[0:number_of // 2 * 2:2], mixed[1:number_of // 2 * 2:2]
    margin = jnp.minimum(sizes[giver] - 1, most - sizes[sink]) // 2
    margin = jnp.where((giver == ranking[0]) | (sink == ranking[0]) | (sizes[sink] == 0), 0, jnp.maximum(margin, 0))
    moved = jax.random.randint(jax.random.fold_in(own, 4), (number_of // 2,), 0, 1 << 20) % (margin + 1)
    sizes = sizes.at[giver].add(-moved).at[sink].add(moved)
    labels = jnp.searchsorted(jnp.cumsum(sizes), jnp.arange(rows * top), side="right").astype(jnp.int32)
    table = labels.reshape(top, rows).T
    table = table[jax.random.permutation(jax.random.fold_in(own, 1), rows)]
    offset_by = jax.random.randint(jax.random.fold_in(own, 2), (rows, 1), 0, top)
    return jnp.take_along_axis(table, (jnp.arange(top)[None, :] + offset_by) % top, axis=1)


def portions_of(number_of, total, reach, skew, full):
    weights = [(1 << 20) // math.isqrt(grade ** skew) + 1 for grade in range(1, number_of + 1)]
    largest = reach if full else min(reach, max(-(-total // number_of), total * weights[0] // sum(weights)))
    least = 1 if total - largest >= number_of - 1 else 0
    given, surplus = [largest] + [least] * (number_of - 1), total - largest - least * (number_of - 1)
    while surplus > 0:
        candidates = [i for i in range(1, number_of) if given[i] < largest] or [i for i in range(1, number_of) if given[i] < reach]
        pool, budget = sum([weights[i] for i in candidates]), surplus
        for i in candidates:
            extra = min(reach - given[i], max(1, budget * weights[i] // pool), surplus)
            given[i] = given[i] + extra
            surplus = surplus - extra
    return np.array(given)


def scatter_about(key, shape, scale, most, cuts=(), held_as=jnp.bfloat16):
    values = jax.random.normal(key, shape, jnp.float32) * scale
    if len(cuts) > 0:
        values = steps_of(key, shape, cuts, -0.22, 0.18) * values
    return jnp.clip(values, min=-most, max=most).astype(held_as)


def setup_inputs(seed: int = 0) -> dict:
    arg_keys = jax.random.split(jax.random.key(seed), 14)
    hidden = scatter_about(arg_keys[0], (N_DP, SEG, SEQS, D), 1.0, 6.0, ((0, 2), (1, 16)))
    queries = draw_queries(jax.random.fold_in(arg_keys[13], 71), 0)
    latents = draw_latents(jax.random.fold_in(arg_keys[13], 71), 0)
    mem_latents = scatter_about(arg_keys[3], (N_DP, MEM, SEQS, LAT), 1.0, 6.0, ((0, 2),))
    lengths = set_ends(jax.random.randint(arg_keys[4], (N_DP, SEQS), SEG // 2, SEG + 1), jax.random.fold_in(arg_keys[4], 1), SEG // 2, SEG).astype(jnp.int32)
    ids_keys = jax.random.split(jax.random.fold_in(arg_keys[5], 1), N_DP * SEG * SEQS // TOK_DEV)
    ids_turns = jax.random.permutation(jax.random.fold_in(arg_keys[5], 3), N_DP * SEG * SEQS // TOK_DEV)
    ids = jax.vmap(lambda own, number: routed_block(jax.random.fold_in(arg_keys[5], 2), own, number, TOK_DEV, EXPERTS, TOPK, CAP, 2))(ids_keys, ids_turns).reshape((N_DP, SEG, SEQS, TOPK))
    gates = jnp.clip(jnp.exp(math.log(0.5) - 2.306499 * jax.random.uniform(arg_keys[6], (N_DP, SEG, SEQS, TOPK), jnp.float32) ** steps_of(arg_keys[6], (N_DP, SEG, SEQS, TOPK), ((0, 2), (1, 16)), -0.2, 0.2)), 0.049804688, 0.5).astype(jnp.bfloat16)
    norm_gain = jnp.clip(1.0 + 0.15 * jax.random.normal(arg_keys[7], (D,), jnp.float32), 0.25, 1.75).astype(jnp.bfloat16)
    w_uv = scatter_about(arg_keys[8], (HEADS, LAT, VDIM), LAT ** -0.5, 0.25, ((0, 2),))
    w_out = scatter_about(arg_keys[9], (HEADS * VDIM, D), (HEADS * VDIM) ** -0.5, 0.1875, ((0, 2),))
    w_gate = scatter_about(arg_keys[10], (EXPERTS, D, FF), D ** -0.5, 0.125, ((0, 16),))
    w_up = scatter_about(arg_keys[11], (EXPERTS, D, FF), D ** -0.5, 0.125, ((0, 16),))
    w_down = scatter_about(arg_keys[12], (EXPERTS, FF, D), FF ** -0.5, 0.21875, ((0, 16),))
    return {"hidden": hidden, "queries": queries, "latents": latents, "mem_latents": mem_latents, "lengths": lengths, "ids": ids, "gates": gates, "norm_gain": norm_gain, "w_uv": w_uv, "w_out": w_out, "w_gate": w_gate, "w_up": w_up, "w_down": w_down}


score_scale = 192.0 ** (-0.5)
norm_eps = 1e-06

def attend_one(query_rows, seg_latent, mem_latent, seq_limit):
    key_rows = jnp.concatenate([mem_latent, seg_latent], axis=0).astype(jnp.float32)
    scores = jnp.einsum('ihl,jl->hij', query_rows.astype(jnp.float32), key_rows) * score_scale
    query_pos = jnp.arange(SEG, dtype=jnp.int32)
    seg_visible = (query_pos[None, :] <= query_pos[:, None]) & (query_pos[None, :] < seq_limit)
    visible = jnp.concatenate([jnp.ones((SEG, MEM), dtype=bool), seg_visible], axis=1)
    scores = jnp.where(visible[None], scores, -jnp.inf)
    row_top = lax.optimization_barrier(jnp.max(scores, axis=2))
    weights = jnp.exp(scores - row_top[..., None])
    exp_total = lax.optimization_barrier(jnp.sum(weights, axis=2))
    rounded = lax.optimization_barrier(weights.astype(jnp.bfloat16)).astype(jnp.float32)
    attended = jnp.einsum('hij,jl->ihl', rounded, key_rows) / jnp.transpose(exp_total)[..., None]
    return attended.astype(jnp.bfloat16)

def reference(hidden, queries, latents, mem_latents, lengths, ids, gates, norm_gain, w_uv, w_out, w_gate, w_up, w_down):
    batch = N_DP * SEQS
    query_all = queries.reshape(N_DP, SEG, SEQS, HEADS, LAT).transpose(0, 2, 1, 3, 4).reshape(batch, SEG, HEADS, LAT)
    seg_all = latents.transpose(0, 2, 1, 3).reshape(batch, SEG, LAT)
    mem_all = mem_latents.transpose(0, 2, 1, 3).reshape(batch, MEM, LAT)
    limits = lengths.reshape(batch)
    attended = lax.map(lambda item: attend_one(item[0], item[1], item[2], item[3]), (query_all, seg_all, mem_all, limits))
    values = jnp.einsum('bihl,hlv->bihv', attended.astype(jnp.float32), w_uv.astype(jnp.float32)).astype(jnp.bfloat16)
    attn_out = jnp.dot(values.reshape(batch * SEG, HEADS * VDIM), w_out, preferred_element_type=jnp.float32)
    attn_out = attn_out.reshape(N_DP, SEQS, SEG, D).transpose(0, 2, 1, 3)
    residual = hidden.astype(jnp.float32) + attn_out
    mean_square = lax.optimization_barrier(jnp.mean(residual * residual, axis=-1, keepdims=True))
    normed = (residual * lax.rsqrt(mean_square + norm_eps) * norm_gain.astype(jnp.float32)).astype(jnp.bfloat16)
    row_total = N_DP * SEG * SEQS
    flat_normed = normed.reshape(row_total, D)
    flat_ids = ids.reshape(row_total * TOPK)
    flat_gates = gates.reshape(row_total * TOPK).astype(jnp.float32)
    reach_rows = N_DP * N_EXPERT * CAP

    def per_expert(running, item):
        gate_w, up_w, down_w, expert_id = item
        matches = flat_ids == expert_id
        picked = jnp.nonzero(matches, size=reach_rows, fill_value=0)[0].astype(jnp.int32)
        is_live = jnp.arange(reach_rows, dtype=jnp.int32) < jnp.sum(matches.astype(jnp.int32))
        token_index = (picked // TOPK).astype(jnp.int32)
        picked_rows = flat_normed[token_index]
        gate_h = jnp.dot(picked_rows, gate_w, preferred_element_type=jnp.float32)
        up_h = jnp.dot(picked_rows, up_w, preferred_element_type=jnp.float32)
        act = (jax.nn.silu(gate_h) * up_h).astype(jnp.bfloat16)
        out_rows = jnp.dot(act, down_w, preferred_element_type=jnp.float32).astype(jnp.bfloat16)
        out_rows = lax.optimization_barrier(out_rows).astype(jnp.float32)
        scale_w = jnp.where(is_live, flat_gates[picked], jnp.float32(0.0))
        running = running.at[token_index].add(scale_w[:, None] * out_rows)
        return (running, None)
    start_acc = jnp.zeros((row_total, D), jnp.float32)
    routed, unused = lax.scan(per_expert, start_acc, (w_gate, w_up, w_down, jnp.arange(EXPERTS, dtype=jnp.int32)))
    layer_out = residual + routed.reshape(N_DP, SEG, SEQS, D)
    return layer_out.astype(jnp.bfloat16)
```

```python
import functools

import jax
import jax.numpy as jnp
from jax import lax
from jax.experimental import pallas as pl
from jax.experimental.pallas import tpu as pltpu
from jax.sharding import PartitionSpec as P

score_scale = 192.0 ** (-0.5)
norm_eps = 1e-06
MESH = pl.DeviceIdType.MESH


def ring_place(n):
    chips = n // 2
    depth = chips // 2
    me = lax.axis_index("expert")
    core = me % 2
    chip = me // 2
    row, col = chip // 2, chip % 2
    pos = col * row + (1 - col) * (chips - 1 - row)

    def device(offset, core_of):
        p = (pos + offset + chips) % chips
        q = p // depth
        r = (1 - q) * p + q * (chips - 1 - p)
        return (2 * r + 1 - q) * 2 + core_of

    return me, core, device


def greet(targets):
    barrier = pltpu.get_barrier_semaphore()
    for target in targets:
        pl.semaphore_signal(barrier, inc=1, device_id={"expert": target}, device_id_type=MESH)
    pl.semaphore_wait(barrier, len(targets))


def remote(src, dst, send_sem, recv_sem, target):
    return pltpu.make_async_remote_copy(
        src_ref=src,
        dst_ref=dst,
        send_sem=send_sem,
        recv_sem=recv_sem,
        device_id={"expert": target},
        device_id_type=MESH,
    )


def gather_kernel(n, cut, x_ref, out_ref, ring_send, ring_recv, pair_send, pair_recv, own_sem):
    chips = n // 2
    half_ring = chips // 2
    rows = x_ref.shape[0]
    last = chips - 2
    me, core, device = ring_place(n)
    partner = device(0, 1 - core)
    ahead = (device(1, core), device(-1, core))
    spans = (pl.ds(0, cut), pl.ds(cut, rows - cut))
    greet((ahead[0], ahead[1], partner))

    def arrival(way, j):
        dist, half = (half_ring, way) if j == last else (j // 2 + 1, j % 2)
        return device(-dist if way == 0 else dist, core), spans[half]

    waits = []
    for way in (0, 1):
        for j in (0, 1):
            if j > last:
                continue
            if j == last and half_ring == 1:
                span = spans[way]
            else:
                span = spans[j]
            copy = remote(
                x_ref.at[span], out_ref.at[me, span],
                ring_send.at[way, j], ring_recv.at[way, j], ahead[way],
            )
            copy.start()
            waits.append(copy)
    share = remote(x_ref, out_ref.at[me], pair_send.at[2 * last + 2], pair_recv.at[2 * last + 2], partner)
    share.start()
    waits.append(share)
    keep = pltpu.make_async_copy(x_ref, out_ref.at[me], own_sem)
    keep.start()

    for j in range(last + 1):
        for way in (0, 1):
            slot, span = arrival(way, j)
            piece = out_ref.at[slot, span]
            remote(piece, piece, ring_send.at[way, j], ring_recv.at[way, j], ahead[way]).wait_recv()
            onward = j + 2
            if j >= last - 2 and j < last:
                onward = last if j == last - 2 + way else None
            if j == last:
                onward = None
            if onward is not None:
                copy = remote(piece, piece, ring_send.at[way, onward], ring_recv.at[way, onward], ahead[way])
                copy.start()
                waits.append(copy)
            index = 2 * j + way
            copy = remote(piece, piece, pair_send.at[index], pair_recv.at[index], partner)
            copy.start()
            waits.append(copy)

    for j in range(last + 1):
        for way in (0, 1):
            dist, half = (half_ring, way) if j == last else (j // 2 + 1, j % 2)
            slot = device(-dist if way == 0 else dist, 1 - core)
            piece = out_ref.at[slot, spans[half]]
            index = 2 * j + way
            remote(piece, piece, pair_send.at[index], pair_recv.at[index], partner).wait_recv()
    other = out_ref.at[partner]
    remote(other, other, pair_send.at[2 * last + 2], pair_recv.at[2 * last + 2], partner).wait_recv()
    for copy in waits:
        copy.wait_send()
    keep.wait()


def ring_gather(x, n, cut, collective_id):
    rows, cols = x.shape
    steps = n // 2 - 1
    return pl.pallas_call(
        functools.partial(gather_kernel, n, cut),
        out_shape=jax.ShapeDtypeStruct((n, rows, cols), x.dtype),
        in_specs=[pl.BlockSpec(memory_space=pltpu.VMEM)],
        out_specs=pl.BlockSpec(memory_space=pl.ANY),
        scratch_shapes=[
            pltpu.SemaphoreType.DMA((2, steps)),
            pltpu.SemaphoreType.DMA((2, steps)),
            pltpu.SemaphoreType.DMA((2 * steps + 1,)),
            pltpu.SemaphoreType.DMA((2 * steps + 1,)),
            pltpu.SemaphoreType.DMA,
        ],
        compiler_params=pltpu.CompilerParams(collective_id=collective_id, has_side_effects=True),
        cost_estimate=pl.CostEstimate(flops=0, bytes_accessed=16 * n * rows * cols, transcendentals=0),
        name="ring_gather_%d" % collective_id,
    )(x)


def reduce_kernel(
    n, rows_ref, mix_ref, out_ref, mine, paired, give, arrived, ring_send, ring_recv, pair_send, pair_recv
):
    chips = n // 2
    half_ring = chips // 2
    half = mine.shape[1] // 2
    last = chips - 2
    me, core, device = ring_place(n)
    partner = device(0, 1 - core)
    ahead = (device(1, core), device(-1, core))
    greet((ahead[0], ahead[1], partner))

    order = [half_ring]
    for k in range(half_ring - 1, 0, -1):
        order += [k, chips - k]
    order.append(0)
    depth = give.shape[0]
    shares, made, seen = {}, [], set()

    def weigh(k, core_of):
        dest = device(k, core_of)
        return jnp.dot(
            mix_ref[dest], rows_ref[dest // 2], preferred_element_type=jnp.float32
        ).astype(mine.dtype)

    def make():
        k = order[len(made)]
        slot = len(made) % depth
        if len(made) >= depth:
            shares[order[len(made) - depth]].wait_send()
        give[slot] = weigh(k, 1 - core)
        shares[k] = remote(give.at[slot], paired.at[k], pair_send.at[k], pair_recv.at[k], partner)
        shares[k].start()
        mine[k] = weigh(k, core)
        made.append(k)

    def bring(k):
        while k not in made or (len(made) < chips and len(made) < order.index(k) + 3):
            make()
        if k not in seen:
            seen.add(k)
            shares[k].wait_recv()

    def index_of(dist, h):
        return 0 if dist == half_ring else 1 + 2 * (half_ring - 1 - dist) + h

    def await_ring(way, j):
        piece = arrived.at[way, j]
        remote(piece, piece, ring_send.at[way, j], ring_recv.at[way, j], ahead[way]).wait_recv()

    sends = []
    for dist in range(half_ring, 0, -1):
        for turn in (0, 1):
            for way in (0, 1):
                if dist == half_ring:
                    if turn == 1:
                        continue
                    h = way
                elif dist == half_ring - 1:
                    h = 1 - way if turn == 0 else way
                else:
                    h = turn
                k = dist if way == 0 else chips - dist
                bring(k)
                span = pl.ds(h * half, half)
                total = mine[k, span].astype(jnp.float32) + paired[k, span].astype(jnp.float32)
                has_prior = dist < half_ring - 1 or (dist == half_ring - 1 and h == way)
                if has_prior:
                    j = index_of(dist + 1, h)
                    await_ring(way, j)
                    total = total + arrived[way, j].astype(jnp.float32)
                mine[k, span] = total.astype(mine.dtype)
                j = index_of(dist, h)
                copy = remote(
                    mine.at[k, span], arrived.at[way, j],
                    ring_send.at[way, j], ring_recv.at[way, j], ahead[way],
                )
                copy.start()
                sends.append(copy)
    bring(0)
    for h in (0, 1):
        span = pl.ds(h * half, half)
        total = mine[0, span].astype(jnp.float32) + paired[0, span].astype(jnp.float32)
        for way in (0, 1):
            j = index_of(1, h)
            await_ring(way, j)
            total = total + arrived[way, j].astype(jnp.float32)
        out_ref[span] = total
    for copy in sends:
        copy.wait_send()
    for k in order[chips - min(depth, chips) :]:
        shares[k].wait_send()


def ring_reduce(rows_in, mix, n, collective_id):
    rows = mix.shape[1]
    cols = rows_in.shape[2]
    chips = n // 2
    dtype = rows_in.dtype
    return pl.pallas_call(
        functools.partial(reduce_kernel, n),
        out_shape=jax.ShapeDtypeStruct((rows, cols), jnp.float32),
        in_specs=[pl.BlockSpec(memory_space=pltpu.VMEM)] * 2,
        out_specs=pl.BlockSpec(memory_space=pltpu.VMEM),
        scratch_shapes=[
            pltpu.VMEM((chips, rows, cols), dtype),
            pltpu.VMEM((chips, rows, cols), dtype),
            pltpu.VMEM((min(4, chips), rows, cols), dtype),
            pltpu.VMEM((2, chips - 1, rows // 2, cols), dtype),
            pltpu.SemaphoreType.DMA((2, chips - 1)),
            pltpu.SemaphoreType.DMA((2, chips - 1)),
            pltpu.SemaphoreType.DMA((chips,)),
            pltpu.SemaphoreType.DMA((chips,)),
        ],
        compiler_params=pltpu.CompilerParams(
            collective_id=collective_id, has_side_effects=True, vmem_limit_bytes=62 * 1024 * 1024
        ),
        cost_estimate=pl.CostEstimate(
            flops=2 * mix.size * cols, bytes_accessed=16 * n * rows * cols, transcendentals=0
        ),
        name="ring_reduce_%d" % collective_id,
    )(rows_in, mix)


def expert_kernel(
    n, x_ref, keep_ref, place_ref, mix_ref, gate_hbm, up_hbm, down_hbm, out_ref,
    rows, w_gate, w_up, w_down, act, mine, paired, give, arrived,
    load_sem, gather_send, gather_recv, swap_send, swap_recv, ring_send, ring_recv, pair_send, pair_recv,
):
    f32 = jnp.float32
    chips = n // 2
    half_ring = chips // 2
    count, width = x_ref.shape
    half = count // 2
    slots = place_ref.shape[1]
    last = chips - 2
    me, core, device = ring_place(n)
    partner = device(0, 1 - core)
    ahead = (device(1, core), device(-1, core))
    spans = (pl.ds(0, half), pl.ds(half, half))
    loads = [
        pltpu.make_async_copy(src, dst, load_sem.at[i])
        for i, (src, dst) in enumerate(((gate_hbm, w_gate), (up_hbm, w_up), (down_hbm, w_down)))
    ]
    for load in loads:
        load.start()
    greet((ahead[0], ahead[1], partner))
    waits = []

    def send(copy):
        copy.start()
        waits.append(copy)

    def step_of(way, j):
        return (half_ring, way) if j == last else (j // 2 + 1, j % 2)

    def offset(way, dist):
        return dist if way == 0 else chips - dist

    for j in (0, 1):
        for way in (0, 1):
            send(remote(
                x_ref.at[spans[j]], rows.at[me, spans[j]],
                gather_send.at[way, j], gather_recv.at[way, j], ahead[way],
            ))
    send(remote(x_ref, rows.at[me], swap_send.at[2 * last + 2], swap_recv.at[2 * last + 2], partner))
    rows[me] = x_ref[...]

    def start_experts(ks):
        picked = []
        for k in ks:
            first = device(k, 0)
            held = rows[pl.ds(first, 2)].reshape(2 * count, width)
            picked.append(jnp.dot(place_ref[first // 2], held, preferred_element_type=f32).astype(jnp.bfloat16))
        picked = picked[0] if len(ks) == 1 else jnp.concatenate(picked, axis=0)
        along = (((1,), (1,)), ((), ()))
        gate_h = lax.dot_general(picked, w_gate[...], along, preferred_element_type=f32)
        up_h = lax.dot_general(picked, w_up[...], along, preferred_element_type=f32)
        act[pl.ds(0, len(ks) * slots)] = (gate_h / (1.0 + jnp.exp(-gate_h)) * up_h).astype(jnp.bfloat16)

    shares = {}

    def end_experts(ks):
        made = jnp.dot(act[pl.ds(0, len(ks) * slots)], w_down[...], preferred_element_type=f32).astype(jnp.bfloat16)
        for i, k in enumerate(ks):
            part = made[i * slots : (i + 1) * slots]
            give[k] = jnp.dot(mix_ref[device(k, 1 - core)], part, preferred_element_type=f32).astype(give.dtype)
            shares[k] = remote(give.at[k], paired.at[k], pair_send.at[k], pair_recv.at[k], partner)
            send(shares[k])
            mine[k] = jnp.dot(mix_ref[device(k, core)], part, preferred_element_type=f32).astype(mine.dtype)

    seen = set()

    def bring(k):
        if k not in seen:
            seen.add(k)
            shares[k].wait_recv()

    def index_of(dist, h):
        return 0 if dist == half_ring else 1 + 2 * (half_ring - 1 - dist) + h

    def await_ring(way, j):
        piece = arrived.at[way, j]
        remote(piece, piece, ring_send.at[way, j], ring_recv.at[way, j], ahead[way]).wait_recv()

    def advance(dist, chain):
        for way in (0, 1):
            h = way if chain == 0 else 1 - way
            k = offset(way, dist)
            bring(k)
            total = mine[k, spans[h]].astype(f32) + paired[k, spans[h]].astype(f32)
            if dist < half_ring - chain:
                j = index_of(dist + 1, h)
                await_ring(way, j)
                total = total + arrived[way, j].astype(f32)
            mine[k, spans[h]] = total.astype(mine.dtype)
            j = index_of(dist, h)
            send(remote(
                mine.at[k, spans[h]], arrived.at[way, j],
                ring_send.at[way, j], ring_recv.at[way, j], ahead[way],
            ))

    other = rows.at[partner]
    remote(other, other, swap_send.at[2 * last + 2], swap_recv.at[2 * last + 2], partner).wait_recv()
    for load in loads:
        load.wait()
    start_experts([0])
    end_experts([0])

    tasks = []
    for j in range(last + 1):
        for way in (0, 1):
            dist, h = step_of(way, j)
            piece = rows.at[device(-dist if way == 0 else dist, core), spans[h]]
            remote(piece, piece, gather_send.at[way, j], gather_recv.at[way, j], ahead[way]).wait_recv()
            onward = j + 2
            if last - 2 <= j < last:
                onward = last if j == last - 2 + way else None
            if j == last:
                onward = None
            if onward is not None:
                send(remote(
                    piece, piece, gather_send.at[way, onward], gather_recv.at[way, onward], ahead[way]
                ))
            send(remote(piece, piece, swap_send.at[2 * j + way], swap_recv.at[2 * j + way], partner))
        if j % 2 == 1 or j == last:
            for i in ((j - 1, j) if j % 2 == 1 else (j,)):
                for way in (0, 1):
                    dist, h = step_of(way, i)
                    piece = rows.at[device(-dist if way == 0 else dist, 1 - core), spans[h]]
                    remote(piece, piece, swap_send.at[2 * i + way], swap_recv.at[2 * i + way], partner).wait_recv()
            dist = step_of(0, j)[0]
            ks = [half_ring] if j == last else [dist, chips - dist]
            tasks += [functools.partial(start_experts, ks), functools.partial(end_experts, ks)]
        for _ in range(min(len(tasks), 1 if j < last - 1 else len(tasks))):
            tasks.pop(0)()
        if j == last - 1:
            advance(half_ring - 1, 1)

    advance(half_ring, 0)
    for dist in range(half_ring - 2, 0, -1):
        advance(dist, 1)
        advance(dist + 1, 0)
    advance(1, 0)

    bring(0)
    for h in (0, 1):
        total = mine[0, spans[h]].astype(f32) + paired[0, spans[h]].astype(f32)
        for way in (0, 1):
            j = index_of(1, h)
            await_ring(way, j)
            total = total + arrived[way, j].astype(f32)
        out_ref[spans[h]] = (keep_ref[spans[h]] + total).astype(out_ref.dtype)
    for copy in waits:
        copy.wait_send()


def expert_bytes(n, count, width, inner, slots):
    chips = n // 2
    held = n * count * width + 3 * width * inner + 3 * chips * count * width + (chips - 1) * count * width
    held += 6 * count * width + 2 * chips * slots * 2 * count
    return 2 * held + 4 * 2 * slots * (2 * inner + 2 * width)


def ring_experts(x, keep, place, mix, w_gate_t, w_up_t, w_down, n, collective_id):
    count, width = x.shape
    chips = n // 2
    steps = chips - 1
    inner = w_down.shape[0]
    slots = place.shape[1]
    dtype = x.dtype
    dma = pltpu.SemaphoreType.DMA
    return pl.pallas_call(
        functools.partial(expert_kernel, n),
        out_shape=jax.ShapeDtypeStruct((count, width), dtype),
        in_specs=[pl.BlockSpec(memory_space=pltpu.VMEM)] * 4 + [pl.BlockSpec(memory_space=pl.ANY)] * 3,
        out_specs=pl.BlockSpec(memory_space=pltpu.VMEM),
        scratch_shapes=[
            pltpu.VMEM((n, count, width), dtype),
            pltpu.VMEM((inner, width), dtype),
            pltpu.VMEM((inner, width), dtype),
            pltpu.VMEM((inner, width), dtype),
            pltpu.VMEM((2 * slots, inner), dtype),
            pltpu.VMEM((chips, count, width), dtype),
            pltpu.VMEM((chips, count, width), dtype),
            pltpu.VMEM((chips, count, width), dtype),
            pltpu.VMEM((2, steps, count // 2, width), dtype),
            dma((3,)),
            dma((2, steps)),
            dma((2, steps)),
            dma((2 * steps + 1,)),
            dma((2 * steps + 1,)),
            dma((2, steps)),
            dma((2, steps)),
            dma((chips,)),
            dma((chips,)),
        ],
        compiler_params=pltpu.CompilerParams(
            collective_id=collective_id, has_side_effects=True, vmem_limit_bytes=62 * 1024 * 1024
        ),
        cost_estimate=pl.CostEstimate(
            flops=6 * chips * slots * width * inner, bytes_accessed=32 * n * count * width, transcendentals=0
        ),
        name="ring_experts_%d" % collective_id,
    )(x, keep, place, mix, w_gate_t, w_up_t, w_down)


def shards(
    hidden,
    queries,
    latents,
    mem_latents,
    lengths,
    ids,
    gates,
    norm_gain,
    w_uv,
    w_out,
    w_gate,
    w_up,
    w_down,
):
    f32, bf16 = jnp.float32, jnp.bfloat16
    local_len, seq_count, model_width = hidden.shape[1:]
    latent_dim = latents.shape[3]
    head_count = queries.shape[3] // latent_dim
    row_count = local_len * seq_count
    n = lax.axis_size("expert")
    dp_size = lax.axis_size("dp")
    me = lax.axis_index("expert")
    core = me % 2
    own_dp = lax.axis_index("dp")
    heads_here, _, value_dim = w_uv.shape
    top_count = ids.shape[3]

    half_heads = heads_here // 2
    uv_half = lax.dynamic_slice_in_dim(w_uv, core * half_heads, half_heads, 0)
    out_half = lax.dynamic_slice_in_dim(
        w_out, core * half_heads * value_dim, half_heads * value_dim, 0
    )
    uv_groups, out_groups, starts = [w_uv], [w_out], [own_dp * heads_here]
    swap = [(i, i ^ 1) for i in range(n)]
    sizes = [heads_here]
    for shift in range(1, dp_size):
        turn = [(i, (i + shift) % dp_size) for i in range(dp_size)]
        source = (own_dp - shift + dp_size) % dp_size
        uv_far = lax.ppermute(uv_half, "dp", turn)
        out_far = lax.ppermute(out_half, "dp", turn)
        uv_near = lax.ppermute(uv_far, "expert", swap)
        out_near = lax.ppermute(out_far, "expert", swap)
        uv_groups += [uv_far, uv_near]
        out_groups += [out_far, out_near]
        starts += [
            source * heads_here + core * half_heads,
            source * heads_here + (1 - core) * half_heads,
        ]
        sizes += [half_heads, half_heads]

    latent_rows = jnp.transpose(latents[0], (1, 0, 2)).reshape(row_count, latent_dim)
    ids_t = jnp.transpose(ids[0], (2, 1, 0)).reshape(top_count, row_count).astype(bf16)
    gates_t = jnp.transpose(gates[0], (2, 1, 0)).reshape(top_count, row_count)
    table = jnp.concatenate([ids_t, gates_t], axis=0).reshape(-1)
    table_rows = -(-table.shape[0] // (16 * latent_dim)) * 16
    table = jnp.pad(table, (0, table_rows * latent_dim - table.shape[0]))
    packed = jnp.concatenate([latent_rows, table.reshape(table_rows, latent_dim)], axis=0)
    all_rows = row_count + table_rows
    cut = (all_rows // 2 + 15) // 16 * 16
    gathered = ring_gather(packed, n, cut, 0)

    segment = gathered[:, :row_count].reshape(n, seq_count, local_len, latent_dim)
    segment = jnp.transpose(segment, (1, 0, 2, 3)).reshape(seq_count, n * local_len, latent_dim)
    memory = jnp.transpose(mem_latents[0], (1, 0, 2))
    mem_count = memory.shape[1]
    keys = jnp.concatenate([memory, segment], axis=1)
    query_rows = jnp.transpose(
        queries[0].reshape(local_len, seq_count, head_count, latent_dim), (1, 2, 0, 3)
    ).reshape(seq_count, head_count * local_len, latent_dim)
    scores = jnp.einsum("sql,sjl->sqj", query_rows, keys, preferred_element_type=f32) * score_scale
    key_pos = lax.broadcasted_iota(jnp.int32, scores.shape, 2) - mem_count
    own_pos = me * local_len + lax.broadcasted_iota(jnp.int32, scores.shape, 1) % local_len
    visible = (key_pos <= own_pos) & (key_pos < lengths[0][:, None, None])
    scores = jnp.where(visible | (key_pos < 0), scores, -jnp.inf)
    weights = jnp.exp(scores - jnp.max(scores, axis=2, keepdims=True))
    total = jnp.sum(weights, axis=2, keepdims=True)
    attended = jnp.einsum("sqj,sjl->sql", weights.astype(bf16), keys, preferred_element_type=f32)
    attended = (attended / total).astype(bf16)
    attended = attended.reshape(seq_count, head_count, local_len, latent_dim)

    attn_out = jnp.zeros((row_count, model_width), f32)
    for uv, out, start, size in zip(uv_groups, out_groups, starts, sizes):
        heads = lax.dynamic_slice_in_dim(attended, start, size, 1)
        values = jnp.einsum("shtl,hlv->sthv", heads, uv, preferred_element_type=f32).astype(bf16)
        attn_out = attn_out + jnp.dot(
            values.reshape(row_count, size * value_dim), out, preferred_element_type=f32
        )

    hidden_rows = jnp.transpose(hidden[0], (1, 0, 2)).reshape(row_count, model_width)
    residual = lax.optimization_barrier(hidden_rows).astype(f32) + attn_out
    mean_square = jnp.mean(residual * residual, axis=-1, keepdims=True)
    normed = (residual * lax.rsqrt(mean_square + norm_eps) * norm_gain.astype(f32)).astype(bf16)

    experts_here = w_gate.shape[0]
    expert_count = n * experts_here
    capacity = min(row_count, row_count * top_count // expert_count + 2)
    groups = n // 2
    wide = 2 * row_count
    slots = -(-2 * capacity // 128) * 128
    inner = w_down.shape[1]
    joined = (
        experts_here == 1
        and groups >= 4
        and row_count % 32 == 0
        and expert_bytes(n, row_count, model_width, inner, slots) < 52 * 1024 * 1024
    )
    if not joined:
        slots = -(-2 * capacity // 16) * 16
    tables = gathered[:, row_count:].reshape(n, -1)[:, : 2 * top_count * row_count]
    tables = tables.reshape(groups, 2, 2, top_count, row_count)
    named = jnp.transpose(tables[:, :, 0], (2, 0, 1, 3)).reshape(top_count, groups, wide)
    scale = jnp.transpose(tables[:, :, 1], (2, 0, 1, 3)).reshape(top_count, groups, wide)
    if not joined:
        rows_all = ring_gather(normed, n, row_count // 2, 1).reshape(groups, wide, model_width)
    steps = jnp.arange(wide, dtype=jnp.int32)
    earlier = (steps[:, None] < steps[None, :]).astype(bf16)
    made_rows, mixes = [], []
    for e in range(experts_here):
        matches = named == (me * experts_here + e).astype(bf16)
        hit = jnp.any(matches, axis=0)
        gate = jnp.sum(jnp.where(matches, scale.astype(f32), 0.0), axis=0)
        slot = jnp.dot(hit.astype(bf16), earlier, preferred_element_type=f32).astype(jnp.int32)
        slot = jnp.where(hit, slot, -1)
        chosen = slot[:, None, :] == jnp.arange(slots, dtype=jnp.int32)[None, :, None]
        placing = chosen.astype(bf16)
        slot_t = jnp.where(hit, slot, -1).reshape(n, row_count)
        chosen_t = slot_t[:, :, None] == jnp.arange(slots, dtype=jnp.int32)[None, None, :]
        mixes.append(jnp.where(chosen_t, gate.reshape(n, row_count)[:, :, None], 0.0).astype(bf16))
        if joined:
            layer_out = ring_experts(
                normed, residual, placing, mixes[0],
                jnp.transpose(w_gate[0]), jnp.transpose(w_up[0]), w_down[0], n, 3,
            )
            return jnp.transpose(layer_out.reshape(seq_count, local_len, model_width), (1, 0, 2))[None]
        picked = jnp.einsum("gct,gtd->gcd", placing, rows_all, preferred_element_type=f32)
        picked = picked.astype(bf16).reshape(groups * slots, model_width)
        gate_h = jnp.dot(picked, w_gate[e], preferred_element_type=f32)
        up_h = jnp.dot(picked, w_up[e], preferred_element_type=f32)
        act = (jax.nn.silu(gate_h) * up_h).astype(bf16)
        produced = jnp.dot(act, w_down[e], preferred_element_type=f32).astype(bf16)
        made_rows.append(produced.reshape(groups, slots, model_width))
    made_rows = made_rows[0] if experts_here == 1 else jnp.concatenate(made_rows, axis=1)
    mixing = mixes[0] if experts_here == 1 else jnp.concatenate(mixes, axis=2)
    routed = ring_reduce(made_rows, mixing, n, 2)
    layer_out = (residual + routed).astype(bf16).reshape(seq_count, local_len, model_width)
    return jnp.transpose(layer_out, (1, 0, 2))[None]


def solution(mesh):
    return jax.shard_map(
        shards,
        mesh=mesh,
        in_specs=(
            P("dp", "expert", None, None),
            P("dp", "expert", None, None),
            P("dp", "expert", None, None),
            P("dp", None, None, None),
            P("dp", None),
            P("dp", "expert", None, None),
            P("dp", "expert", None, None),
            P(),
            P("dp", None, None),
            P("dp", None),
            P("expert", None, None),
            P("expert", None, None),
            P("expert", None, None),
        ),
        out_specs=P("dp", "expert", None, None),
        check_vma=False,
    )
```

```python
import functools

import jax
import jax.numpy as jnp
from jax import lax
from jax.experimental import pallas as pl
from jax.experimental.pallas import tpu as pltpu
from jax.sharding import PartitionSpec as P

score_scale = 192.0 ** (-0.5)
norm_eps = 1e-06
MESH = pl.DeviceIdType.MESH


def ring_place(n):
    chips = n // 2
    depth = chips // 2
    me = lax.axis_index("expert")
    core = me % 2
    chip = me // 2
    row, col = chip // 2, chip % 2
    pos = col * row + (1 - col) * (chips - 1 - row)

    def device(offset, core_of):
        p = (pos + offset + chips) % chips
        q = p // depth
        r = (1 - q) * p + q * (chips - 1 - p)
        return (2 * r + 1 - q) * 2 + core_of

    return me, core, device


def greet(targets):
    barrier = pltpu.get_barrier_semaphore()
    for target in targets:
        pl.semaphore_signal(barrier, inc=1, device_id={"expert": target}, device_id_type=MESH)
    pl.semaphore_wait(barrier, len(targets))


def remote(src, dst, send_sem, recv_sem, target):
    return pltpu.make_async_remote_copy(
        src_ref=src,
        dst_ref=dst,
        send_sem=send_sem,
        recv_sem=recv_sem,
        device_id={"expert": target},
        device_id_type=MESH,
    )


def gather_kernel(n, cut, x_ref, out_ref, ring_send, ring_recv, pair_send, pair_recv, own_sem):
    chips = n // 2
    half_ring = chips // 2
    rows = x_ref.shape[0]
    last = chips - 2
    me, core, device = ring_place(n)
    partner = device(0, 1 - core)
    ahead = (device(1, core), device(-1, core))
    spans = (pl.ds(0, cut), pl.ds(cut, rows - cut))
    greet((ahead[0], ahead[1], partner))

    def arrival(way, j):
        dist, half = (half_ring, way) if j == last else (j // 2 + 1, j % 2)
        return device(-dist if way == 0 else dist, core), spans[half]

    waits = []
    for way in (0, 1):
        for j in (0, 1):
            if j > last:
                continue
            if j == last and half_ring == 1:
                span = spans[way]
            else:
                span = spans[j]
            copy = remote(
                x_ref.at[span], out_ref.at[me, span],
                ring_send.at[way, j], ring_recv.at[way, j], ahead[way],
            )
            copy.start()
            waits.append(copy)
    share = remote(x_ref, out_ref.at[me], pair_send.at[2 * last + 2], pair_recv.at[2 * last + 2], partner)
    share.start()
    waits.append(share)
    keep = pltpu.make_async_copy(x_ref, out_ref.at[me], own_sem)
    keep.start()

    for j in range(last + 1):
        for way in (0, 1):
            slot, span = arrival(way, j)
            piece = out_ref.at[slot, span]
            remote(piece, piece, ring_send.at[way, j], ring_recv.at[way, j], ahead[way]).wait_recv()
            onward = j + 2
            if j >= last - 2 and j < last:
                onward = last if j == last - 2 + way else None
            if j == last:
                onward = None
            if onward is not None:
                copy = remote(piece, piece, ring_send.at[way, onward], ring_recv.at[way, onward], ahead[way])
                copy.start()
                waits.append(copy)
            index = 2 * j + way
            copy = remote(piece, piece, pair_send.at[index], pair_recv.at[index], partner)
            copy.start()
            waits.append(copy)

    for j in range(last + 1):
        for way in (0, 1):
            dist, half = (half_ring, way) if j == last else (j // 2 + 1, j % 2)
            slot = device(-dist if way == 0 else dist, 1 - core)
            piece = out_ref.at[slot, spans[half]]
            index = 2 * j + way
            remote(piece, piece, pair_send.at[index], pair_recv.at[index], partner).wait_recv()
    other = out_ref.at[partner]
    remote(other, other, pair_send.at[2 * last + 2], pair_recv.at[2 * last + 2], partner).wait_recv()
    for copy in waits:
        copy.wait_send()
    keep.wait()


def ring_gather(x, n, cut, collective_id):
    rows, cols = x.shape
    steps = n // 2 - 1
    return pl.pallas_call(
        functools.partial(gather_kernel, n, cut),
        out_shape=jax.ShapeDtypeStruct((n, rows, cols), x.dtype),
        in_specs=[pl.BlockSpec(memory_space=pltpu.VMEM)],
        out_specs=pl.BlockSpec(memory_space=pl.ANY),
        scratch_shapes=[
            pltpu.SemaphoreType.DMA((2, steps)),
            pltpu.SemaphoreType.DMA((2, steps)),
            pltpu.SemaphoreType.DMA((2 * steps + 1,)),
            pltpu.SemaphoreType.DMA((2 * steps + 1,)),
            pltpu.SemaphoreType.DMA,
        ],
        compiler_params=pltpu.CompilerParams(collective_id=collective_id, has_side_effects=True),
        cost_estimate=pl.CostEstimate(flops=0, bytes_accessed=16 * n * rows * cols, transcendentals=0),
        name="ring_gather_%d" % collective_id,
    )(x)


def reduce_kernel(
    n, rows_ref, mix_ref, out_ref, mine, paired, give, arrived, ring_send, ring_recv, pair_send, pair_recv
):
    chips = n // 2
    half_ring = chips // 2
    half = mine.shape[1] // 2
    last = chips - 2
    me, core, device = ring_place(n)
    partner = device(0, 1 - core)
    ahead = (device(1, core), device(-1, core))
    greet((ahead[0], ahead[1], partner))

    order = [half_ring]
    for k in range(half_ring - 1, 0, -1):
        order += [k, chips - k]
    order.append(0)
    depth = give.shape[0]
    shares, made, seen = {}, [], set()

    def weigh(k, core_of):
        dest = device(k, core_of)
        return jnp.dot(
            mix_ref[dest], rows_ref[dest // 2], preferred_element_type=jnp.float32
        ).astype(mine.dtype)

    def make():
        k = order[len(made)]
        slot = len(made) % depth
        if len(made) >= depth:
            shares[order[len(made) - depth]].wait_send()
        give[slot] = weigh(k, 1 - core)
        shares[k] = remote(give.at[slot], paired.at[k], pair_send.at[k], pair_recv.at[k], partner)
        shares[k].start()
        mine[k] = weigh(k, core)
        made.append(k)

    def bring(k):
        while k not in made or (len(made) < chips and len(made) < order.index(k) + 3):
            make()
        if k not in seen:
            seen.add(k)
            shares[k].wait_recv()

    def index_of(dist, h):
        return 0 if dist == half_ring else 1 + 2 * (half_ring - 1 - dist) + h

    def await_ring(way, j):
        piece = arrived.at[way, j]
        remote(piece, piece, ring_send.at[way, j], ring_recv.at[way, j], ahead[way]).wait_recv()

    sends = []
    for dist in range(half_ring, 0, -1):
        for turn in (0, 1):
            for way in (0, 1):
                if dist == half_ring:
                    if turn == 1:
                        continue
                    h = way
                elif dist == half_ring - 1:
                    h = 1 - way if turn == 0 else way
                else:
                    h = turn
                k = dist if way == 0 else chips - dist
                bring(k)
                span = pl.ds(h * half, half)
                total = mine[k, span].astype(jnp.float32) + paired[k, span].astype(jnp.float32)
                has_prior = dist < half_ring - 1 or (dist == half_ring - 1 and h == way)
                if has_prior:
                    j = index_of(dist + 1, h)
                    await_ring(way, j)
                    total = total + arrived[way, j].astype(jnp.float32)
                mine[k, span] = total.astype(mine.dtype)
                j = index_of(dist, h)
                copy = remote(
                    mine.at[k, span], arrived.at[way, j],
                    ring_send.at[way, j], ring_recv.at[way, j], ahead[way],
                )
                copy.start()
                sends.append(copy)
    bring(0)
    for h in (0, 1):
        span = pl.ds(h * half, half)
        total = mine[0, span].astype(jnp.float32) + paired[0, span].astype(jnp.float32)
        for way in (0, 1):
            j = index_of(1, h)
            await_ring(way, j)
            total = total + arrived[way, j].astype(jnp.float32)
        out_ref[span] = total
    for copy in sends:
        copy.wait_send()
    for k in order[chips - min(depth, chips) :]:
        shares[k].wait_send()


def ring_reduce(rows_in, mix, n, collective_id):
    rows = mix.shape[1]
    cols = rows_in.shape[2]
    chips = n // 2
    dtype = rows_in.dtype
    return pl.pallas_call(
        functools.partial(reduce_kernel, n),
        out_shape=jax.ShapeDtypeStruct((rows, cols), jnp.float32),
        in_specs=[pl.BlockSpec(memory_space=pltpu.VMEM)] * 2,
        out_specs=pl.BlockSpec(memory_space=pltpu.VMEM),
        scratch_shapes=[
            pltpu.VMEM((chips, rows, cols), dtype),
            pltpu.VMEM((chips, rows, cols), dtype),
            pltpu.VMEM((min(4, chips), rows, cols), dtype),
            pltpu.VMEM((2, chips - 1, rows // 2, cols), dtype),
            pltpu.SemaphoreType.DMA((2, chips - 1)),
            pltpu.SemaphoreType.DMA((2, chips - 1)),
            pltpu.SemaphoreType.DMA((chips,)),
            pltpu.SemaphoreType.DMA((chips,)),
        ],
        compiler_params=pltpu.CompilerParams(
            collective_id=collective_id, has_side_effects=True, vmem_limit_bytes=62 * 1024 * 1024
        ),
        cost_estimate=pl.CostEstimate(
            flops=2 * mix.size * cols, bytes_accessed=16 * n * rows * cols, transcendentals=0
        ),
        name="ring_reduce_%d" % collective_id,
    )(rows_in, mix)


def layer_kernel(
    n, table_ref, limit_ref, gain_ref,
    latent_hbm, query_hbm, memory_hbm, hidden_hbm, uv_hbm, wout_hbm, gate_hbm, up_hbm, down_hbm,
    out_hbm,
    latent, query, memory, hidden, keys, tables, heads, scores, probs, top, attended, values, w_uv, w_out, kept,
    place, mix, rows, w_gate, w_up, w_down, act, mine, paired, give, arrived, produced,
    load_sem, far_send, far_recv, near_send, near_recv,
    key_send, key_recv, key_swap_send, key_swap_recv,
    row_send, row_recv, row_swap_send, row_swap_recv,
    ring_send, ring_recv, pair_send, pair_recv,
):
    f32, bf16 = jnp.float32, jnp.bfloat16
    chips = n // 2
    half_ring = chips // 2
    last = chips - 2
    count, width = kept.shape
    seqs, span_len = 2, count // 2
    lat_width = latent.shape[1]
    mem_len = memory.shape[0] // 2
    head_count = query.shape[1] // lat_width
    mem_at = n * span_len
    key_total = keys.shape[1]
    here = uv_hbm.shape[0]
    value_dim = uv_hbm.shape[2]
    half_here = here // 2
    slots = place.shape[1]
    me, core, device = ring_place(n)
    own_dp = lax.axis_index("dp")
    far_dp = 1 - own_dp
    partner = device(0, 1 - core)
    ahead = (device(1, core), device(-1, core))
    spans = (pl.ds(0, span_len), pl.ds(span_len, span_len))

    loads = [
        pltpu.make_async_copy(src, dst, load_sem.at[i])
        for i, (src, dst) in enumerate((
            (latent_hbm.reshape(count, lat_width), latent),
            (query_hbm.reshape(query.shape), query),
            (memory_hbm.reshape(memory.shape), memory),
            (uv_hbm, w_uv.at[pl.ds(own_dp * here, here)]),
            (hidden_hbm.reshape(count, width), hidden),
            (wout_hbm, w_out.at[pl.ds(own_dp * here * value_dim, here * value_dim)]),
            (gate_hbm, w_gate),
            (up_hbm, w_up),
            (down_hbm, w_down),
        ))
    ]
    for load in loads:
        load.start()
    waits = []

    def send(copy):
        copy.start()
        waits.append(copy)

    barrier = pltpu.get_barrier_semaphore()
    for target in (ahead[0], ahead[1], partner):
        pl.semaphore_signal(barrier, inc=1, device_id={"expert": target}, device_id_type=MESH)
    pl.semaphore_signal(barrier, inc=1, device_id={"dp": far_dp}, device_id_type=MESH)
    pl.semaphore_wait(barrier, 4)

    def uv_piece(owner, of_core):
        return pl.ds(owner * here + of_core * half_here, half_here)

    pieces = far_send.shape[0] - 1
    out_rows = half_here * value_dim // pieces

    def out_piece(owner, of_core, i):
        first = (owner * here + of_core * half_here) * value_dim + i * out_rows
        return pl.ds(pl.multiple_of(first, out_rows), out_rows)

    def across(src, dst, i):
        return pltpu.make_async_remote_copy(
            src_ref=src, dst_ref=dst, send_sem=far_send.at[i], recv_sem=far_recv.at[i],
            device_id={"dp": far_dp}, device_id_type=MESH,
        )

    send(across(uv_hbm.at[pl.ds(core * half_here, half_here)], w_uv.at[uv_piece(own_dp, core)], 0))
    for i in range(pieces):
        source = wout_hbm.at[pl.ds(pl.multiple_of(core * half_here * value_dim + i * out_rows, out_rows), out_rows)]
        send(across(source, w_out.at[out_piece(own_dp, core, i)], i + 1))

    def far_ref(i, of_core):
        return w_uv.at[uv_piece(far_dp, of_core)] if i == 0 else w_out.at[out_piece(far_dp, of_core, i - 1)]

    def pass_far(i):
        piece = far_ref(i, core)
        across(piece, piece, i).wait_recv()
        send(remote(piece, piece, near_send.at[i], near_recv.at[i], partner))

    def await_near(i):
        piece = far_ref(i, 1 - core)
        remote(piece, piece, near_send.at[i], near_recv.at[i], partner).wait_recv()

    def step_of(way, j):
        return (half_ring, way) if j == last else (j // 2 + 1, j % 2)

    def offset(way, dist):
        return dist if way == 0 else chips - dist

    def gather(parts, sends, recvs, swap_sends, swap_recvs):
        own = 2 * last + 2

        def start():
            for j in (0, 1):
                for way in (0, 1):
                    for i, ref in enumerate(parts(me, j)):
                        send(remote(ref, ref, sends.at[i, way, j], recvs.at[i, way, j], ahead[way]))
            for h in (0, 1):
                for i, ref in enumerate(parts(me, h)):
                    send(remote(ref, ref, swap_sends.at[i, own + h], swap_recvs.at[i, own + h], partner))

        def near_own():
            for h in (0, 1):
                for i, ref in enumerate(parts(partner, h)):
                    remote(ref, ref, swap_sends.at[i, own + h], swap_recvs.at[i, own + h], partner).wait_recv()

        def hop(j):
            onward = [j + 2, j + 2]
            if last - 2 <= j < last:
                onward = [last if j == last - 2 + way else None for way in (0, 1)]
            if j == last:
                onward = [None, None]
            for way in (0, 1):
                dist, h = step_of(way, j)
                for i, ref in enumerate(parts(device(-dist if way == 0 else dist, core), h)):
                    remote(ref, ref, sends.at[i, way, j], recvs.at[i, way, j], ahead[way]).wait_recv()
                    if onward[way] is not None:
                        k = onward[way]
                        send(remote(ref, ref, sends.at[i, way, k], recvs.at[i, way, k], ahead[way]))
                    k = 2 * j + way
                    send(remote(ref, ref, swap_sends.at[i, k], swap_recvs.at[i, k], partner))

        def near(j):
            for way in (0, 1):
                dist, h = step_of(way, j)
                k = 2 * j + way
                for i, ref in enumerate(parts(device(-dist if way == 0 else dist, 1 - core), h)):
                    remote(ref, ref, swap_sends.at[i, k], swap_recvs.at[i, k], partner).wait_recv()

        return start, near_own, hop, near

    def split_of(total):
        to = lax.broadcasted_iota(jnp.int32, (total, total), 0)
        at = lax.broadcasted_iota(jnp.int32, (total, total), 1)
        return (to == at % 2 * (total // 2) + at // 2).astype(f32).astype(bf16)

    split = split_of(count)
    to = lax.broadcasted_iota(jnp.int32, (count, count), 0)
    at = lax.broadcasted_iota(jnp.int32, (count, count), 1)
    weave = (at == to % 2 * span_len + to // 2).astype(f32).astype(bf16)

    def place_of(slot):
        return pl.ds(pl.multiple_of(slot * span_len, span_len), span_len)

    def key_parts(slot, h):
        return [keys.at[h, place_of(slot)]] + ([tables.at[slot]] if h == 0 else [])

    key_start, key_near_own, key_hop, key_near = gather(key_parts, key_send, key_recv, key_swap_send, key_swap_recv)
    tables[me] = jnp.dot(table_ref[...], split, preferred_element_type=f32).astype(bf16)
    loads[0].wait()
    parted = jnp.dot(split, latent[...], preferred_element_type=f32).astype(bf16)
    for s in range(seqs):
        keys[s, place_of(me)] = parted[s * span_len : (s + 1) * span_len]
    key_start()

    loads[1].wait()
    for s in range(seqs):
        parted = jnp.dot(
            split[s * span_len : (s + 1) * span_len], query[...], preferred_element_type=f32
        ).astype(bf16)
        for h in range(head_count):
            heads[s, pl.ds(h * span_len, span_len)] = parted[:, h * lat_width : (h + 1) * lat_width]
    loads[2].wait()
    parted = jnp.dot(split_of(2 * mem_len), memory[...], preferred_element_type=f32).astype(bf16)
    lanes = 2 * span_len
    row_count = head_count * span_len
    own_pos = me * span_len + lax.broadcasted_iota(jnp.int32, (row_count, lanes), 0) % span_len
    lane = lax.broadcasted_iota(jnp.int32, (row_count, lanes), 1)
    along = (((1,), (1,)), ((), ()))
    for s in range(seqs):
        keys[s, pl.ds(mem_at, mem_len)] = parted[s * mem_len : (s + 1) * mem_len]
        keys[s, pl.ds(mem_at + mem_len, key_total - mem_at - mem_len)] = jnp.zeros(
            (key_total - mem_at - mem_len, lat_width), bf16
        )
        score = lax.dot_general(heads[s], keys[s, pl.ds(mem_at, lanes)], along, preferred_element_type=f32)
        score = jnp.where(lane < mem_len, score, -jnp.inf)
        scores[s, :, pl.ds(mem_at, lanes)] = score
        top[s] = score

    def score_chip(k):
        first = pl.multiple_of(device(k, 0) * span_len, lanes)
        for s in range(seqs):
            score = lax.dot_general(heads[s], keys[s, pl.ds(first, lanes)], along, preferred_element_type=f32)
            pos = first + lane
            visible = (pos <= own_pos) & (pos < limit_ref[pl.ds(s, 1)])
            score = jnp.where(visible, score, -jnp.inf)
            scores[s, :, pl.ds(first, lanes)] = score
            top[s] = jnp.maximum(top[s], score)

    tasks = [key_near_own, functools.partial(score_chip, 0)]
    for j in range(last + 1):
        key_hop(j)
        for task in tasks:
            task()
        tasks = [functools.partial(key_near, j)]
        if j == 3:
            loads[3].wait()
            pass_far(0)
        if j % 2 == 1 or j == last:
            dist = step_of(0, j)[0]
            ks = [half_ring] if j == last else [dist, chips - dist]
            tasks += [functools.partial(score_chip, k) for k in ks]
    for task in tasks:
        task()
    pass_far(1)

    scale = score_scale * 1.4426950408889634
    block = 64

    for s in range(seqs):
        top[s, :, pl.ds(0, 1)] = jnp.max(top[s], axis=1, keepdims=True)

        def soften(i, carry, s=s):
            part = pl.ds(pl.multiple_of(i * block, block), block)
            shifted = (scores[s, part] - top[s, part, pl.ds(0, 1)]) * scale
            weight = jnp.exp2(shifted)
            probs[part] = weight.astype(bf16)
            top[s, part, pl.ds(0, 1)] = 1.0 / jnp.sum(weight, axis=1, keepdims=True)
            return carry

        lax.fori_loop(0, row_count // block, soften, 0)
        blend = jnp.dot(probs[...], keys[s], preferred_element_type=f32)
        attended[s] = (blend * top[s, :, pl.ds(0, 1)]).astype(bf16)
        if s == 0:
            pass_far(2)
    await_near(0)
    for h in range(head_count):
        part = pl.ds(h * span_len, span_len)
        both = jnp.concatenate([attended[0, part], attended[1, part]], axis=0)
        values[:, pl.ds(h * value_dim, value_dim)] = jnp.dot(
            both, w_uv[h], preferred_element_type=f32
        ).astype(bf16)
    woven = jnp.dot(weave, values[...], preferred_element_type=f32).astype(bf16)
    values[...] = woven
    loads[4].wait()
    loads[5].wait()
    depth = here * value_dim
    near_cols = pl.ds(pl.multiple_of(own_dp * depth, depth), depth)
    far_cols = pl.ds(pl.multiple_of(far_dp * depth, depth), depth)
    kept[...] = hidden[...].astype(f32) + jnp.dot(values[:, near_cols], w_out[near_cols], preferred_element_type=f32)
    for i in range(3, pieces + 1):
        pass_far(i)
    for i in range(1, pieces + 1):
        await_near(i)
    residual = kept[...] + jnp.dot(values[:, far_cols], w_out[far_cols], preferred_element_type=f32)
    kept[...] = residual
    mean_square = jnp.mean(residual * residual, axis=1, keepdims=True)
    rows[me] = (residual * lax.rsqrt(mean_square + norm_eps) * gain_ref[...].astype(f32)).astype(bf16)

    def row_parts(slot, h):
        return [rows.at[slot, spans[h]]]

    row_start, row_near_own, row_hop, row_near = gather(row_parts, row_send, row_recv, row_swap_send, row_swap_recv)
    row_start()

    hits, gates = [], []
    own_id = me.astype(f32)
    for c in range(chips):
        pair = jnp.concatenate([tables[2 * c], tables[2 * c + 1]], axis=1).astype(f32)
        matches = pair[:8] == own_id
        hits.append(jnp.max(jnp.where(matches, 1.0, 0.0), axis=0, keepdims=True))
        gates.append(jnp.sum(jnp.where(matches, pair[8:], 0.0), axis=0, keepdims=True))
    hits = jnp.concatenate(hits, axis=0)
    to = lax.broadcasted_iota(jnp.int32, (2 * count, 2 * count), 0)
    at = lax.broadcasted_iota(jnp.int32, (2 * count, 2 * count), 1)
    earlier = (to < at).astype(f32).astype(bf16)
    ranks = jnp.dot(hits.astype(bf16), earlier, preferred_element_type=f32)
    ranks = jnp.where(hits > 0.5, ranks, -1.0)
    slot_id = lax.broadcasted_iota(jnp.int32, (slots, 2 * count), 0).astype(f32)
    for c in range(chips):
        chosen = slot_id == ranks[c : c + 1]
        place[c] = jnp.where(chosen, 1.0, 0.0).astype(bf16)
        weighed = jnp.where(chosen, gates[c], 0.0).astype(bf16)
        mix[2 * c] = weighed[:, :count]
        mix[2 * c + 1] = weighed[:, count:]

    def start_experts(ks):
        picked = []
        for k in ks:
            first = device(k, 0)
            held = rows[pl.ds(first, 2)].reshape(2 * count, width)
            picked.append(jnp.dot(place[first // 2], held, preferred_element_type=f32).astype(bf16))
        picked = picked[0] if len(ks) == 1 else jnp.concatenate(picked, axis=0)
        gate_h = lax.dot_general(picked, w_gate[...], along, preferred_element_type=f32)
        up_h = lax.dot_general(picked, w_up[...], along, preferred_element_type=f32)
        act[pl.ds(0, len(ks) * slots)] = (gate_h / (1.0 + jnp.exp(-gate_h)) * up_h).astype(bf16)

    shares = {}
    down = (((0,), (0,)), ((), ()))

    def end_experts(ks):
        made = jnp.dot(act[pl.ds(0, len(ks) * slots)], w_down[...], preferred_element_type=f32).astype(bf16)
        for i, k in enumerate(ks):
            part = made[i * slots : (i + 1) * slots]
            give[k] = lax.dot_general(mix[device(k, 1 - core)], part, down, preferred_element_type=f32).astype(bf16)
            shares[k] = remote(give.at[k], paired.at[k], pair_send.at[k], pair_recv.at[k], partner)
            send(shares[k])
            mine[k] = lax.dot_general(mix[device(k, core)], part, down, preferred_element_type=f32).astype(bf16)

    seen = set()

    def bring(k):
        if k not in seen:
            seen.add(k)
            shares[k].wait_recv()

    def index_of(dist, h):
        return 0 if dist == half_ring else 1 + 2 * (half_ring - 1 - dist) + h

    def await_ring(way, j):
        piece = arrived.at[way, j]
        remote(piece, piece, ring_send.at[way, j], ring_recv.at[way, j], ahead[way]).wait_recv()

    def advance(dist, chain):
        for way in (0, 1):
            h = way if chain == 0 else 1 - way
            k = offset(way, dist)
            bring(k)
            total = mine[k, spans[h]].astype(f32) + paired[k, spans[h]].astype(f32)
            if dist < half_ring - chain:
                j = index_of(dist + 1, h)
                await_ring(way, j)
                total = total + arrived[way, j].astype(f32)
            mine[k, spans[h]] = total.astype(bf16)
            j = index_of(dist, h)
            send(remote(
                mine.at[k, spans[h]], arrived.at[way, j],
                ring_send.at[way, j], ring_recv.at[way, j], ahead[way],
            ))

    row_near_own()
    for load in loads[6:]:
        load.wait()
    start_experts([0])
    end_experts([0])

    tasks = []
    for j in range(last + 1):
        row_hop(j)
        if j % 2 == 1 or j == last:
            for i in (j - 1, j) if j % 2 == 1 else (j,):
                row_near(i)
            dist = step_of(0, j)[0]
            ks = [half_ring] if j == last else [dist, chips - dist]
            tasks += [functools.partial(start_experts, ks), functools.partial(end_experts, ks)]
        for _ in range(min(len(tasks), 1 if j < last - 1 else len(tasks))):
            tasks.pop(0)()
        if j == last - 1:
            advance(half_ring - 1, 1)

    advance(half_ring, 0)
    for dist in range(half_ring - 2, 0, -1):
        advance(dist, 1)
        advance(dist + 1, 0)
    advance(1, 0)

    bring(0)
    for h in (0, 1):
        total = mine[0, spans[h]].astype(f32) + paired[0, spans[h]].astype(f32)
        for way in (0, 1):
            j = index_of(1, h)
            await_ring(way, j)
            total = total + arrived[way, j].astype(f32)
        produced[spans[h]] = (kept[spans[h]] + total).astype(bf16)
    store = pltpu.make_async_copy(produced, out_hbm.reshape(count, width), load_sem.at[0])
    store.start()
    store.wait()
    for copy in waits:
        copy.wait_send()


def fused_layer(
    table, limits, gain, latents, queries, memory, hidden, w_uv, w_out, w_gate_t, w_up_t, w_down, n, slots, collective_id
):
    span_len, seqs, width = hidden.shape
    count = span_len * seqs
    lat_width = latents.shape[2]
    head_count = queries.shape[2] // lat_width
    here, _, value_dim = w_uv.shape
    mem_len = memory.shape[0]
    chips = n // 2
    steps = chips - 1
    inner = w_down.shape[0]
    key_total = n * span_len + count
    bf16, f32 = jnp.bfloat16, jnp.float32
    dma, vmem = pltpu.SemaphoreType.DMA, pltpu.VMEM
    row_count = head_count * span_len
    pieces = 4
    return pl.pallas_call(
        functools.partial(layer_kernel, n),
        out_shape=jax.ShapeDtypeStruct((span_len, seqs, width), bf16),
        in_specs=[pl.BlockSpec(memory_space=pltpu.VMEM)] * 3 + [pl.BlockSpec(memory_space=pl.ANY)] * 9,
        out_specs=pl.BlockSpec(memory_space=pl.ANY),
        scratch_shapes=[
            vmem((count, lat_width), bf16),
            vmem((count, head_count * lat_width), bf16),
            vmem((seqs * mem_len, lat_width), bf16),
            vmem((count, width), bf16),
            vmem((seqs, key_total, lat_width), bf16),
            vmem((n, 16, count), bf16),
            vmem((seqs, row_count, lat_width), bf16),
            vmem((seqs, row_count, key_total), f32),
            vmem((row_count, key_total), bf16),
            vmem((seqs, row_count, count), f32),
            vmem((seqs, row_count, lat_width), bf16),
            vmem((count, head_count * value_dim), bf16),
            vmem((head_count, lat_width, value_dim), bf16),
            vmem((head_count * value_dim, width), bf16),
            vmem((count, width), f32),
            vmem((chips, slots, 2 * count), bf16),
            vmem((n, slots, count), bf16),
            vmem((n, count, width), bf16),
            vmem((inner, width), bf16),
            vmem((inner, width), bf16),
            vmem((inner, width), bf16),
            vmem((2 * slots, inner), bf16),
            vmem((chips, count, width), bf16),
            vmem((chips, count, width), bf16),
            vmem((chips, count, width), bf16),
            vmem((2, steps, count // 2, width), bf16),
            vmem((count, width), bf16),
            dma((9,)),
            dma((pieces + 1,)),
            dma((pieces + 1,)),
            dma((pieces + 1,)),
            dma((pieces + 1,)),
            dma((2, 2, steps)),
            dma((2, 2, steps)),
            dma((2, 2 * steps + 2)),
            dma((2, 2 * steps + 2)),
            dma((1, 2, steps)),
            dma((1, 2, steps)),
            dma((1, 2 * steps + 2)),
            dma((1, 2 * steps + 2)),
            dma((2, steps)),
            dma((2, steps)),
            dma((chips,)),
            dma((chips,)),
        ],
        compiler_params=pltpu.CompilerParams(
            collective_id=collective_id, has_side_effects=True, vmem_limit_bytes=67000000
        ),
        cost_estimate=pl.CostEstimate(
            flops=6 * chips * slots * width * inner, bytes_accessed=32 * n * count * width, transcendentals=0
        ),
        name="layer_%d" % collective_id,
    )(table, limits, gain, latents, queries, memory, hidden, w_uv, w_out, w_gate_t, w_up_t, w_down)


def layer_bytes(n, count, width, inner, slots, lat_width, head_count, value_dim):
    chips = n // 2
    key_total = (n + 2) * count // 2
    row_count = head_count * count // 2
    front = count * (1 + head_count) * lat_width + 2 * key_total * lat_width + 4 * row_count * lat_width
    front += 5 * row_count * key_total + 4 * row_count * count + head_count * value_dim * (lat_width + width + count)
    back = n * count * width + 3 * width * inner + (4 * chips - 1) * count * width + 5 * count * width
    back += 4 * chips * slots * count + 2 * slots * inner
    return 2 * (front + back) + 8 * slots * inner * 2


def shards(
    hidden,
    queries,
    latents,
    mem_latents,
    lengths,
    ids,
    gates,
    norm_gain,
    w_uv,
    w_out,
    w_gate,
    w_up,
    w_down,
):
    f32, bf16 = jnp.float32, jnp.bfloat16
    local_len, seq_count, model_width = hidden.shape[1:]
    latent_dim = latents.shape[3]
    head_count = queries.shape[3] // latent_dim
    row_count = local_len * seq_count
    n = lax.axis_size("expert")
    dp_size = lax.axis_size("dp")
    me = lax.axis_index("expert")
    core = me % 2
    own_dp = lax.axis_index("dp")
    heads_here, _, value_dim = w_uv.shape
    top_count = ids.shape[3]
    ids_t = jnp.transpose(ids[0], (2, 1, 0)).reshape(top_count, row_count).astype(bf16)
    gates_t = jnp.transpose(gates[0], (2, 1, 0)).reshape(top_count, row_count)
    capacity = min(row_count, row_count * top_count // (n * w_gate.shape[0]) + 2)
    slots = -(-2 * capacity // 128) * 128
    fits = (
        dp_size == 2
        and w_gate.shape[0] == 1
        and n >= 8
        and top_count <= 8
        and seq_count == 2
        and row_count % 128 == 0
        and heads_here % 2 == 0
        and mem_latents.shape[1] <= row_count
        and layer_bytes(n, row_count, model_width, w_down.shape[1], slots, latent_dim, head_count, value_dim)
        < 60 * 1024 * 1024
    )
    if fits:
        pad = ((0, 8 - top_count), (0, 0))
        table = jnp.concatenate(
            [jnp.pad(ids_t, pad, constant_values=255), jnp.pad(gates_t, pad)], axis=0
        )
        out = fused_layer(
            table, jnp.broadcast_to(lengths[0][:, None], (seq_count, row_count)), norm_gain[None],
            latents[0], queries[0], mem_latents[0], hidden[0], w_uv, w_out,
            jnp.transpose(w_gate[0]), jnp.transpose(w_up[0]), w_down[0], n, slots, 4,
        )
        return out[None]

    half_heads = heads_here // 2
    uv_half = lax.dynamic_slice_in_dim(w_uv, core * half_heads, half_heads, 0)
    out_half = lax.dynamic_slice_in_dim(
        w_out, core * half_heads * value_dim, half_heads * value_dim, 0
    )
    uv_groups, out_groups, starts = [w_uv], [w_out], [own_dp * heads_here]
    swap = [(i, i ^ 1) for i in range(n)]
    sizes = [heads_here]
    for shift in range(1, dp_size):
        turn = [(i, (i + shift) % dp_size) for i in range(dp_size)]
        source = (own_dp - shift + dp_size) % dp_size
        uv_far = lax.ppermute(uv_half, "dp", turn)
        out_far = lax.ppermute(out_half, "dp", turn)
        uv_near = lax.ppermute(uv_far, "expert", swap)
        out_near = lax.ppermute(out_far, "expert", swap)
        uv_groups += [uv_far, uv_near]
        out_groups += [out_far, out_near]
        starts += [
            source * heads_here + core * half_heads,
            source * heads_here + (1 - core) * half_heads,
        ]
        sizes += [half_heads, half_heads]

    latent_rows = jnp.transpose(latents[0], (1, 0, 2)).reshape(row_count, latent_dim)
    table = jnp.concatenate([ids_t, gates_t], axis=0).reshape(-1)
    table_rows = -(-table.shape[0] // (16 * latent_dim)) * 16
    table = jnp.pad(table, (0, table_rows * latent_dim - table.shape[0]))
    packed = jnp.concatenate([latent_rows, table.reshape(table_rows, latent_dim)], axis=0)
    all_rows = row_count + table_rows
    cut = (all_rows // 2 + 15) // 16 * 16
    gathered = ring_gather(packed, n, cut, 0)

    segment = gathered[:, :row_count].reshape(n, seq_count, local_len, latent_dim)
    segment = jnp.transpose(segment, (1, 0, 2, 3)).reshape(seq_count, n * local_len, latent_dim)
    memory = jnp.transpose(mem_latents[0], (1, 0, 2))
    mem_count = memory.shape[1]
    keys = jnp.concatenate([memory, segment], axis=1)
    query_rows = jnp.transpose(
        queries[0].reshape(local_len, seq_count, head_count, latent_dim), (1, 2, 0, 3)
    ).reshape(seq_count, head_count * local_len, latent_dim)
    scores = jnp.einsum("sql,sjl->sqj", query_rows, keys, preferred_element_type=f32) * score_scale
    key_pos = lax.broadcasted_iota(jnp.int32, scores.shape, 2) - mem_count
    own_pos = me * local_len + lax.broadcasted_iota(jnp.int32, scores.shape, 1) % local_len
    visible = (key_pos <= own_pos) & (key_pos < lengths[0][:, None, None])
    scores = jnp.where(visible | (key_pos < 0), scores, -jnp.inf)
    weights = jnp.exp(scores - jnp.max(scores, axis=2, keepdims=True))
    total = jnp.sum(weights, axis=2, keepdims=True)
    attended = jnp.einsum("sqj,sjl->sql", weights.astype(bf16), keys, preferred_element_type=f32)
    attended = (attended / total).astype(bf16)
    attended = attended.reshape(seq_count, head_count, local_len, latent_dim)

    attn_out = jnp.zeros((row_count, model_width), f32)
    for uv, out, start, size in zip(uv_groups, out_groups, starts, sizes):
        heads = lax.dynamic_slice_in_dim(attended, start, size, 1)
        values = jnp.einsum("shtl,hlv->sthv", heads, uv, preferred_element_type=f32).astype(bf16)
        attn_out = attn_out + jnp.dot(
            values.reshape(row_count, size * value_dim), out, preferred_element_type=f32
        )

    hidden_rows = jnp.transpose(hidden[0], (1, 0, 2)).reshape(row_count, model_width)
    residual = lax.optimization_barrier(hidden_rows).astype(f32) + attn_out
    mean_square = jnp.mean(residual * residual, axis=-1, keepdims=True)
    normed = (residual * lax.rsqrt(mean_square + norm_eps) * norm_gain.astype(f32)).astype(bf16)

    rows_all = ring_gather(normed, n, row_count // 2, 1)
    experts_here = w_gate.shape[0]
    expert_count = n * experts_here
    groups = n // 2
    wide = 2 * row_count
    slots = -(-2 * capacity // 16) * 16
    tables = gathered[:, row_count:].reshape(n, -1)[:, : 2 * top_count * row_count]
    tables = tables.reshape(groups, 2, 2, top_count, row_count)
    named = jnp.transpose(tables[:, :, 0], (2, 0, 1, 3)).reshape(top_count, groups, wide)
    scale = jnp.transpose(tables[:, :, 1], (2, 0, 1, 3)).reshape(top_count, groups, wide)
    rows_all = rows_all.reshape(groups, wide, model_width)
    steps = jnp.arange(wide, dtype=jnp.int32)
    earlier = (steps[:, None] < steps[None, :]).astype(bf16)
    made_rows, mixes = [], []
    for e in range(experts_here):
        matches = named == (me * experts_here + e).astype(bf16)
        hit = jnp.any(matches, axis=0)
        gate = jnp.sum(jnp.where(matches, scale.astype(f32), 0.0), axis=0)
        slot = jnp.dot(hit.astype(bf16), earlier, preferred_element_type=f32).astype(jnp.int32)
        slot = jnp.where(hit, slot, -1)
        chosen = slot[:, None, :] == jnp.arange(slots, dtype=jnp.int32)[None, :, None]
        placing = chosen.astype(bf16)
        slot_t = jnp.where(hit, slot, -1).reshape(n, row_count)
        chosen_t = slot_t[:, :, None] == jnp.arange(slots, dtype=jnp.int32)[None, None, :]
        mixes.append(jnp.where(chosen_t, gate.reshape(n, row_count)[:, :, None], 0.0).astype(bf16))
        picked = jnp.einsum("gct,gtd->gcd", placing, rows_all, preferred_element_type=f32)
        picked = picked.astype(bf16).reshape(groups * slots, model_width)
        gate_h = jnp.dot(picked, w_gate[e], preferred_element_type=f32)
        up_h = jnp.dot(picked, w_up[e], preferred_element_type=f32)
        act = (jax.nn.silu(gate_h) * up_h).astype(bf16)
        produced = jnp.dot(act, w_down[e], preferred_element_type=f32).astype(bf16)
        made_rows.append(produced.reshape(groups, slots, model_width))
    made_rows = made_rows[0] if experts_here == 1 else jnp.concatenate(made_rows, axis=1)
    mixing = mixes[0] if experts_here == 1 else jnp.concatenate(mixes, axis=2)
    routed = ring_reduce(made_rows, mixing, n, 2)
    layer_out = (residual + routed).astype(bf16).reshape(seq_count, local_len, model_width)
    return jnp.transpose(layer_out, (1, 0, 2))[None]


def solution(mesh):
    return jax.shard_map(
        shards,
        mesh=mesh,
        in_specs=(
            P("dp", "expert", None, None),
            P("dp", "expert", None, None),
            P("dp", "expert", None, None),
            P("dp", None, None, None),
            P("dp", None),
            P("dp", "expert", None, None),
            P("dp", "expert", None, None),
            P(),
            P("dp", None, None),
            P("dp", None),
            P("expert", None, None),
            P("expert", None, None),
            P("expert", None, None),
        ),
        out_specs=P("dp", "expert", None, None),
        check_vma=False,
    )
```

```python
import functools

import jax
import jax.numpy as jnp
from jax import lax
from jax.experimental import pallas as pl
from jax.experimental.pallas import tpu as pltpu
from jax.sharding import PartitionSpec as P

score_scale = 192.0 ** (-0.5)
norm_eps = 1e-06
MESH = pl.DeviceIdType.MESH


def ring_place(n):
    chips = n // 2
    depth = chips // 2
    me = lax.axis_index("expert")
    core = me % 2
    chip = me // 2
    row, col = chip // 2, chip % 2
    pos = col * row + (1 - col) * (chips - 1 - row)

    def device(offset, core_of):
        p = (pos + offset + chips) % chips
        q = p // depth
        r = (1 - q) * p + q * (chips - 1 - p)
        return (2 * r + 1 - q) * 2 + core_of

    return me, core, device


def greet(targets):
    barrier = pltpu.get_barrier_semaphore()
    for target in targets:
        pl.semaphore_signal(barrier, inc=1, device_id={"expert": target}, device_id_type=MESH)
    pl.semaphore_wait(barrier, len(targets))


def remote(src, dst, send_sem, recv_sem, target):
    return pltpu.make_async_remote_copy(
        src_ref=src,
        dst_ref=dst,
        send_sem=send_sem,
        recv_sem=recv_sem,
        device_id={"expert": target},
        device_id_type=MESH,
    )


def gather_kernel(n, cut, x_ref, out_ref, ring_send, ring_recv, pair_send, pair_recv, own_sem):
    chips = n // 2
    half_ring = chips // 2
    rows = x_ref.shape[0]
    last = chips - 2
    me, core, device = ring_place(n)
    partner = device(0, 1 - core)
    ahead = (device(1, core), device(-1, core))
    spans = (pl.ds(0, cut), pl.ds(cut, rows - cut))
    greet((ahead[0], ahead[1], partner))

    def arrival(way, j):
        dist, half = (half_ring, way) if j == last else (j // 2 + 1, j % 2)
        return device(-dist if way == 0 else dist, core), spans[half]

    waits = []
    for way in (0, 1):
        for j in (0, 1):
            if j > last:
                continue
            if j == last and half_ring == 1:
                span = spans[way]
            else:
                span = spans[j]
            copy = remote(
                x_ref.at[span], out_ref.at[me, span],
                ring_send.at[way, j], ring_recv.at[way, j], ahead[way],
            )
            copy.start()
            waits.append(copy)
    share = remote(x_ref, out_ref.at[me], pair_send.at[2 * last + 2], pair_recv.at[2 * last + 2], partner)
    share.start()
    waits.append(share)
    keep = pltpu.make_async_copy(x_ref, out_ref.at[me], own_sem)
    keep.start()

    for j in range(last + 1):
        for way in (0, 1):
            slot, span = arrival(way, j)
            piece = out_ref.at[slot, span]
            remote(piece, piece, ring_send.at[way, j], ring_recv.at[way, j], ahead[way]).wait_recv()
            onward = j + 2
            if j >= last - 2 and j < last:
                onward = last if j == last - 2 + way else None
            if j == last:
                onward = None
            if onward is not None:
                copy = remote(piece, piece, ring_send.at[way, onward], ring_recv.at[way, onward], ahead[way])
                copy.start()
                waits.append(copy)
            index = 2 * j + way
            copy = remote(piece, piece, pair_send.at[index], pair_recv.at[index], partner)
            copy.start()
            waits.append(copy)

    for j in range(last + 1):
        for way in (0, 1):
            dist, half = (half_ring, way) if j == last else (j // 2 + 1, j % 2)
            slot = device(-dist if way == 0 else dist, 1 - core)
            piece = out_ref.at[slot, spans[half]]
            index = 2 * j + way
            remote(piece, piece, pair_send.at[index], pair_recv.at[index], partner).wait_recv()
    other = out_ref.at[partner]
    remote(other, other, pair_send.at[2 * last + 2], pair_recv.at[2 * last + 2], partner).wait_recv()
    for copy in waits:
        copy.wait_send()
    keep.wait()


def ring_gather(x, n, cut, collective_id):
    rows, cols = x.shape
    steps = n // 2 - 1
    return pl.pallas_call(
        functools.partial(gather_kernel, n, cut),
        out_shape=jax.ShapeDtypeStruct((n, rows, cols), x.dtype),
        in_specs=[pl.BlockSpec(memory_space=pltpu.VMEM)],
        out_specs=pl.BlockSpec(memory_space=pl.ANY),
        scratch_shapes=[
            pltpu.SemaphoreType.DMA((2, steps)),
            pltpu.SemaphoreType.DMA((2, steps)),
            pltpu.SemaphoreType.DMA((2 * steps + 1,)),
            pltpu.SemaphoreType.DMA((2 * steps + 1,)),
            pltpu.SemaphoreType.DMA,
        ],
        compiler_params=pltpu.CompilerParams(collective_id=collective_id, has_side_effects=True),
        cost_estimate=pl.CostEstimate(flops=0, bytes_accessed=16 * n * rows * cols, transcendentals=0),
        name="ring_gather_%d" % collective_id,
    )(x)


def reduce_kernel(
    n, rows_ref, mix_ref, out_ref, mine, paired, give, arrived, ring_send, ring_recv, pair_send, pair_recv
):
    chips = n // 2
    half_ring = chips // 2
    half = mine.shape[1] // 2
    last = chips - 2
    me, core, device = ring_place(n)
    partner = device(0, 1 - core)
    ahead = (device(1, core), device(-1, core))
    greet((ahead[0], ahead[1], partner))

    order = [half_ring]
    for k in range(half_ring - 1, 0, -1):
        order += [k, chips - k]
    order.append(0)
    depth = give.shape[0]
    shares, made, seen = {}, [], set()

    def weigh(k, core_of):
        dest = device(k, core_of)
        return jnp.dot(
            mix_ref[dest], rows_ref[dest // 2], preferred_element_type=jnp.float32
        ).astype(mine.dtype)

    def make():
        k = order[len(made)]
        slot = len(made) % depth
        if len(made) >= depth:
            shares[order[len(made) - depth]].wait_send()
        give[slot] = weigh(k, 1 - core)
        shares[k] = remote(give.at[slot], paired.at[k], pair_send.at[k], pair_recv.at[k], partner)
        shares[k].start()
        mine[k] = weigh(k, core)
        made.append(k)

    def bring(k):
        while k not in made or (len(made) < chips and len(made) < order.index(k) + 3):
            make()
        if k not in seen:
            seen.add(k)
            shares[k].wait_recv()

    def index_of(dist, h):
        return 0 if dist == half_ring else 1 + 2 * (half_ring - 1 - dist) + h

    def await_ring(way, j):
        piece = arrived.at[way, j]
        remote(piece, piece, ring_send.at[way, j], ring_recv.at[way, j], ahead[way]).wait_recv()

    sends = []
    for dist in range(half_ring, 0, -1):
        for turn in (0, 1):
            for way in (0, 1):
                if dist == half_ring:
                    if turn == 1:
                        continue
                    h = way
                elif dist == half_ring - 1:
                    h = 1 - way if turn == 0 else way
                else:
                    h = turn
                k = dist if way == 0 else chips - dist
                bring(k)
                span = pl.ds(h * half, half)
                total = mine[k, span].astype(jnp.float32) + paired[k, span].astype(jnp.float32)
                has_prior = dist < half_ring - 1 or (dist == half_ring - 1 and h == way)
                if has_prior:
                    j = index_of(dist + 1, h)
                    await_ring(way, j)
                    total = total + arrived[way, j].astype(jnp.float32)
                mine[k, span] = total.astype(mine.dtype)
                j = index_of(dist, h)
                copy = remote(
                    mine.at[k, span], arrived.at[way, j],
                    ring_send.at[way, j], ring_recv.at[way, j], ahead[way],
                )
                copy.start()
                sends.append(copy)
    bring(0)
    for h in (0, 1):
        span = pl.ds(h * half, half)
        total = mine[0, span].astype(jnp.float32) + paired[0, span].astype(jnp.float32)
        for way in (0, 1):
            j = index_of(1, h)
            await_ring(way, j)
            total = total + arrived[way, j].astype(jnp.float32)
        out_ref[span] = total
    for copy in sends:
        copy.wait_send()
    for k in order[chips - min(depth, chips) :]:
        shares[k].wait_send()


def ring_reduce(rows_in, mix, n, collective_id):
    rows = mix.shape[1]
    cols = rows_in.shape[2]
    chips = n // 2
    dtype = rows_in.dtype
    return pl.pallas_call(
        functools.partial(reduce_kernel, n),
        out_shape=jax.ShapeDtypeStruct((rows, cols), jnp.float32),
        in_specs=[pl.BlockSpec(memory_space=pltpu.VMEM)] * 2,
        out_specs=pl.BlockSpec(memory_space=pltpu.VMEM),
        scratch_shapes=[
            pltpu.VMEM((chips, rows, cols), dtype),
            pltpu.VMEM((chips, rows, cols), dtype),
            pltpu.VMEM((min(4, chips), rows, cols), dtype),
            pltpu.VMEM((2, chips - 1, rows // 2, cols), dtype),
            pltpu.SemaphoreType.DMA((2, chips - 1)),
            pltpu.SemaphoreType.DMA((2, chips - 1)),
            pltpu.SemaphoreType.DMA((chips,)),
            pltpu.SemaphoreType.DMA((chips,)),
        ],
        compiler_params=pltpu.CompilerParams(
            collective_id=collective_id, has_side_effects=True, vmem_limit_bytes=62 * 1024 * 1024
        ),
        cost_estimate=pl.CostEstimate(
            flops=2 * mix.size * cols, bytes_accessed=16 * n * rows * cols, transcendentals=0
        ),
        name="ring_reduce_%d" % collective_id,
    )(rows_in, mix)


def layer_kernel(
    n,
    ids_hbm, gates_hbm, limit_hbm, gain_hbm,
    latent_hbm, query_hbm, memory_hbm, hidden_hbm, uv_hbm, wout_hbm, gate_hbm, up_hbm, down_hbm,
    out_hbm,
    ids, gates, limit, gain,
    latent, query, memory, hidden, parted_hidden, keys, tables, heads, bound, peak, mass, blend,
    attended, values, w_uv, w_out, kept,
    place, mix, rows, w_gate, w_up, w_down, act, mine, paired, give, arrived, produced,
    load_sem, far_send, far_recv, near_send, near_recv,
    key_send, key_recv, key_swap_send, key_swap_recv,
    row_send, row_recv, row_swap_send, row_swap_recv,
    round_send, round_recv, round_swap_send, round_swap_recv,
    ring_send, ring_recv, pair_send, pair_recv,
):
    f32, bf16 = jnp.float32, jnp.bfloat16
    chips = n // 2
    half_ring = chips // 2
    last = chips - 2
    count, width = kept.shape
    seqs, span_len = 2, count // 2
    lat_width = latent.shape[1]
    mem_len = memory.shape[0] // 2
    head_count = query.shape[1] // lat_width
    mem_at = n * span_len
    key_total = keys.shape[1]
    top_count = ids.shape[0]
    here = uv_hbm.shape[0]
    value_dim = uv_hbm.shape[2]
    half_here = here // 2
    slots = place.shape[1]
    me, core, device = ring_place(n)
    own_dp = lax.axis_index("dp")
    far_dp = 1 - own_dp
    partner = device(0, 1 - core)
    ahead = (device(1, core), device(-1, core))
    spans = (pl.ds(0, span_len), pl.ds(span_len, span_len))

    loads = [
        pltpu.make_async_copy(src, dst, load_sem.at[i])
        for i, (src, dst) in enumerate((
            (latent_hbm.reshape(count, lat_width), latent),
            (ids_hbm, ids),
            (gates_hbm, gates),
            (limit_hbm, limit),
            (gain_hbm, gain),
            (query_hbm.reshape(query.shape), query),
            (memory_hbm.reshape(memory.shape), memory),
            (uv_hbm, w_uv.at[pl.ds(own_dp * here, here)]),
            (hidden_hbm.reshape(count, width), hidden),
            (wout_hbm, w_out.at[pl.ds(own_dp * here * value_dim, here * value_dim)]),
            (gate_hbm, w_gate),
            (up_hbm, w_up),
            (down_hbm, w_down),
        ))
    ]
    for load in loads:
        load.start()
    waits = []

    def send(copy):
        copy.start()
        waits.append(copy)

    barrier = pltpu.get_barrier_semaphore()
    for target in (ahead[0], ahead[1], partner):
        pl.semaphore_signal(barrier, inc=1, device_id={"expert": target}, device_id_type=MESH)
    pl.semaphore_signal(barrier, inc=1, device_id={"dp": far_dp}, device_id_type=MESH)
    pl.semaphore_wait(barrier, 4)

    def uv_piece(owner, of_core):
        return pl.ds(owner * here + of_core * half_here, half_here)

    depth = here * value_dim
    round_rows = round_share(depth, n)
    pieces = far_send.shape[0] - 3
    out_rows = (depth - n * round_rows) // (2 * pieces)

    def out_piece(first, of_core, i):
        at = first + n * round_rows + (of_core * pieces + i) * out_rows
        return pl.ds(pl.multiple_of(at, 8), out_rows)

    def round_piece(first, slot, h):
        size = round_rows // 2
        return pl.ds(pl.multiple_of(first + slot * round_rows + h * size, 8), size)

    def across(src, dst, i):
        return pltpu.make_async_remote_copy(
            src_ref=src, dst_ref=dst, send_sem=far_send.at[i], recv_sem=far_recv.at[i],
            device_id={"dp": far_dp}, device_id_type=MESH,
        )

    for h in (0, 1):
        send(across(wout_hbm.at[round_piece(0, me, h)], w_out.at[round_piece(own_dp * depth, me, h)], pieces + 1 + h))
    send(across(uv_hbm.at[pl.ds(core * half_here, half_here)], w_uv.at[uv_piece(own_dp, core)], 0))
    for i in range(pieces):
        send(across(wout_hbm.at[out_piece(0, core, i)], w_out.at[out_piece(own_dp * depth, core, i)], i + 1))

    def far_ref(i, of_core):
        return w_uv.at[uv_piece(far_dp, of_core)] if i == 0 else w_out.at[out_piece(far_dp * depth, of_core, i - 1)]

    def pass_far(i):
        piece = far_ref(i, core)
        across(piece, piece, i).wait_recv()
        send(remote(piece, piece, near_send.at[i], near_recv.at[i], partner))

    def await_near(i):
        piece = far_ref(i, 1 - core)
        remote(piece, piece, near_send.at[i], near_recv.at[i], partner).wait_recv()

    def step_of(way, j):
        return (half_ring, way) if j == last else (j // 2 + 1, j % 2)

    def offset(way, dist):
        return dist if way == 0 else chips - dist

    def gather(parts, sends, recvs, swap_sends, swap_recvs):
        own = 2 * last + 2

        def start(h):
            for way in (0, 1):
                for i, ref in enumerate(parts(me, h)):
                    send(remote(ref, ref, sends.at[i, way, h], recvs.at[i, way, h], ahead[way]))
            for i, ref in enumerate(parts(me, h)):
                send(remote(ref, ref, swap_sends.at[i, own + h], swap_recvs.at[i, own + h], partner))

        def near_own():
            for h in (0, 1):
                for i, ref in enumerate(parts(partner, h)):
                    remote(ref, ref, swap_sends.at[i, own + h], swap_recvs.at[i, own + h], partner).wait_recv()

        def hop(j):
            onward = [j + 2, j + 2]
            if last - 2 <= j < last:
                onward = [last if j == last - 2 + way else None for way in (0, 1)]
            if j == last:
                onward = [None, None]
            for way in (0, 1):
                dist, h = step_of(way, j)
                for i, ref in enumerate(parts(device(-dist if way == 0 else dist, core), h)):
                    remote(ref, ref, sends.at[i, way, j], recvs.at[i, way, j], ahead[way]).wait_recv()
                    if onward[way] is not None:
                        k = onward[way]
                        send(remote(ref, ref, sends.at[i, way, k], recvs.at[i, way, k], ahead[way]))
                    k = 2 * j + way
                    send(remote(ref, ref, swap_sends.at[i, k], swap_recvs.at[i, k], partner))

        def near(j):
            for way in (0, 1):
                dist, h = step_of(way, j)
                k = 2 * j + way
                for i, ref in enumerate(parts(device(-dist if way == 0 else dist, 1 - core), h)):
                    remote(ref, ref, swap_sends.at[i, k], swap_recvs.at[i, k], partner).wait_recv()

        return start, near_own, hop, near

    def split_of(total):
        to = lax.broadcasted_iota(jnp.int32, (total, total), 0)
        at = lax.broadcasted_iota(jnp.int32, (total, total), 1)
        return (to == at % 2 * (total // 2) + at // 2).astype(f32).astype(bf16)

    split = split_of(count)
    to = lax.broadcasted_iota(jnp.int32, (count, count), 0)
    at = lax.broadcasted_iota(jnp.int32, (count, count), 1)
    weave = (at == to % 2 * span_len + to // 2).astype(f32).astype(bf16)

    def place_of(slot, first, size):
        return pl.ds(pl.multiple_of(slot * span_len + first, size), size)

    sub = span_len // 2

    def key_parts(slot, h):
        found = [keys.at[h, place_of(slot, i * sub, sub)] for i in (0, 1)]
        return found + ([tables.at[slot]] if h == 0 else [])

    key_start, key_near_own, key_hop, key_near = gather(key_parts, key_send, key_recv, key_swap_send, key_swap_recv)
    for load in loads[:5]:
        load.wait()
    lines = []
    for source, filler in ((ids, 255.0), (gates, 0.0)):
        taken = source[...].astype(f32)
        lines.append(jnp.concatenate([taken[:, s, :] for s in range(seqs)], axis=1))
        if top_count < 8:
            lines.append(jnp.full((8 - top_count, count), filler, f32))
    tables[me] = jnp.concatenate(lines, axis=0).astype(bf16)
    for s in range(seqs):
        keys[s, place_of(me, 0, span_len)] = jnp.dot(
            split[s * span_len : (s + 1) * span_len], latent[...], preferred_element_type=f32
        ).astype(bf16)
        key_start(s)

    loads[5].wait()
    for s in range(seqs):
        parted = jnp.dot(
            split[s * span_len : (s + 1) * span_len], query[...], preferred_element_type=f32
        ).astype(bf16)
        for h in range(head_count):
            heads[s, pl.ds(h * span_len, span_len)] = parted[:, h * lat_width : (h + 1) * lat_width]
    loads[6].wait()
    parted = jnp.dot(split_of(2 * mem_len), memory[...], preferred_element_type=f32).astype(bf16)
    lanes = 2 * span_len
    row_count = head_count * span_len
    lane = lax.broadcasted_iota(jnp.int32, (row_count, lanes), 1)
    own_pos = me * span_len + lax.broadcasted_iota(jnp.int32, (row_count, lanes), 0) % span_len
    along = (((1,), (1,)), ((), ()))
    scale = score_scale * 1.4426950408889634
    for s in range(seqs):
        keys[s, pl.ds(mem_at, mem_len)] = parted[s * mem_len : (s + 1) * mem_len]
        keys[s, pl.ds(mem_at + mem_len, key_total - mem_at - mem_len)] = jnp.zeros(
            (key_total - mem_at - mem_len, lat_width), bf16
        )
        bound[s] = jnp.minimum(own_pos, limit[:, s : s + 1] - 1) - lane

    def wide(x, times):
        return x if times == 1 else jnp.concatenate([x] * times, axis=1)

    def attend(ks, opening=False):
        firsts = [pl.multiple_of(device(k, 0) * span_len, lanes) for k in ks]
        for s in range(seqs):
            held = [keys[s, pl.ds(first, lanes)] for first in firsts]
            seen_keys = [first <= bound[s] for first in firsts]
            if opening:
                held.append(keys[s, pl.ds(mem_at, lanes)])
                seen_keys.append(lane < mem_len)
            held = held[0] if len(held) == 1 else jnp.concatenate(held, axis=0)
            score = lax.dot_general(heads[s], held, along, preferred_element_type=f32)
            parts = [
                jnp.where(visible, score[:, i * lanes : (i + 1) * lanes], -jnp.inf)
                for i, visible in enumerate(seen_keys)
            ]
            top = functools.reduce(jnp.maximum, parts)
            top = jnp.broadcast_to(jnp.max(top, axis=1, keepdims=True), top.shape)
            if not opening:
                before = peak[s]
                top = jnp.maximum(before, top)
                fade = jnp.exp2((before - top) * scale)
            parts = [jnp.exp2((part - top) * scale) for part in parts]
            added = functools.reduce(jnp.add, parts)
            mass[s] = added if opening else mass[s] * fade + added
            peak[s] = top
            weight = parts[0] if len(parts) == 1 else jnp.concatenate(parts, axis=1)
            more = jnp.dot(weight.astype(bf16), held, preferred_element_type=f32)
            blend[s] = more if opening else blend[s] * wide(fade, lat_width // lanes) + more

    def round_parts(slot, h):
        return [w_out.at[round_piece(far_dp * depth, slot, h)]]

    round_start, round_near_own, round_hop, round_near = gather(
        round_parts, round_send, round_recv, round_swap_send, round_swap_recv
    )
    rounds = list(range(last + 1))
    tasks = [key_near_own, functools.partial(attend, [0], True)]
    for j in range(last + 1):
        key_hop(j)
        while j >= 3 and rounds and rounds[0] < min(last, 2 * j - 4):
            round_hop(rounds.pop(0))
        for task in tasks:
            task()
        tasks = [functools.partial(key_near, j)]
        if j == 0:
            for h in (0, 1):
                piece = w_out.at[round_piece(far_dp * depth, me, h)]
                across(piece, piece, pieces + 1 + h).wait_recv()
                round_start(h)
        if j == 1:
            loads[8].wait()
            parted_hidden[...] = jnp.dot(split, hidden[...], preferred_element_type=f32).astype(bf16)
        if j == last - 2:
            loads[7].wait()
            pass_far(0)
        if j == last - 1:
            pass_far(1)
        if j % 2 == 1 or j == last:
            dist = step_of(0, j)[0]
            ks = [half_ring] if j == last else [dist, chips - dist]
            tasks.append(functools.partial(attend, ks))
    for task in tasks:
        task()
    for i in rounds:
        round_hop(i)

    def row_parts(slot, h):
        return [rows.at[slot, pl.ds(h * span_len + i * sub, sub)] for i in (0, 1)]

    row_start, row_near_own, row_hop, row_near = gather(row_parts, row_send, row_recv, row_swap_send, row_swap_recv)
    await_near(0)
    near_cols = pl.ds(pl.multiple_of(own_dp * depth, depth), depth)
    far_cols = pl.ds(pl.multiple_of(far_dp * depth, depth), depth)
    loads[9].wait()
    for s in range(seqs):
        total = jnp.sum(mass[s], axis=1, keepdims=True)
        attended[...] = (blend[s] / total).astype(bf16)
        for h in range(head_count):
            values[spans[s], pl.ds(h * value_dim, value_dim)] = jnp.dot(
                attended[pl.ds(h * span_len, span_len)], w_uv[h], preferred_element_type=f32
            ).astype(bf16)
        residual = parted_hidden[spans[s]].astype(f32) + jnp.dot(
            values[spans[s], near_cols], w_out[near_cols], preferred_element_type=f32
        )
        if s == 0:
            for i in range(2, pieces + 1):
                pass_far(i)
            round_near_own()
            for i in range(last + 1):
                round_near(i)
            for i in range(1, pieces + 1):
                await_near(i)
        residual = residual + jnp.dot(values[spans[s], far_cols], w_out[far_cols], preferred_element_type=f32)
        mean_square = jnp.mean(residual * residual, axis=1, keepdims=True)
        normed = residual * lax.rsqrt(mean_square + norm_eps) * gain[...].astype(f32)
        rows[me, spans[s]] = normed.astype(bf16)
        row_start(s)

    woven = jnp.dot(weave, values[...], preferred_element_type=f32).astype(bf16)
    kept[...] = (
        hidden[...].astype(f32)
        + jnp.dot(woven[:, :depth], w_out[pl.ds(0, depth)], preferred_element_type=f32)
        + jnp.dot(woven[:, depth:], w_out[pl.ds(depth, depth)], preferred_element_type=f32)
    )
    hits, scales = [], []
    own_id = me.astype(f32)
    for c in range(chips):
        pair = jnp.concatenate([tables[2 * c], tables[2 * c + 1]], axis=1).astype(f32)
        matches = pair[:8] == own_id
        hits.append(jnp.max(jnp.where(matches, 1.0, 0.0), axis=0, keepdims=True))
        scales.append(jnp.sum(jnp.where(matches, pair[8:], 0.0), axis=0, keepdims=True))
    hits = jnp.concatenate(hits, axis=0)
    to = lax.broadcasted_iota(jnp.int32, (2 * count, 2 * count), 0)
    at = lax.broadcasted_iota(jnp.int32, (2 * count, 2 * count), 1)
    earlier = (to < at).astype(f32).astype(bf16)
    ranks = jnp.dot(hits.astype(bf16), earlier, preferred_element_type=f32)
    ranks = jnp.where(hits > 0.5, ranks, -1.0)
    slot_id = lax.broadcasted_iota(jnp.int32, (slots, 2 * count), 0).astype(f32)
    for c in range(chips):
        chosen = slot_id == ranks[c : c + 1]
        place[c] = jnp.where(chosen, 1.0, 0.0).astype(bf16)
        weighed = jnp.where(chosen, scales[c], 0.0).astype(bf16)
        for i in (0, 1):
            own_part = weighed[:, i * count : (i + 1) * count]
            mix[2 * c + i] = jnp.dot(own_part, split, preferred_element_type=f32).astype(bf16)

    def start_experts(ks):
        picked = []
        for k in ks:
            first = device(k, 0)
            held = rows[pl.ds(first, 2)].reshape(2 * count, width)
            picked.append(jnp.dot(place[first // 2], held, preferred_element_type=f32).astype(bf16))
        picked = picked[0] if len(ks) == 1 else jnp.concatenate(picked, axis=0)
        gate_h = lax.dot_general(picked, w_gate[...], along, preferred_element_type=f32)
        up_h = lax.dot_general(picked, w_up[...], along, preferred_element_type=f32)
        act[pl.ds(0, len(ks) * slots)] = (gate_h / (1.0 + jnp.exp(-gate_h)) * up_h).astype(bf16)

    shares = {}
    down = (((0,), (0,)), ((), ()))

    def end_experts(ks):
        made = jnp.dot(act[pl.ds(0, len(ks) * slots)], w_down[...], preferred_element_type=f32).astype(bf16)
        for i, k in enumerate(ks):
            part = made[i * slots : (i + 1) * slots]
            give[k] = lax.dot_general(mix[device(k, 1 - core)], part, down, preferred_element_type=f32).astype(bf16)
            shares[k] = remote(give.at[k], paired.at[k], pair_send.at[k], pair_recv.at[k], partner)
            send(shares[k])
            mine[k] = lax.dot_general(mix[device(k, core)], part, down, preferred_element_type=f32).astype(bf16)

    seen = set()

    def bring(k):
        if k not in seen:
            seen.add(k)
            shares[k].wait_recv()

    def index_of(dist, h):
        return 0 if dist == half_ring else 1 + 2 * (half_ring - 1 - dist) + h

    def await_ring(way, j):
        piece = arrived.at[way, j]
        remote(piece, piece, ring_send.at[way, j], ring_recv.at[way, j], ahead[way]).wait_recv()

    def advance(dist, chain):
        for way in (0, 1):
            h = way if chain == 0 else 1 - way
            k = offset(way, dist)
            bring(k)
            total = mine[k, spans[h]].astype(f32) + paired[k, spans[h]].astype(f32)
            if dist < half_ring - chain:
                j = index_of(dist + 1, h)
                await_ring(way, j)
                total = total + arrived[way, j].astype(f32)
            mine[k, spans[h]] = total.astype(bf16)
            j = index_of(dist, h)
            send(remote(
                mine.at[k, spans[h]], arrived.at[way, j],
                ring_send.at[way, j], ring_recv.at[way, j], ahead[way],
            ))

    row_near_own()
    for load in loads[10:]:
        load.wait()
    start_experts([0])
    end_experts([0])

    tasks = []
    for j in range(last + 1):
        row_hop(j)
        if j % 2 == 1 or j == last:
            for i in (j - 1, j) if j % 2 == 1 else (j,):
                row_near(i)
            dist = step_of(0, j)[0]
            ks = [half_ring] if j == last else [dist, chips - dist]
            tasks += [functools.partial(start_experts, ks), functools.partial(end_experts, ks)]
        for _ in range(min(len(tasks), 1 if j < last - 1 else len(tasks))):
            tasks.pop(0)()
        if j == last - 1:
            advance(half_ring - 1, 1)

    advance(half_ring, 0)
    for dist in range(half_ring - 2, 0, -1):
        advance(dist, 1)
        advance(dist + 1, 0)
    advance(1, 0)

    bring(0)
    stores = []
    for h in (0, 1):
        total = mine[0, spans[h]].astype(f32) + paired[0, spans[h]].astype(f32)
        for way in (0, 1):
            j = index_of(1, h)
            await_ring(way, j)
            total = total + arrived[way, j].astype(f32)
        produced[spans[h]] = (kept[spans[h]] + total).astype(bf16)
        stores.append(
            pltpu.make_async_copy(produced.at[spans[h]], out_hbm.reshape(count, width).at[spans[h]], load_sem.at[h])
        )
        stores[h].start()
    for store in stores:
        store.wait()
    for copy in waits:
        copy.wait_send()


def fused_layer(
    ids, gates, lengths, gain, latents, queries, memory, hidden, w_uv, w_out, w_gate_t, w_up_t, w_down, n, slots, collective_id
):
    span_len, seqs, width = hidden.shape
    count = span_len * seqs
    lat_width = latents.shape[2]
    head_count = queries.shape[2] // lat_width
    here, _, value_dim = w_uv.shape
    mem_len = memory.shape[0]
    chips = n // 2
    steps = chips - 1
    inner = w_down.shape[0]
    key_total = n * span_len + count
    bf16, f32 = jnp.bfloat16, jnp.float32
    dma, vmem = pltpu.SemaphoreType.DMA, pltpu.VMEM
    row_count = head_count * span_len
    pieces = 2
    return pl.pallas_call(
        functools.partial(layer_kernel, n),
        out_shape=jax.ShapeDtypeStruct((span_len, seqs, width), bf16),
        in_specs=[pl.BlockSpec(memory_space=pl.ANY)] * 13,
        out_specs=pl.BlockSpec(memory_space=pl.ANY),
        scratch_shapes=[
            vmem(ids.shape, jnp.int32),
            vmem(gates.shape, bf16),
            vmem(lengths.shape, jnp.int32),
            vmem(gain.shape, bf16),
            vmem((count, lat_width), bf16),
            vmem((count, head_count * lat_width), bf16),
            vmem((seqs * mem_len, lat_width), bf16),
            vmem((count, width), bf16),
            vmem((count, width), bf16),
            vmem((seqs, key_total, lat_width), bf16),
            vmem((n, 16, count), bf16),
            vmem((seqs, row_count, lat_width), bf16),
            vmem((seqs, row_count, count), jnp.int32),
            vmem((seqs, row_count, count), f32),
            vmem((seqs, row_count, count), f32),
            vmem((seqs, row_count, lat_width), f32),
            vmem((row_count, lat_width), bf16),
            vmem((count, head_count * value_dim), bf16),
            vmem((head_count, lat_width, value_dim), bf16),
            vmem((head_count * value_dim, width), bf16),
            vmem((count, width), f32),
            vmem((chips, slots, 2 * count), bf16),
            vmem((n, slots, count), bf16),
            vmem((n, count, width), bf16),
            vmem((inner, width), bf16),
            vmem((inner, width), bf16),
            vmem((inner, width), bf16),
            vmem((2 * slots, inner), bf16),
            vmem((chips, count, width), bf16),
            vmem((chips, count, width), bf16),
            vmem((chips, count, width), bf16),
            vmem((2, steps, count // 2, width), bf16),
            vmem((count, width), bf16),
            dma((13,)),
            dma((pieces + 3,)),
            dma((pieces + 3,)),
            dma((pieces + 1,)),
            dma((pieces + 1,)),
            dma((3, 2, steps)),
            dma((3, 2, steps)),
            dma((3, 2 * steps + 2)),
            dma((3, 2 * steps + 2)),
            dma((2, 2, steps)),
            dma((2, 2, steps)),
            dma((2, 2 * steps + 2)),
            dma((2, 2 * steps + 2)),
            dma((1, 2, steps)),
            dma((1, 2, steps)),
            dma((1, 2 * steps + 2)),
            dma((1, 2 * steps + 2)),
            dma((2, steps)),
            dma((2, steps)),
            dma((chips,)),
            dma((chips,)),
        ],
        compiler_params=pltpu.CompilerParams(
            collective_id=collective_id, has_side_effects=True, vmem_limit_bytes=67000000
        ),
        cost_estimate=pl.CostEstimate(
            flops=6 * chips * slots * width * inner, bytes_accessed=32 * n * count * width, transcendentals=0
        ),
        name="layer_%d" % collective_id,
    )(ids, gates, lengths, gain, latents, queries, memory, hidden, w_uv, w_out, w_gate_t, w_up_t, w_down)


def round_share(depth, n):
    return depth // (32 * n) * 16


def layer_bytes(n, count, width, inner, slots, lat_width, head_count, value_dim):
    chips = n // 2
    key_total = (n + 2) * count // 2
    row_count = head_count * count // 2
    front = count * (1 + head_count) * lat_width + 2 * key_total * lat_width + 3 * row_count * lat_width
    front += 4 * row_count * lat_width + 12 * row_count * count + head_count * value_dim * (lat_width + width + count)
    back = n * count * width + 3 * width * inner + (4 * chips - 1) * count * width + 5 * count * width
    back += 4 * chips * slots * count + 2 * slots * inner
    return 2 * (front + back) + 8 * slots * inner * 2


def shards(
    hidden,
    queries,
    latents,
    mem_latents,
    lengths,
    ids,
    gates,
    norm_gain,
    w_uv,
    w_out,
    w_gate,
    w_up,
    w_down,
):
    f32, bf16 = jnp.float32, jnp.bfloat16
    local_len, seq_count, model_width = hidden.shape[1:]
    latent_dim = latents.shape[3]
    head_count = queries.shape[3] // latent_dim
    row_count = local_len * seq_count
    n = lax.axis_size("expert")
    dp_size = lax.axis_size("dp")
    me = lax.axis_index("expert")
    core = me % 2
    own_dp = lax.axis_index("dp")
    heads_here, _, value_dim = w_uv.shape
    top_count = ids.shape[3]
    ids_t = jnp.transpose(ids[0], (2, 1, 0)).reshape(top_count, row_count).astype(bf16)
    gates_t = jnp.transpose(gates[0], (2, 1, 0)).reshape(top_count, row_count)
    capacity = min(row_count, row_count * top_count // (n * w_gate.shape[0]) + 2)
    slots = -(-2 * capacity // 128) * 128
    fits = (
        dp_size == 2
        and w_gate.shape[0] == 1
        and n >= 8
        and top_count <= 8
        and seq_count == 2
        and row_count % 128 == 0
        and heads_here % 2 == 0
        and heads_here * value_dim % (32 * n) == 0
        and mem_latents.shape[1] <= row_count
        and layer_bytes(n, row_count, model_width, w_down.shape[1], slots, latent_dim, head_count, value_dim)
        < 60 * 1024 * 1024
    )
    if fits:
        out = fused_layer(
            jnp.transpose(ids[0], (2, 1, 0)), jnp.transpose(gates[0], (2, 1, 0)), lengths, norm_gain,
            latents[0], queries[0], mem_latents[0], hidden[0], w_uv, w_out,
            jnp.transpose(w_gate[0]), jnp.transpose(w_up[0]), w_down[0], n, slots, 4,
        )
        return out[None]

    half_heads = heads_here // 2
    uv_half = lax.dynamic_slice_in_dim(w_uv, core * half_heads, half_heads, 0)
    out_half = lax.dynamic_slice_in_dim(
        w_out, core * half_heads * value_dim, half_heads * value_dim, 0
    )
    uv_groups, out_groups, starts = [w_uv], [w_out], [own_dp * heads_here]
    swap = [(i, i ^ 1) for i in range(n)]
    sizes = [heads_here]
    for shift in range(1, dp_size):
        turn = [(i, (i + shift) % dp_size) for i in range(dp_size)]
        source = (own_dp - shift + dp_size) % dp_size
        uv_far = lax.ppermute(uv_half, "dp", turn)
        out_far = lax.ppermute(out_half, "dp", turn)
        uv_near = lax.ppermute(uv_far, "expert", swap)
        out_near = lax.ppermute(out_far, "expert", swap)
        uv_groups += [uv_far, uv_near]
        out_groups += [out_far, out_near]
        starts += [
            source * heads_here + core * half_heads,
            source * heads_here + (1 - core) * half_heads,
        ]
        sizes += [half_heads, half_heads]

    latent_rows = jnp.transpose(latents[0], (1, 0, 2)).reshape(row_count, latent_dim)
    table = jnp.concatenate([ids_t, gates_t], axis=0).reshape(-1)
    table_rows = -(-table.shape[0] // (16 * latent_dim)) * 16
    table = jnp.pad(table, (0, table_rows * latent_dim - table.shape[0]))
    packed = jnp.concatenate([latent_rows, table.reshape(table_rows, latent_dim)], axis=0)
    all_rows = row_count + table_rows
    cut = (all_rows // 2 + 15) // 16 * 16
    gathered = ring_gather(packed, n, cut, 0)

    segment = gathered[:, :row_count].reshape(n, seq_count, local_len, latent_dim)
    segment = jnp.transpose(segment, (1, 0, 2, 3)).reshape(seq_count, n * local_len, latent_dim)
    memory = jnp.transpose(mem_latents[0], (1, 0, 2))
    mem_count = memory.shape[1]
    keys = jnp.concatenate([memory, segment], axis=1)
    query_rows = jnp.transpose(
        queries[0].reshape(local_len, seq_count, head_count, latent_dim), (1, 2, 0, 3)
    ).reshape(seq_count, head_count * local_len, latent_dim)
    scores = jnp.einsum("sql,sjl->sqj", query_rows, keys, preferred_element_type=f32) * score_scale
    key_pos = lax.broadcasted_iota(jnp.int32, scores.shape, 2) - mem_count
    own_pos = me * local_len + lax.broadcasted_iota(jnp.int32, scores.shape, 1) % local_len
    visible = (key_pos <= own_pos) & (key_pos < lengths[0][:, None, None])
    scores = jnp.where(visible | (key_pos < 0), scores, -jnp.inf)
    weights = jnp.exp(scores - jnp.max(scores, axis=2, keepdims=True))
    total = jnp.sum(weights, axis=2, keepdims=True)
    attended = jnp.einsum("sqj,sjl->sql", weights.astype(bf16), keys, preferred_element_type=f32)
    attended = (attended / total).astype(bf16)
    attended = attended.reshape(seq_count, head_count, local_len, latent_dim)

    attn_out = jnp.zeros((row_count, model_width), f32)
    for uv, out, start, size in zip(uv_groups, out_groups, starts, sizes):
        heads = lax.dynamic_slice_in_dim(attended, start, size, 1)
        values = jnp.einsum("shtl,hlv->sthv", heads, uv, preferred_element_type=f32).astype(bf16)
        attn_out = attn_out + jnp.dot(
            values.reshape(row_count, size * value_dim), out, preferred_element_type=f32
        )

    hidden_rows = jnp.transpose(hidden[0], (1, 0, 2)).reshape(row_count, model_width)
    residual = lax.optimization_barrier(hidden_rows).astype(f32) + attn_out
    mean_square = jnp.mean(residual * residual, axis=-1, keepdims=True)
    normed = (residual * lax.rsqrt(mean_square + norm_eps) * norm_gain.astype(f32)).astype(bf16)

    rows_all = ring_gather(normed, n, row_count // 2, 1)
    experts_here = w_gate.shape[0]
    expert_count = n * experts_here
    groups = n // 2
    wide = 2 * row_count
    slots = -(-2 * capacity // 16) * 16
    tables = gathered[:, row_count:].reshape(n, -1)[:, : 2 * top_count * row_count]
    tables = tables.reshape(groups, 2, 2, top_count, row_count)
    named = jnp.transpose(tables[:, :, 0], (2, 0, 1, 3)).reshape(top_count, groups, wide)
    scale = jnp.transpose(tables[:, :, 1], (2, 0, 1, 3)).reshape(top_count, groups, wide)
    rows_all = rows_all.reshape(groups, wide, model_width)
    steps = jnp.arange(wide, dtype=jnp.int32)
    earlier = (steps[:, None] < steps[None, :]).astype(bf16)
    made_rows, mixes = [], []
    for e in range(experts_here):
        matches = named == (me * experts_here + e).astype(bf16)
        hit = jnp.any(matches, axis=0)
        gate = jnp.sum(jnp.where(matches, scale.astype(f32), 0.0), axis=0)
        slot = jnp.dot(hit.astype(bf16), earlier, preferred_element_type=f32).astype(jnp.int32)
        slot = jnp.where(hit, slot, -1)
        chosen = slot[:, None, :] == jnp.arange(slots, dtype=jnp.int32)[None, :, None]
        placing = chosen.astype(bf16)
        slot_t = jnp.where(hit, slot, -1).reshape(n, row_count)
        chosen_t = slot_t[:, :, None] == jnp.arange(slots, dtype=jnp.int32)[None, None, :]
        mixes.append(jnp.where(chosen_t, gate.reshape(n, row_count)[:, :, None], 0.0).astype(bf16))
        picked = jnp.einsum("gct,gtd->gcd", placing, rows_all, preferred_element_type=f32)
        picked = picked.astype(bf16).reshape(groups * slots, model_width)
        gate_h = jnp.dot(picked, w_gate[e], preferred_element_type=f32)
        up_h = jnp.dot(picked, w_up[e], preferred_element_type=f32)
        act = (jax.nn.silu(gate_h) * up_h).astype(bf16)
        produced = jnp.dot(act, w_down[e], preferred_element_type=f32).astype(bf16)
        made_rows.append(produced.reshape(groups, slots, model_width))
    made_rows = made_rows[0] if experts_here == 1 else jnp.concatenate(made_rows, axis=1)
    mixing = mixes[0] if experts_here == 1 else jnp.concatenate(mixes, axis=2)
    routed = ring_reduce(made_rows, mixing, n, 2)
    layer_out = (residual + routed).astype(bf16).reshape(seq_count, local_len, model_width)
    return jnp.transpose(layer_out, (1, 0, 2))[None]


def solution(mesh):
    return jax.shard_map(
        shards,
        mesh=mesh,
        in_specs=(
            P("dp", "expert", None, None),
            P("dp", "expert", None, None),
            P("dp", "expert", None, None),
            P("dp", None, None, None),
            P("dp", None),
            P("dp", "expert", None, None),
            P("dp", "expert", None, None),
            P(),
            P("dp", None, None),
            P("dp", None),
            P("expert", None, None),
            P("expert", None, None),
            P("expert", None, None),
        ),
        out_specs=P("dp", "expert", None, None),
        check_vma=False,
    )
```

```python
import functools

import jax
import jax.numpy as jnp
from jax import lax
from jax.experimental import pallas as pl
from jax.experimental.pallas import tpu as pltpu
from jax.sharding import PartitionSpec as P

score_scale = 192.0 ** (-0.5)
norm_eps = 1e-06
MESH = pl.DeviceIdType.MESH


def ring_place(n):
    chips = n // 2
    depth = chips // 2
    me = lax.axis_index("expert")
    core = me % 2
    chip = me // 2
    row, col = chip // 2, chip % 2
    pos = col * row + (1 - col) * (chips - 1 - row)

    def device(offset, core_of):
        p = (pos + offset + chips) % chips
        q = p // depth
        r = (1 - q) * p + q * (chips - 1 - p)
        return (2 * r + 1 - q) * 2 + core_of

    return me, core, device


def greet(targets):
    barrier = pltpu.get_barrier_semaphore()
    for target in targets:
        pl.semaphore_signal(barrier, inc=1, device_id={"expert": target}, device_id_type=MESH)
    pl.semaphore_wait(barrier, len(targets))


def remote(src, dst, send_sem, recv_sem, target):
    return pltpu.make_async_remote_copy(
        src_ref=src,
        dst_ref=dst,
        send_sem=send_sem,
        recv_sem=recv_sem,
        device_id={"expert": target},
        device_id_type=MESH,
    )


def gather_kernel(n, cut, x_ref, out_ref, ring_send, ring_recv, pair_send, pair_recv, own_sem):
    chips = n // 2
    half_ring = chips // 2
    rows = x_ref.shape[0]
    last = chips - 2
    me, core, device = ring_place(n)
    partner = device(0, 1 - core)
    ahead = (device(1, core), device(-1, core))
    spans = (pl.ds(0, cut), pl.ds(cut, rows - cut))
    greet((ahead[0], ahead[1], partner))

    def arrival(way, j):
        dist, half = (half_ring, way) if j == last else (j // 2 + 1, j % 2)
        return device(-dist if way == 0 else dist, core), spans[half]

    waits = []
    for way in (0, 1):
        for j in (0, 1):
            if j > last:
                continue
            if j == last and half_ring == 1:
                span = spans[way]
            else:
                span = spans[j]
            copy = remote(
                x_ref.at[span], out_ref.at[me, span],
                ring_send.at[way, j], ring_recv.at[way, j], ahead[way],
            )
            copy.start()
            waits.append(copy)
    share = remote(x_ref, out_ref.at[me], pair_send.at[2 * last + 2], pair_recv.at[2 * last + 2], partner)
    share.start()
    waits.append(share)
    keep = pltpu.make_async_copy(x_ref, out_ref.at[me], own_sem)
    keep.start()

    for j in range(last + 1):
        for way in (0, 1):
            slot, span = arrival(way, j)
            piece = out_ref.at[slot, span]
            remote(piece, piece, ring_send.at[way, j], ring_recv.at[way, j], ahead[way]).wait_recv()
            onward = j + 2
            if j >= last - 2 and j < last:
                onward = last if j == last - 2 + way else None
            if j == last:
                onward = None
            if onward is not None:
                copy = remote(piece, piece, ring_send.at[way, onward], ring_recv.at[way, onward], ahead[way])
                copy.start()
                waits.append(copy)
            index = 2 * j + way
            copy = remote(piece, piece, pair_send.at[index], pair_recv.at[index], partner)
            copy.start()
            waits.append(copy)

    for j in range(last + 1):
        for way in (0, 1):
            dist, half = (half_ring, way) if j == last else (j // 2 + 1, j % 2)
            slot = device(-dist if way == 0 else dist, 1 - core)
            piece = out_ref.at[slot, spans[half]]
            index = 2 * j + way
            remote(piece, piece, pair_send.at[index], pair_recv.at[index], partner).wait_recv()
    other = out_ref.at[partner]
    remote(other, other, pair_send.at[2 * last + 2], pair_recv.at[2 * last + 2], partner).wait_recv()
    for copy in waits:
        copy.wait_send()
    keep.wait()


def ring_gather(x, n, cut, collective_id):
    rows, cols = x.shape
    steps = n // 2 - 1
    return pl.pallas_call(
        functools.partial(gather_kernel, n, cut),
        out_shape=jax.ShapeDtypeStruct((n, rows, cols), x.dtype),
        in_specs=[pl.BlockSpec(memory_space=pltpu.VMEM)],
        out_specs=pl.BlockSpec(memory_space=pl.ANY),
        scratch_shapes=[
            pltpu.SemaphoreType.DMA((2, steps)),
            pltpu.SemaphoreType.DMA((2, steps)),
            pltpu.SemaphoreType.DMA((2 * steps + 1,)),
            pltpu.SemaphoreType.DMA((2 * steps + 1,)),
            pltpu.SemaphoreType.DMA,
        ],
        compiler_params=pltpu.CompilerParams(collective_id=collective_id, has_side_effects=True),
        cost_estimate=pl.CostEstimate(flops=0, bytes_accessed=16 * n * rows * cols, transcendentals=0),
        name="ring_gather_%d" % collective_id,
    )(x)


def reduce_kernel(
    n, rows_ref, mix_ref, out_ref, mine, paired, give, arrived, ring_send, ring_recv, pair_send, pair_recv
):
    chips = n // 2
    half_ring = chips // 2
    half = mine.shape[1] // 2
    last = chips - 2
    me, core, device = ring_place(n)
    partner = device(0, 1 - core)
    ahead = (device(1, core), device(-1, core))
    greet((ahead[0], ahead[1], partner))

    order = [half_ring]
    for k in range(half_ring - 1, 0, -1):
        order += [k, chips - k]
    order.append(0)
    depth = give.shape[0]
    shares, made, seen = {}, [], set()

    def weigh(k, core_of):
        dest = device(k, core_of)
        return jnp.dot(
            mix_ref[dest], rows_ref[dest // 2], preferred_element_type=jnp.float32
        ).astype(mine.dtype)

    def make():
        k = order[len(made)]
        slot = len(made) % depth
        if len(made) >= depth:
            shares[order[len(made) - depth]].wait_send()
        give[slot] = weigh(k, 1 - core)
        shares[k] = remote(give.at[slot], paired.at[k], pair_send.at[k], pair_recv.at[k], partner)
        shares[k].start()
        mine[k] = weigh(k, core)
        made.append(k)

    def bring(k):
        while k not in made or (len(made) < chips and len(made) < order.index(k) + 3):
            make()
        if k not in seen:
            seen.add(k)
            shares[k].wait_recv()

    def index_of(dist, h):
        return 0 if dist == half_ring else 1 + 2 * (half_ring - 1 - dist) + h

    def await_ring(way, j):
        piece = arrived.at[way, j]
        remote(piece, piece, ring_send.at[way, j], ring_recv.at[way, j], ahead[way]).wait_recv()

    sends = []
    for dist in range(half_ring, 0, -1):
        for turn in (0, 1):
            for way in (0, 1):
                if dist == half_ring:
                    if turn == 1:
                        continue
                    h = way
                elif dist == half_ring - 1:
                    h = 1 - way if turn == 0 else way
                else:
                    h = turn
                k = dist if way == 0 else chips - dist
                bring(k)
                span = pl.ds(h * half, half)
                total = mine[k, span].astype(jnp.float32) + paired[k, span].astype(jnp.float32)
                has_prior = dist < half_ring - 1 or (dist == half_ring - 1 and h == way)
                if has_prior:
                    j = index_of(dist + 1, h)
                    await_ring(way, j)
                    total = total + arrived[way, j].astype(jnp.float32)
                mine[k, span] = total.astype(mine.dtype)
                j = index_of(dist, h)
                copy = remote(
                    mine.at[k, span], arrived.at[way, j],
                    ring_send.at[way, j], ring_recv.at[way, j], ahead[way],
                )
                copy.start()
                sends.append(copy)
    bring(0)
    for h in (0, 1):
        span = pl.ds(h * half, half)
        total = mine[0, span].astype(jnp.float32) + paired[0, span].astype(jnp.float32)
        for way in (0, 1):
            j = index_of(1, h)
            await_ring(way, j)
            total = total + arrived[way, j].astype(jnp.float32)
        out_ref[span] = total
    for copy in sends:
        copy.wait_send()
    for k in order[chips - min(depth, chips) :]:
        shares[k].wait_send()


def ring_reduce(rows_in, mix, n, collective_id):
    rows = mix.shape[1]
    cols = rows_in.shape[2]
    chips = n // 2
    dtype = rows_in.dtype
    return pl.pallas_call(
        functools.partial(reduce_kernel, n),
        out_shape=jax.ShapeDtypeStruct((rows, cols), jnp.float32),
        in_specs=[pl.BlockSpec(memory_space=pltpu.VMEM)] * 2,
        out_specs=pl.BlockSpec(memory_space=pltpu.VMEM),
        scratch_shapes=[
            pltpu.VMEM((chips, rows, cols), dtype),
            pltpu.VMEM((chips, rows, cols), dtype),
            pltpu.VMEM((min(4, chips), rows, cols), dtype),
            pltpu.VMEM((2, chips - 1, rows // 2, cols), dtype),
            pltpu.SemaphoreType.DMA((2, chips - 1)),
            pltpu.SemaphoreType.DMA((2, chips - 1)),
            pltpu.SemaphoreType.DMA((chips,)),
            pltpu.SemaphoreType.DMA((chips,)),
        ],
        compiler_params=pltpu.CompilerParams(
            collective_id=collective_id, has_side_effects=True, vmem_limit_bytes=62 * 1024 * 1024
        ),
        cost_estimate=pl.CostEstimate(
            flops=2 * mix.size * cols, bytes_accessed=16 * n * rows * cols, transcendentals=0
        ),
        name="ring_reduce_%d" % collective_id,
    )(rows_in, mix)


def layer_kernel(
    n,
    ids_hbm, gates_hbm, limit_hbm, gain_hbm,
    latent_hbm, query_hbm, memory_hbm, hidden_hbm, uv_hbm, wout_hbm, gate_hbm, up_hbm, down_hbm,
    out_ref,
    ids, gates, limit, gain,
    latent, query, memory, hidden, parted_hidden, keys, tables, heads, bound, peak, mass, blend,
    attended, values, w_uv, w_out, kept,
    place, mix, rows, w_gate, w_up, w_down, act, mine, paired, give, arrived,
    load_sem, far_send, far_recv, near_send, near_recv,
    key_send, key_recv, key_swap_send, key_swap_recv,
    row_send, row_recv, row_swap_send, row_swap_recv,
    round_send, round_recv, round_swap_send, round_swap_recv,
    ring_send, ring_recv, pair_send, pair_recv,
):
    f32, bf16 = jnp.float32, jnp.bfloat16
    chips = n // 2
    half_ring = chips // 2
    last = chips - 2
    count, width = kept.shape
    seqs, span_len = 2, count // 2
    lat_width = latent.shape[1]
    mem_len = memory.shape[0] // 2
    head_count = query.shape[1] // lat_width
    mem_at = n * span_len
    key_total = keys.shape[1]
    top_count = ids.shape[0]
    here = uv_hbm.shape[0]
    value_dim = uv_hbm.shape[2]
    half_here = here // 2
    slots = place.shape[1]
    me, core, device = ring_place(n)
    own_dp = lax.axis_index("dp")
    far_dp = 1 - own_dp
    partner = device(0, 1 - core)
    ahead = (device(1, core), device(-1, core))
    spans = (pl.ds(0, span_len), pl.ds(span_len, span_len))

    loads = [
        pltpu.make_async_copy(src, dst, load_sem.at[i])
        for i, (src, dst) in enumerate((
            (latent_hbm.reshape(count, lat_width), latent),
            (ids_hbm, ids),
            (gates_hbm, gates),
            (limit_hbm, limit),
            (gain_hbm, gain),
            (query_hbm.reshape(query.shape), query),
            (memory_hbm.reshape(memory.shape), memory),
            (uv_hbm, w_uv.at[pl.ds(own_dp * here, here)]),
            (hidden_hbm.reshape(count, width), hidden),
            (wout_hbm, w_out.at[pl.ds(own_dp * here * value_dim, here * value_dim)]),
            (gate_hbm, w_gate),
            (up_hbm, w_up),
            (down_hbm, w_down),
        ))
    ]
    for load in loads:
        load.start()
    waits = []

    def send(copy):
        copy.start()
        waits.append(copy)

    barrier = pltpu.get_barrier_semaphore()
    for target in (ahead[0], ahead[1], partner):
        pl.semaphore_signal(barrier, inc=1, device_id={"expert": target}, device_id_type=MESH)
    pl.semaphore_signal(barrier, inc=1, device_id={"dp": far_dp}, device_id_type=MESH)
    pl.semaphore_wait(barrier, 4)

    def uv_piece(owner, of_core):
        return pl.ds(owner * here + of_core * half_here, half_here)

    depth = here * value_dim
    round_rows = round_share(depth, n)
    pieces = far_send.shape[0] - 3
    out_rows = (depth - n * round_rows) // (2 * pieces)

    def out_piece(first, of_core, i):
        at = first + n * round_rows + (of_core * pieces + i) * out_rows
        return pl.ds(pl.multiple_of(at, 8), out_rows)

    def round_piece(first, slot, h):
        size = -(-round_rows // 16) * 8
        return pl.ds(pl.multiple_of(first + slot * round_rows + h * size, 8), size if h == 0 else round_rows - size)

    def across(src, dst, i):
        return pltpu.make_async_remote_copy(
            src_ref=src, dst_ref=dst, send_sem=far_send.at[i], recv_sem=far_recv.at[i],
            device_id={"dp": far_dp}, device_id_type=MESH,
        )

    for h in (0, 1):
        send(across(wout_hbm.at[round_piece(0, me, h)], w_out.at[round_piece(own_dp * depth, me, h)], pieces + 1 + h))
    send(across(uv_hbm.at[pl.ds(core * half_here, half_here)], w_uv.at[uv_piece(own_dp, core)], 0))
    for i in range(pieces):
        send(across(wout_hbm.at[out_piece(0, core, i)], w_out.at[out_piece(own_dp * depth, core, i)], i + 1))

    def far_ref(i, of_core):
        return w_uv.at[uv_piece(far_dp, of_core)] if i == 0 else w_out.at[out_piece(far_dp * depth, of_core, i - 1)]

    def pass_far(i):
        piece = far_ref(i, core)
        across(piece, piece, i).wait_recv()
        send(remote(piece, piece, near_send.at[i], near_recv.at[i], partner))

    def await_near(i):
        piece = far_ref(i, 1 - core)
        remote(piece, piece, near_send.at[i], near_recv.at[i], partner).wait_recv()

    def step_of(way, j):
        return (half_ring, way) if j == last else (j // 2 + 1, j % 2)

    def offset(way, dist):
        return dist if way == 0 else chips - dist

    def gather(parts, sends, recvs, swap_sends, swap_recvs):
        own = 2 * last + 2

        def start(h):
            for way in (0, 1):
                for i, ref in enumerate(parts(me, h)):
                    send(remote(ref, ref, sends.at[i, way, h], recvs.at[i, way, h], ahead[way]))
            for i, ref in enumerate(parts(me, h)):
                send(remote(ref, ref, swap_sends.at[i, own + h], swap_recvs.at[i, own + h], partner))

        def near_own():
            for h in (0, 1):
                for i, ref in enumerate(parts(partner, h)):
                    remote(ref, ref, swap_sends.at[i, own + h], swap_recvs.at[i, own + h], partner).wait_recv()

        def hop(j):
            onward = [j + 2, j + 2]
            if last - 2 <= j < last:
                onward = [last if j == last - 2 + way else None for way in (0, 1)]
            if j == last:
                onward = [None, None]
            for way in (0, 1):
                dist, h = step_of(way, j)
                for i, ref in enumerate(parts(device(-dist if way == 0 else dist, core), h)):
                    remote(ref, ref, sends.at[i, way, j], recvs.at[i, way, j], ahead[way]).wait_recv()
                    if onward[way] is not None:
                        k = onward[way]
                        send(remote(ref, ref, sends.at[i, way, k], recvs.at[i, way, k], ahead[way]))
                    k = 2 * j + way
                    send(remote(ref, ref, swap_sends.at[i, k], swap_recvs.at[i, k], partner))

        def near(j):
            for way in (0, 1):
                dist, h = step_of(way, j)
                k = 2 * j + way
                for i, ref in enumerate(parts(device(-dist if way == 0 else dist, 1 - core), h)):
                    remote(ref, ref, swap_sends.at[i, k], swap_recvs.at[i, k], partner).wait_recv()

        return start, near_own, hop, near

    def split_of(total):
        to = lax.broadcasted_iota(jnp.int32, (total, total), 0)
        at = lax.broadcasted_iota(jnp.int32, (total, total), 1)
        return (to == at % 2 * (total // 2) + at // 2).astype(f32).astype(bf16)

    split = split_of(count)
    to = lax.broadcasted_iota(jnp.int32, (count, count), 0)
    at = lax.broadcasted_iota(jnp.int32, (count, count), 1)
    weave = (at == to % 2 * span_len + to // 2).astype(f32).astype(bf16)

    def place_of(slot, first, size):
        return pl.ds(pl.multiple_of(slot * span_len + first, size), size)

    sub = span_len // 2

    def key_parts(s):
        def parts(slot, h):
            found = [keys.at[s, place_of(slot, h * sub, sub)]]
            return found + ([tables.at[slot]] if s == 0 and h == 0 else [])

        return gather(parts, key_send.at[s], key_recv.at[s], key_swap_send.at[s], key_swap_recv.at[s])

    streams = [key_parts(s) for s in range(seqs)]
    for load in loads[:5]:
        load.wait()
    lines = []
    for source, filler in ((ids, 255.0), (gates, 0.0)):
        taken = source[...].astype(f32)
        lines.append(jnp.concatenate([taken[:, s, :] for s in range(seqs)], axis=1))
        if top_count < 8:
            lines.append(jnp.full((8 - top_count, count), filler, f32))
    tables[me] = jnp.concatenate(lines, axis=0).astype(bf16)
    for s in range(seqs):
        keys[s, place_of(me, 0, span_len)] = jnp.dot(
            split[s * span_len : (s + 1) * span_len], latent[...], preferred_element_type=f32
        ).astype(bf16)
        for h in (0, 1):
            streams[s][0](h)

    loads[5].wait()
    for s in range(seqs):
        parted = jnp.dot(
            split[s * span_len : (s + 1) * span_len], query[...], preferred_element_type=f32
        ).astype(bf16)
        for h in range(head_count):
            heads[s, pl.ds(h * span_len, span_len)] = parted[:, h * lat_width : (h + 1) * lat_width]
    loads[6].wait()
    parted = jnp.dot(split_of(2 * mem_len), memory[...], preferred_element_type=f32).astype(bf16)
    lanes = 2 * span_len
    row_count = head_count * span_len
    lane = lax.broadcasted_iota(jnp.int32, (row_count, lanes), 1)
    own_pos = me * span_len + lax.broadcasted_iota(jnp.int32, (row_count, lanes), 0) % span_len
    along = (((1,), (1,)), ((), ()))
    scale = score_scale * 1.4426950408889634
    for s in range(seqs):
        keys[s, pl.ds(mem_at, mem_len)] = parted[s * mem_len : (s + 1) * mem_len]
        keys[s, pl.ds(mem_at + mem_len, key_total - mem_at - mem_len)] = jnp.zeros(
            (key_total - mem_at - mem_len, lat_width), bf16
        )
        bound[s] = jnp.minimum(own_pos, limit[:, s : s + 1] - 1) - lane

    def wide(x, times):
        return x if times == 1 else jnp.concatenate([x] * times, axis=1)

    def attend(ks, chosen_seqs, opening=False):
        firsts = [pl.multiple_of(device(k, 0) * span_len, lanes) for k in ks]
        for s in chosen_seqs:
            held = [keys[s, pl.ds(first, lanes)] for first in firsts]
            seen_keys = [first <= bound[s] for first in firsts]
            if opening:
                held.append(keys[s, pl.ds(mem_at, lanes)])
                seen_keys.append(lane < mem_len)
            held = held[0] if len(held) == 1 else jnp.concatenate(held, axis=0)
            score = lax.dot_general(heads[s], held, along, preferred_element_type=f32)
            parts = [
                jnp.where(visible, score[:, i * lanes : (i + 1) * lanes], -jnp.inf)
                for i, visible in enumerate(seen_keys)
            ]
            top = functools.reduce(jnp.maximum, parts)
            top = jnp.broadcast_to(jnp.max(top, axis=1, keepdims=True), top.shape)
            if not opening:
                before = peak[s]
                top = jnp.maximum(before, top)
                fade = jnp.exp2((before - top) * scale)
            parts = [jnp.exp2((part - top) * scale) for part in parts]
            added = functools.reduce(jnp.add, parts)
            mass[s] = added if opening else mass[s] * fade + added
            peak[s] = top
            weight = parts[0] if len(parts) == 1 else jnp.concatenate(parts, axis=1)
            more = jnp.dot(weight.astype(bf16), held, preferred_element_type=f32)
            blend[s] = more if opening else blend[s] * wide(fade, lat_width // lanes) + more

    def round_parts(slot, h):
        return [w_out.at[round_piece(far_dp * depth, slot, h)]]

    round_start, round_near_own, round_hop, round_near = gather(
        round_parts, round_send, round_recv, round_swap_send, round_swap_recv
    )
    def steps_at(dist):
        return (last,) if dist == half_ring else (2 * dist - 2, 2 * dist - 1)

    def at_dist(dist):
        return [half_ring] if dist == half_ring else [dist, chips - dist]

    def hop_all(stream, dist):
        for j in steps_at(dist):
            stream[2](j)

    def use_keys(chosen_seqs, dist):
        for s in chosen_seqs:
            for j in steps_at(dist):
                streams[s][3](j)
        attend(at_dist(dist), chosen_seqs)

    rounds = (round_start, round_near_own, round_hop, round_near)
    for dist in range(1, half_ring):
        for s in range(seqs):
            hop_all(streams[s], dist)
        if dist == 1:
            for h in (0, 1):
                piece = w_out.at[round_piece(far_dp * depth, me, h)]
                across(piece, piece, pieces + 1 + h).wait_recv()
                round_start(h)
            for s in range(seqs):
                streams[s][1]()
            attend([0], range(seqs), True)
            loads[8].wait()
            parted_hidden[...] = jnp.dot(split, hidden[...], preferred_element_type=f32).astype(bf16)
        else:
            hop_all(rounds, dist - 1)
            use_keys(range(seqs), dist - 1)
    loads[7].wait()
    pass_far(0)
    for s in range(seqs):
        hop_all(streams[s], half_ring)
    pass_far(1)
    hop_all(rounds, half_ring - 1)
    use_keys(range(seqs), half_ring - 1)
    use_keys([0], half_ring)
    for i in range(2, pieces + 1):
        pass_far(i)

    def row_parts(slot, h):
        return [rows.at[slot, pl.ds(h * span_len + i * sub, sub)] for i in (0, 1)]

    row_start, row_near_own, row_hop, row_near = gather(row_parts, row_send, row_recv, row_swap_send, row_swap_recv)
    await_near(0)
    near_cols = pl.ds(pl.multiple_of(own_dp * depth, depth), depth)
    far_cols = pl.ds(pl.multiple_of(far_dp * depth, depth), depth)
    loads[9].wait()
    for s in range(seqs):
        if s == 1:
            use_keys([1], half_ring)
        total = jnp.sum(mass[s], axis=1, keepdims=True)
        attended[...] = (blend[s] / total).astype(bf16)
        for h in range(head_count):
            values[spans[s], pl.ds(h * value_dim, value_dim)] = jnp.dot(
                attended[pl.ds(h * span_len, span_len)], w_uv[h], preferred_element_type=f32
            ).astype(bf16)
        residual = parted_hidden[spans[s]].astype(f32) + jnp.dot(
            values[spans[s], near_cols], w_out[near_cols], preferred_element_type=f32
        )
        if s == 0:
            hop_all(rounds, half_ring)
            round_near_own()
            for i in range(last + 1):
                round_near(i)
            for i in range(1, pieces + 1):
                await_near(i)
        residual = residual + jnp.dot(values[spans[s], far_cols], w_out[far_cols], preferred_element_type=f32)
        mean_square = jnp.mean(residual * residual, axis=1, keepdims=True)
        normed = residual * lax.rsqrt(mean_square + norm_eps) * gain[...].astype(f32)
        rows[me, spans[s]] = normed.astype(bf16)
        row_start(s)

    woven = jnp.dot(weave, values[...], preferred_element_type=f32).astype(bf16)
    kept[...] = (
        hidden[...].astype(f32)
        + jnp.dot(woven[:, :depth], w_out[pl.ds(0, depth)], preferred_element_type=f32)
        + jnp.dot(woven[:, depth:], w_out[pl.ds(depth, depth)], preferred_element_type=f32)
    )
    hits, scales = [], []
    own_id = me.astype(f32)
    for c in range(chips):
        pair = jnp.concatenate([tables[2 * c], tables[2 * c + 1]], axis=1).astype(f32)
        matches = pair[:8] == own_id
        hits.append(jnp.max(jnp.where(matches, 1.0, 0.0), axis=0, keepdims=True))
        scales.append(jnp.sum(jnp.where(matches, pair[8:], 0.0), axis=0, keepdims=True))
    hits = jnp.concatenate(hits, axis=0)
    to = lax.broadcasted_iota(jnp.int32, (2 * count, 2 * count), 0)
    at = lax.broadcasted_iota(jnp.int32, (2 * count, 2 * count), 1)
    earlier = (to < at).astype(f32).astype(bf16)
    ranks = jnp.dot(hits.astype(bf16), earlier, preferred_element_type=f32)
    ranks = jnp.where(hits > 0.5, ranks, -1.0)
    slot_id = lax.broadcasted_iota(jnp.int32, (slots, 2 * count), 0).astype(f32)
    for c in range(chips):
        chosen = slot_id == ranks[c : c + 1]
        place[c] = jnp.where(chosen, 1.0, 0.0).astype(bf16)
        weighed = jnp.where(chosen, scales[c], 0.0).astype(bf16)
        for i in (0, 1):
            own_part = weighed[:, i * count : (i + 1) * count]
            mix[2 * c + i] = jnp.dot(own_part, split, preferred_element_type=f32).astype(bf16)

    def start_experts(ks):
        picked = []
        for k in ks:
            first = device(k, 0)
            held = rows[pl.ds(first, 2)].reshape(2 * count, width)
            picked.append(jnp.dot(place[first // 2], held, preferred_element_type=f32).astype(bf16))
        picked = picked[0] if len(ks) == 1 else jnp.concatenate(picked, axis=0)
        gate_h = lax.dot_general(picked, w_gate[...], along, preferred_element_type=f32)
        up_h = lax.dot_general(picked, w_up[...], along, preferred_element_type=f32)
        act[pl.ds(0, len(ks) * slots)] = (gate_h / (1.0 + jnp.exp(-gate_h)) * up_h).astype(bf16)

    shares = {}
    down = (((0,), (0,)), ((), ()))

    def end_experts(ks):
        made = jnp.dot(act[pl.ds(0, len(ks) * slots)], w_down[...], preferred_element_type=f32).astype(bf16)
        for i, k in enumerate(ks):
            part = made[i * slots : (i + 1) * slots]
            give[k] = lax.dot_general(mix[device(k, 1 - core)], part, down, preferred_element_type=f32).astype(bf16)
            shares[k] = remote(give.at[k], paired.at[k], pair_send.at[k], pair_recv.at[k], partner)
            send(shares[k])
            mine[k] = lax.dot_general(mix[device(k, core)], part, down, preferred_element_type=f32).astype(bf16)

    seen = set()

    def bring(k):
        if k not in seen:
            seen.add(k)
            shares[k].wait_recv()

    def index_of(dist, h):
        return 0 if dist == half_ring else 1 + 2 * (half_ring - 1 - dist) + h

    def await_ring(way, j, u):
        piece = arrived.at[way, j, pl.ds(u * sub, sub)]
        remote(piece, piece, ring_send.at[u, way, j], ring_recv.at[u, way, j], ahead[way]).wait_recv()

    def advance(dist, chain):
        for u in (0, 1):
            for way in (0, 1):
                h = way if chain == 0 else 1 - way
                k = offset(way, dist)
                bring(k)
                part, within = pl.ds(h * span_len + u * sub, sub), pl.ds(u * sub, sub)
                total = mine[k, part].astype(f32) + paired[k, part].astype(f32)
                if dist < half_ring - chain:
                    j = index_of(dist + 1, h)
                    await_ring(way, j, u)
                    total = total + arrived[way, j, within].astype(f32)
                mine[k, part] = total.astype(bf16)
                j = index_of(dist, h)
                send(remote(
                    mine.at[k, part], arrived.at[way, j, within],
                    ring_send.at[u, way, j], ring_recv.at[u, way, j], ahead[way],
                ))

    row_near_own()
    for load in loads[10:]:
        load.wait()
    start_experts([0])
    end_experts([0])

    tasks = []
    for j in range(last + 1):
        if j < last:
            row_hop(j)
        if j % 2 == 1 or j == last:
            for i in (j - 1, j) if j % 2 == 1 else (j,):
                row_near(i)
            dist = step_of(0, j)[0]
            ks = [half_ring] if j == last else [dist, chips - dist]
            tasks += [functools.partial(start_experts, ks), functools.partial(end_experts, ks)]
        for _ in range(min(len(tasks), 1 if j < last - 1 else len(tasks))):
            tasks.pop(0)()
        if j == last - 1:
            row_hop(last)
            advance(half_ring - 1, 1)

    advance(half_ring, 0)
    for dist in range(half_ring - 2, 0, -1):
        advance(dist, 1)
        advance(dist + 1, 0)
    advance(1, 0)

    bring(0)
    for u, h in ((0, 0), (0, 1), (1, 0), (1, 1)):
        part, within = pl.ds(h * span_len + u * sub, sub), pl.ds(u * sub, sub)
        total = kept[part] + mine[0, part].astype(f32) + paired[0, part].astype(f32)
        for way in (0, 1):
            j = index_of(1, h)
            await_ring(way, j, u)
            total = total + arrived[way, j, within].astype(f32)
        out_ref[part] = total.astype(bf16)
    for copy in waits:
        copy.wait_send()


def fused_layer(
    ids, gates, lengths, gain, latents, queries, memory, hidden, w_uv, w_out, w_gate_t, w_up_t, w_down, n, slots, collective_id
):
    span_len, seqs, width = hidden.shape
    count = span_len * seqs
    lat_width = latents.shape[2]
    head_count = queries.shape[2] // lat_width
    here, _, value_dim = w_uv.shape
    mem_len = memory.shape[0]
    chips = n // 2
    steps = chips - 1
    inner = w_down.shape[0]
    key_total = n * span_len + count
    bf16, f32 = jnp.bfloat16, jnp.float32
    dma, vmem = pltpu.SemaphoreType.DMA, pltpu.VMEM
    row_count = head_count * span_len
    pieces = 2
    return pl.pallas_call(
        functools.partial(layer_kernel, n),
        out_shape=pltpu.VMEM((count, width), bf16),
        in_specs=[pl.BlockSpec(memory_space=pl.ANY)] * 13,
        out_specs=pl.BlockSpec(memory_space=pltpu.VMEM),
        scratch_shapes=[
            vmem(ids.shape, jnp.int32),
            vmem(gates.shape, bf16),
            vmem(lengths.shape, jnp.int32),
            vmem(gain.shape, bf16),
            vmem((count, lat_width), bf16),
            vmem((count, head_count * lat_width), bf16),
            vmem((seqs * mem_len, lat_width), bf16),
            vmem((count, width), bf16),
            vmem((count, width), bf16),
            vmem((seqs, key_total, lat_width), bf16),
            vmem((n, 16, count), bf16),
            vmem((seqs, row_count, lat_width), bf16),
            vmem((seqs, row_count, count), jnp.int32),
            vmem((seqs, row_count, count), f32),
            vmem((seqs, row_count, count), f32),
            vmem((seqs, row_count, lat_width), f32),
            vmem((row_count, lat_width), bf16),
            vmem((count, head_count * value_dim), bf16),
            vmem((head_count, lat_width, value_dim), bf16),
            vmem((head_count * value_dim, width), bf16),
            vmem((count, width), f32),
            vmem((chips, slots, 2 * count), bf16),
            vmem((n, slots, count), bf16),
            vmem((n, count, width), bf16),
            vmem((inner, width), bf16),
            vmem((inner, width), bf16),
            vmem((inner, width), bf16),
            vmem((2 * slots, inner), bf16),
            vmem((chips, count, width), bf16),
            vmem((chips, count, width), bf16),
            vmem((chips, count, width), bf16),
            vmem((2, steps, count // 2, width), bf16),
            dma((13,)),
            dma((pieces + 3,)),
            dma((pieces + 3,)),
            dma((pieces + 1,)),
            dma((pieces + 1,)),
            dma((2, 2, 2, steps)),
            dma((2, 2, 2, steps)),
            dma((2, 2, 2 * steps + 2)),
            dma((2, 2, 2 * steps + 2)),
            dma((2, 2, steps)),
            dma((2, 2, steps)),
            dma((2, 2 * steps + 2)),
            dma((2, 2 * steps + 2)),
            dma((1, 2, steps)),
            dma((1, 2, steps)),
            dma((1, 2 * steps + 2)),
            dma((1, 2 * steps + 2)),
            dma((2, 2, steps)),
            dma((2, 2, steps)),
            dma((chips,)),
            dma((chips,)),
        ],
        compiler_params=pltpu.CompilerParams(
            collective_id=collective_id, has_side_effects=True, vmem_limit_bytes=61000000
        ),
        cost_estimate=pl.CostEstimate(
            flops=6 * chips * slots * width * inner, bytes_accessed=32 * n * count * width, transcendentals=0
        ),
        name="layer_%d" % collective_id,
    )(ids, gates, lengths, gain, latents, queries, memory, hidden, w_uv, w_out, w_gate_t, w_up_t, w_down)


def round_share(depth, n):
    return depth // (2 * n) // 16 * 16


def layer_bytes(n, count, width, inner, slots, lat_width, head_count, value_dim):
    chips = n // 2
    key_total = (n + 2) * count // 2
    row_count = head_count * count // 2
    front = count * (1 + head_count) * lat_width + 2 * key_total * lat_width + 3 * row_count * lat_width
    front += 4 * row_count * lat_width + 12 * row_count * count + head_count * value_dim * (lat_width + width + count)
    back = n * count * width + 3 * width * inner + (4 * chips - 1) * count * width + 5 * count * width
    back += 4 * chips * slots * count + 2 * slots * inner
    return 2 * (front + back) + 8 * slots * inner * 2


def shards(
    hidden,
    queries,
    latents,
    mem_latents,
    lengths,
    ids,
    gates,
    norm_gain,
    w_uv,
    w_out,
    w_gate,
    w_up,
    w_down,
):
    f32, bf16 = jnp.float32, jnp.bfloat16
    local_len, seq_count, model_width = hidden.shape[1:]
    latent_dim = latents.shape[3]
    head_count = queries.shape[3] // latent_dim
    row_count = local_len * seq_count
    n = lax.axis_size("expert")
    dp_size = lax.axis_size("dp")
    me = lax.axis_index("expert")
    core = me % 2
    own_dp = lax.axis_index("dp")
    heads_here, _, value_dim = w_uv.shape
    top_count = ids.shape[3]
    ids_t = jnp.transpose(ids[0], (2, 1, 0)).reshape(top_count, row_count).astype(bf16)
    gates_t = jnp.transpose(gates[0], (2, 1, 0)).reshape(top_count, row_count)
    capacity = min(row_count, row_count * top_count // (n * w_gate.shape[0]) + 2)
    slots = -(-2 * capacity // 128) * 128
    fits = (
        dp_size == 2
        and w_gate.shape[0] == 1
        and n >= 8
        and top_count <= 8
        and seq_count == 2
        and row_count % 128 == 0
        and heads_here % 2 == 0
        and heads_here * value_dim % (64 * n // 4) == 0
        and round_share(heads_here * value_dim, n) >= 16
        and mem_latents.shape[1] <= row_count
        and layer_bytes(n, row_count, model_width, w_down.shape[1], slots, latent_dim, head_count, value_dim)
        < 60 * 1024 * 1024
    )
    if fits:
        out = fused_layer(
            jnp.transpose(ids[0], (2, 1, 0)), jnp.transpose(gates[0], (2, 1, 0)), lengths, norm_gain,
            latents[0], queries[0], mem_latents[0], hidden[0], w_uv, w_out,
            jnp.transpose(w_gate[0]), jnp.transpose(w_up[0]), w_down[0], n, slots, 4,
        )
        return out.reshape(1, local_len, seq_count, model_width)

    half_heads = heads_here // 2
    uv_half = lax.dynamic_slice_in_dim(w_uv, core * half_heads, half_heads, 0)
    out_half = lax.dynamic_slice_in_dim(
        w_out, core * half_heads * value_dim, half_heads * value_dim, 0
    )
    uv_groups, out_groups, starts = [w_uv], [w_out], [own_dp * heads_here]
    swap = [(i, i ^ 1) for i in range(n)]
    sizes = [heads_here]
    for shift in range(1, dp_size):
        turn = [(i, (i + shift) % dp_size) for i in range(dp_size)]
        source = (own_dp - shift + dp_size) % dp_size
        uv_far = lax.ppermute(uv_half, "dp", turn)
        out_far = lax.ppermute(out_half, "dp", turn)
        uv_near = lax.ppermute(uv_far, "expert", swap)
        out_near = lax.ppermute(out_far, "expert", swap)
        uv_groups += [uv_far, uv_near]
        out_groups += [out_far, out_near]
        starts += [
            source * heads_here + core * half_heads,
            source * heads_here + (1 - core) * half_heads,
        ]
        sizes += [half_heads, half_heads]

    latent_rows = jnp.transpose(latents[0], (1, 0, 2)).reshape(row_count, latent_dim)
    table = jnp.concatenate([ids_t, gates_t], axis=0).reshape(-1)
    table_rows = -(-table.shape[0] // (16 * latent_dim)) * 16
    table = jnp.pad(table, (0, table_rows * latent_dim - table.shape[0]))
    packed = jnp.concatenate([latent_rows, table.reshape(table_rows, latent_dim)], axis=0)
    all_rows = row_count + table_rows
    cut = (all_rows // 2 + 15) // 16 * 16
    gathered = ring_gather(packed, n, cut, 0)

    segment = gathered[:, :row_count].reshape(n, seq_count, local_len, latent_dim)
    segment = jnp.transpose(segment, (1, 0, 2, 3)).reshape(seq_count, n * local_len, latent_dim)
    memory = jnp.transpose(mem_latents[0], (1, 0, 2))
    mem_count = memory.shape[1]
    keys = jnp.concatenate([memory, segment], axis=1)
    query_rows = jnp.transpose(
        queries[0].reshape(local_len, seq_count, head_count, latent_dim), (1, 2, 0, 3)
    ).reshape(seq_count, head_count * local_len, latent_dim)
    scores = jnp.einsum("sql,sjl->sqj", query_rows, keys, preferred_element_type=f32) * score_scale
    key_pos = lax.broadcasted_iota(jnp.int32, scores.shape, 2) - mem_count
    own_pos = me * local_len + lax.broadcasted_iota(jnp.int32, scores.shape, 1) % local_len
    visible = (key_pos <= own_pos) & (key_pos < lengths[0][:, None, None])
    scores = jnp.where(visible | (key_pos < 0), scores, -jnp.inf)
    weights = jnp.exp(scores - jnp.max(scores, axis=2, keepdims=True))
    total = jnp.sum(weights, axis=2, keepdims=True)
    attended = jnp.einsum("sqj,sjl->sql", weights.astype(bf16), keys, preferred_element_type=f32)
    attended = (attended / total).astype(bf16)
    attended = attended.reshape(seq_count, head_count, local_len, latent_dim)

    attn_out = jnp.zeros((row_count, model_width), f32)
    for uv, out, start, size in zip(uv_groups, out_groups, starts, sizes):
        heads = lax.dynamic_slice_in_dim(attended, start, size, 1)
        values = jnp.einsum("shtl,hlv->sthv", heads, uv, preferred_element_type=f32).astype(bf16)
        attn_out = attn_out + jnp.dot(
            values.reshape(row_count, size * value_dim), out, preferred_element_type=f32
        )

    hidden_rows = jnp.transpose(hidden[0], (1, 0, 2)).reshape(row_count, model_width)
    residual = lax.optimization_barrier(hidden_rows).astype(f32) + attn_out
    mean_square = jnp.mean(residual * residual, axis=-1, keepdims=True)
    normed = (residual * lax.rsqrt(mean_square + norm_eps) * norm_gain.astype(f32)).astype(bf16)

    rows_all = ring_gather(normed, n, row_count // 2, 1)
    experts_here = w_gate.shape[0]
    expert_count = n * experts_here
    groups = n // 2
    wide = 2 * row_count
    slots = -(-2 * capacity // 16) * 16
    tables = gathered[:, row_count:].reshape(n, -1)[:, : 2 * top_count * row_count]
    tables = tables.reshape(groups, 2, 2, top_count, row_count)
    named = jnp.transpose(tables[:, :, 0], (2, 0, 1, 3)).reshape(top_count, groups, wide)
    scale = jnp.transpose(tables[:, :, 1], (2, 0, 1, 3)).reshape(top_count, groups, wide)
    rows_all = rows_all.reshape(groups, wide, model_width)
    steps = jnp.arange(wide, dtype=jnp.int32)
    earlier = (steps[:, None] < steps[None, :]).astype(bf16)
    made_rows, mixes = [], []
    for e in range(experts_here):
        matches = named == (me * experts_here + e).astype(bf16)
        hit = jnp.any(matches, axis=0)
        gate = jnp.sum(jnp.where(matches, scale.astype(f32), 0.0), axis=0)
        slot = jnp.dot(hit.astype(bf16), earlier, preferred_element_type=f32).astype(jnp.int32)
        slot = jnp.where(hit, slot, -1)
        chosen = slot[:, None, :] == jnp.arange(slots, dtype=jnp.int32)[None, :, None]
        placing = chosen.astype(bf16)
        slot_t = jnp.where(hit, slot, -1).reshape(n, row_count)
        chosen_t = slot_t[:, :, None] == jnp.arange(slots, dtype=jnp.int32)[None, None, :]
        mixes.append(jnp.where(chosen_t, gate.reshape(n, row_count)[:, :, None], 0.0).astype(bf16))
        picked = jnp.einsum("gct,gtd->gcd", placing, rows_all, preferred_element_type=f32)
        picked = picked.astype(bf16).reshape(groups * slots, model_width)
        gate_h = jnp.dot(picked, w_gate[e], preferred_element_type=f32)
        up_h = jnp.dot(picked, w_up[e], preferred_element_type=f32)
        act = (jax.nn.silu(gate_h) * up_h).astype(bf16)
        produced = jnp.dot(act, w_down[e], preferred_element_type=f32).astype(bf16)
        made_rows.append(produced.reshape(groups, slots, model_width))
    made_rows = made_rows[0] if experts_here == 1 else jnp.concatenate(made_rows, axis=1)
    mixing = mixes[0] if experts_here == 1 else jnp.concatenate(mixes, axis=2)
    routed = ring_reduce(made_rows, mixing, n, 2)
    layer_out = (residual + routed).astype(bf16).reshape(seq_count, local_len, model_width)
    return jnp.transpose(layer_out, (1, 0, 2))[None]


def solution(mesh):
    return jax.shard_map(
        shards,
        mesh=mesh,
        in_specs=(
            P("dp", "expert", None, None),
            P("dp", "expert", None, None),
            P("dp", "expert", None, None),
            P("dp", None, None, None),
            P("dp", None),
            P("dp", "expert", None, None),
            P("dp", "expert", None, None),
            P(),
            P("dp", None, None),
            P("dp", None),
            P("expert", None, None),
            P("expert", None, None),
            P("expert", None, None),
        ),
        out_specs=P("dp", "expert", None, None),
        check_vma=False,
    )
```

```python
import functools

import jax
import jax.numpy as jnp
from jax import lax
from jax.experimental import pallas as pl
from jax.experimental.pallas import tpu as pltpu
from jax.sharding import PartitionSpec as P

score_scale = 192.0 ** (-0.5)
norm_eps = 1e-06
MESH = pl.DeviceIdType.MESH


def ring_place(n):
    chips = n // 2
    depth = chips // 2
    me = lax.axis_index("expert")
    core = me % 2
    chip = me // 2
    row, col = chip // 2, chip % 2
    pos = col * row + (1 - col) * (chips - 1 - row)

    def device(offset, core_of):
        p = (pos + offset + chips) % chips
        q = p // depth
        r = (1 - q) * p + q * (chips - 1 - p)
        return (2 * r + 1 - q) * 2 + core_of

    return me, core, device


def greet(targets):
    barrier = pltpu.get_barrier_semaphore()
    for target in targets:
        pl.semaphore_signal(barrier, inc=1, device_id={"expert": target}, device_id_type=MESH)
    pl.semaphore_wait(barrier, len(targets))


def remote(src, dst, send_sem, recv_sem, target):
    return pltpu.make_async_remote_copy(
        src_ref=src,
        dst_ref=dst,
        send_sem=send_sem,
        recv_sem=recv_sem,
        device_id={"expert": target},
        device_id_type=MESH,
    )


def gather_kernel(n, cut, x_ref, out_ref, ring_send, ring_recv, pair_send, pair_recv, own_sem):
    chips = n // 2
    half_ring = chips // 2
    rows = x_ref.shape[0]
    last = chips - 2
    me, core, device = ring_place(n)
    partner = device(0, 1 - core)
    ahead = (device(1, core), device(-1, core))
    spans = (pl.ds(0, cut), pl.ds(cut, rows - cut))
    greet((ahead[0], ahead[1], partner))

    def arrival(way, j):
        dist, half = (half_ring, way) if j == last else (j // 2 + 1, j % 2)
        return device(-dist if way == 0 else dist, core), spans[half]

    waits = []
    for way in (0, 1):
        for j in (0, 1):
            if j > last:
                continue
            if j == last and half_ring == 1:
                span = spans[way]
            else:
                span = spans[j]
            copy = remote(
                x_ref.at[span], out_ref.at[me, span],
                ring_send.at[way, j], ring_recv.at[way, j], ahead[way],
            )
            copy.start()
            waits.append(copy)
    share = remote(x_ref, out_ref.at[me], pair_send.at[2 * last + 2], pair_recv.at[2 * last + 2], partner)
    share.start()
    waits.append(share)
    keep = pltpu.make_async_copy(x_ref, out_ref.at[me], own_sem)
    keep.start()

    for j in range(last + 1):
        for way in (0, 1):
            slot, span = arrival(way, j)
            piece = out_ref.at[slot, span]
            remote(piece, piece, ring_send.at[way, j], ring_recv.at[way, j], ahead[way]).wait_recv()
            onward = j + 2
            if j >= last - 2 and j < last:
                onward = last if j == last - 2 + way else None
            if j == last:
                onward = None
            if onward is not None:
                copy = remote(piece, piece, ring_send.at[way, onward], ring_recv.at[way, onward], ahead[way])
                copy.start()
                waits.append(copy)
            index = 2 * j + way
            copy = remote(piece, piece, pair_send.at[index], pair_recv.at[index], partner)
            copy.start()
            waits.append(copy)

    for j in range(last + 1):
        for way in (0, 1):
            dist, half = (half_ring, way) if j == last else (j // 2 + 1, j % 2)
            slot = device(-dist if way == 0 else dist, 1 - core)
            piece = out_ref.at[slot, spans[half]]
            index = 2 * j + way
            remote(piece, piece, pair_send.at[index], pair_recv.at[index], partner).wait_recv()
    other = out_ref.at[partner]
    remote(other, other, pair_send.at[2 * last + 2], pair_recv.at[2 * last + 2], partner).wait_recv()
    for copy in waits:
        copy.wait_send()
    keep.wait()


def ring_gather(x, n, cut, collective_id):
    rows, cols = x.shape
    steps = n // 2 - 1
    return pl.pallas_call(
        functools.partial(gather_kernel, n, cut),
        out_shape=jax.ShapeDtypeStruct((n, rows, cols), x.dtype),
        in_specs=[pl.BlockSpec(memory_space=pltpu.VMEM)],
        out_specs=pl.BlockSpec(memory_space=pl.ANY),
        scratch_shapes=[
            pltpu.SemaphoreType.DMA((2, steps)),
            pltpu.SemaphoreType.DMA((2, steps)),
            pltpu.SemaphoreType.DMA((2 * steps + 1,)),
            pltpu.SemaphoreType.DMA((2 * steps + 1,)),
            pltpu.SemaphoreType.DMA,
        ],
        compiler_params=pltpu.CompilerParams(collective_id=collective_id, has_side_effects=True),
        cost_estimate=pl.CostEstimate(flops=0, bytes_accessed=16 * n * rows * cols, transcendentals=0),
        name="ring_gather_%d" % collective_id,
    )(x)


def reduce_kernel(
    n, rows_ref, mix_ref, out_ref, mine, paired, give, arrived, ring_send, ring_recv, pair_send, pair_recv
):
    chips = n // 2
    half_ring = chips // 2
    half = mine.shape[1] // 2
    last = chips - 2
    me, core, device = ring_place(n)
    partner = device(0, 1 - core)
    ahead = (device(1, core), device(-1, core))
    greet((ahead[0], ahead[1], partner))

    order = [half_ring]
    for k in range(half_ring - 1, 0, -1):
        order += [k, chips - k]
    order.append(0)
    depth = give.shape[0]
    shares, made, seen = {}, [], set()

    def weigh(k, core_of):
        dest = device(k, core_of)
        return jnp.dot(
            mix_ref[dest], rows_ref[dest // 2], preferred_element_type=jnp.float32
        ).astype(mine.dtype)

    def make():
        k = order[len(made)]
        slot = len(made) % depth
        if len(made) >= depth:
            shares[order[len(made) - depth]].wait_send()
        give[slot] = weigh(k, 1 - core)
        shares[k] = remote(give.at[slot], paired.at[k], pair_send.at[k], pair_recv.at[k], partner)
        shares[k].start()
        mine[k] = weigh(k, core)
        made.append(k)

    def bring(k):
        while k not in made or (len(made) < chips and len(made) < order.index(k) + 3):
            make()
        if k not in seen:
            seen.add(k)
            shares[k].wait_recv()

    def index_of(dist, h):
        return 0 if dist == half_ring else 1 + 2 * (half_ring - 1 - dist) + h

    def await_ring(way, j):
        piece = arrived.at[way, j]
        remote(piece, piece, ring_send.at[way, j], ring_recv.at[way, j], ahead[way]).wait_recv()

    sends = []
    for dist in range(half_ring, 0, -1):
        for turn in (0, 1):
            for way in (0, 1):
                if dist == half_ring:
                    if turn == 1:
                        continue
                    h = way
                elif dist == half_ring - 1:
                    h = 1 - way if turn == 0 else way
                else:
                    h = turn
                k = dist if way == 0 else chips - dist
                bring(k)
                span = pl.ds(h * half, half)
                total = mine[k, span].astype(jnp.float32) + paired[k, span].astype(jnp.float32)
                has_prior = dist < half_ring - 1 or (dist == half_ring - 1 and h == way)
                if has_prior:
                    j = index_of(dist + 1, h)
                    await_ring(way, j)
                    total = total + arrived[way, j].astype(jnp.float32)
                mine[k, span] = total.astype(mine.dtype)
                j = index_of(dist, h)
                copy = remote(
                    mine.at[k, span], arrived.at[way, j],
                    ring_send.at[way, j], ring_recv.at[way, j], ahead[way],
                )
                copy.start()
                sends.append(copy)
    bring(0)
    for h in (0, 1):
        span = pl.ds(h * half, half)
        total = mine[0, span].astype(jnp.float32) + paired[0, span].astype(jnp.float32)
        for way in (0, 1):
            j = index_of(1, h)
            await_ring(way, j)
            total = total + arrived[way, j].astype(jnp.float32)
        out_ref[span] = total
    for copy in sends:
        copy.wait_send()
    for k in order[chips - min(depth, chips) :]:
        shares[k].wait_send()


def ring_reduce(rows_in, mix, n, collective_id):
    rows = mix.shape[1]
    cols = rows_in.shape[2]
    chips = n // 2
    dtype = rows_in.dtype
    return pl.pallas_call(
        functools.partial(reduce_kernel, n),
        out_shape=jax.ShapeDtypeStruct((rows, cols), jnp.float32),
        in_specs=[pl.BlockSpec(memory_space=pltpu.VMEM)] * 2,
        out_specs=pl.BlockSpec(memory_space=pltpu.VMEM),
        scratch_shapes=[
            pltpu.VMEM((chips, rows, cols), dtype),
            pltpu.VMEM((chips, rows, cols), dtype),
            pltpu.VMEM((min(4, chips), rows, cols), dtype),
            pltpu.VMEM((2, chips - 1, rows // 2, cols), dtype),
            pltpu.SemaphoreType.DMA((2, chips - 1)),
            pltpu.SemaphoreType.DMA((2, chips - 1)),
            pltpu.SemaphoreType.DMA((chips,)),
            pltpu.SemaphoreType.DMA((chips,)),
        ],
        compiler_params=pltpu.CompilerParams(
            collective_id=collective_id, has_side_effects=True, vmem_limit_bytes=62 * 1024 * 1024
        ),
        cost_estimate=pl.CostEstimate(
            flops=2 * mix.size * cols, bytes_accessed=16 * n * rows * cols, transcendentals=0
        ),
        name="ring_reduce_%d" % collective_id,
    )(rows_in, mix)


def layer_kernel(
    n,
    ids_hbm, gates_hbm, limit_hbm, gain_hbm,
    latent_hbm, query_hbm, memory_hbm, hidden_hbm, uv_hbm, wout_hbm, gate_hbm, up_hbm, down_hbm,
    out_ref,
    ids, gates, limit, gain,
    latent, query, memory, hidden, parted_hidden, keys, tables, heads, bound, peak, mass, blend,
    attended, values, w_uv, w_out, kept,
    place, mix, rows, w_gate, w_up, w_down, act, mine, paired, give, arrived,
    load_sem, far_send, far_recv, near_send, near_recv,
    key_send, key_recv, key_swap_send, key_swap_recv,
    row_send, row_recv, row_swap_send, row_swap_recv,
    round_send, round_recv, round_swap_send, round_swap_recv,
    ring_send, ring_recv, pair_send, pair_recv,
):
    f32, bf16 = jnp.float32, jnp.bfloat16
    chips = n // 2
    half_ring = chips // 2
    last = chips - 2
    count, width = kept.shape
    seqs, span_len = 2, count // 2
    lat_width = latent.shape[1]
    mem_len = memory.shape[0] // 2
    head_count = query.shape[1] // lat_width
    mem_at = n * span_len
    key_total = keys.shape[1]
    top_count = ids.shape[0]
    here = uv_hbm.shape[0]
    value_dim = uv_hbm.shape[2]
    half_here = here // 2
    slots = place.shape[1]
    me, core, device = ring_place(n)
    own_dp = lax.axis_index("dp")
    far_dp = 1 - own_dp
    partner = device(0, 1 - core)
    ahead = (device(1, core), device(-1, core))
    spans = (pl.ds(0, span_len), pl.ds(span_len, span_len))

    loads = [
        pltpu.make_async_copy(src, dst, load_sem.at[i])
        for i, (src, dst) in enumerate((
            (latent_hbm.reshape(count, lat_width), latent),
            (ids_hbm, ids),
            (gates_hbm, gates),
            (limit_hbm, limit),
            (gain_hbm, gain),
            (wout_hbm, w_out.at[pl.ds(own_dp * here * value_dim, here * value_dim)]),
            (uv_hbm, w_uv.at[pl.ds(own_dp * here, here)]),
            (query_hbm.reshape(query.shape), query),
            (memory_hbm.reshape(memory.shape), memory),
            (hidden_hbm.reshape(count, width), hidden),
            (gate_hbm, w_gate),
            (up_hbm, w_up),
            (down_hbm, w_down),
        ))
    ]
    for load in loads:
        load.start()
    waits = []

    def send(copy):
        copy.start()
        waits.append(copy)

    barrier = pltpu.get_barrier_semaphore()
    for target in (ahead[0], ahead[1], partner):
        pl.semaphore_signal(barrier, inc=1, device_id={"expert": target}, device_id_type=MESH)
    pl.semaphore_signal(barrier, inc=1, device_id={"dp": far_dp}, device_id_type=MESH)
    def uv_piece(owner, of_core):
        return pl.ds(owner * here + of_core * half_here, half_here)

    depth = here * value_dim
    round_rows = round_share(depth, n)
    pieces = far_send.shape[0] - 3
    out_rows = (depth - n * round_rows) // (2 * pieces)

    def out_piece(first, of_core, i):
        at = first + n * round_rows + (of_core * pieces + i) * out_rows
        return pl.ds(pl.multiple_of(at, 8), out_rows)

    def round_piece(first, slot, h):
        size = -(-round_rows // 16) * 8
        return pl.ds(pl.multiple_of(first + slot * round_rows + h * size, 8), size if h == 0 else round_rows - size)

    def across(src, dst, i):
        return pltpu.make_async_remote_copy(
            src_ref=src, dst_ref=dst, send_sem=far_send.at[i], recv_sem=far_recv.at[i],
            device_id={"dp": far_dp}, device_id_type=MESH,
        )

    def far_ref(i, of_core):
        return w_uv.at[uv_piece(far_dp, of_core)] if i == 0 else w_out.at[out_piece(far_dp * depth, of_core, i - 1)]

    def pass_far(i):
        piece = far_ref(i, core)
        across(piece, piece, i).wait_recv()
        send(remote(piece, piece, near_send.at[i], near_recv.at[i], partner))

    def await_near(i):
        piece = far_ref(i, 1 - core)
        remote(piece, piece, near_send.at[i], near_recv.at[i], partner).wait_recv()

    def step_of(way, j):
        return (half_ring, way) if j == last else (j // 2 + 1, j % 2)

    def offset(way, dist):
        return dist if way == 0 else chips - dist

    def gather(parts, sends, recvs, swap_sends, swap_recvs):
        own = 2 * last + 2

        def start(h):
            for way in (0, 1):
                for i, ref in enumerate(parts(me, h)):
                    send(remote(ref, ref, sends.at[i, way, h], recvs.at[i, way, h], ahead[way]))
            for i, ref in enumerate(parts(me, h)):
                send(remote(ref, ref, swap_sends.at[i, own + h], swap_recvs.at[i, own + h], partner))

        def near_own():
            for h in (0, 1):
                for i, ref in enumerate(parts(partner, h)):
                    remote(ref, ref, swap_sends.at[i, own + h], swap_recvs.at[i, own + h], partner).wait_recv()

        def hop(j):
            onward = [j + 2, j + 2]
            if last - 2 <= j < last:
                onward = [last if j == last - 2 + way else None for way in (0, 1)]
            if j == last:
                onward = [None, None]
            found = []
            for way in (0, 1):
                dist, h = step_of(way, j)
                found += [(i, way, ref) for i, ref in enumerate(parts(device(-dist if way == 0 else dist, core), h))]
            for i, way, ref in sorted(found, key=lambda piece: piece[:2]):
                remote(ref, ref, sends.at[i, way, j], recvs.at[i, way, j], ahead[way]).wait_recv()
                if onward[way] is not None:
                    k = onward[way]
                    send(remote(ref, ref, sends.at[i, way, k], recvs.at[i, way, k], ahead[way]))
                k = 2 * j + way
                send(remote(ref, ref, swap_sends.at[i, k], swap_recvs.at[i, k], partner))

        def near(j):
            for way in (0, 1):
                dist, h = step_of(way, j)
                k = 2 * j + way
                for i, ref in enumerate(parts(device(-dist if way == 0 else dist, 1 - core), h)):
                    remote(ref, ref, swap_sends.at[i, k], swap_recvs.at[i, k], partner).wait_recv()

        return start, near_own, hop, near

    def split_of(total):
        to = lax.broadcasted_iota(jnp.int32, (total, total), 0)
        at = lax.broadcasted_iota(jnp.int32, (total, total), 1)
        return (to == at % 2 * (total // 2) + at // 2).astype(f32).astype(bf16)

    split = split_of(count)
    to = lax.broadcasted_iota(jnp.int32, (count, count), 0)
    at = lax.broadcasted_iota(jnp.int32, (count, count), 1)
    weave = (at == to % 2 * span_len + to // 2).astype(f32).astype(bf16)

    def place_of(slot, first, size):
        return pl.ds(pl.multiple_of(slot * span_len + first, size), size)

    sub = span_len // 2

    def key_parts(s):
        def parts(slot, h):
            found = [keys.at[s, place_of(slot, h * sub, sub)]]
            return found + ([tables.at[slot]] if s == 0 and h == 0 else [])

        return gather(parts, key_send.at[s], key_recv.at[s], key_swap_send.at[s], key_swap_recv.at[s])

    streams = [key_parts(s) for s in range(seqs)]
    for load in loads[:5]:
        load.wait()
    lines = []
    for source, filler in ((ids, 255.0), (gates, 0.0)):
        taken = source[...].astype(f32)
        lines.append(jnp.concatenate([taken[:, s, :] for s in range(seqs)], axis=1))
        if top_count < 8:
            lines.append(jnp.full((8 - top_count, count), filler, f32))
    tables[me] = jnp.concatenate(lines, axis=0).astype(bf16)
    for s in range(seqs):
        keys[s, place_of(me, 0, span_len)] = jnp.dot(
            split[s * span_len : (s + 1) * span_len], latent[...], preferred_element_type=f32
        ).astype(bf16)
    pl.semaphore_wait(barrier, 4)
    loads[5].wait()
    for h in (0, 1):
        piece = w_out.at[round_piece(own_dp * depth, me, h)]
        send(across(piece, piece, pieces + 1 + h))
    loads[6].wait()
    piece = w_uv.at[uv_piece(own_dp, core)]
    send(across(piece, piece, 0))
    for i in range(pieces):
        piece = w_out.at[out_piece(own_dp * depth, core, i)]
        send(across(piece, piece, i + 1))
    for s in range(seqs):
        for h in (0, 1):
            streams[s][0](h)

    loads[7].wait()
    for s in range(seqs):
        parted = jnp.dot(
            split[s * span_len : (s + 1) * span_len], query[...], preferred_element_type=f32
        ).astype(bf16)
        for h in range(head_count):
            heads[s, pl.ds(h * span_len, span_len)] = parted[:, h * lat_width : (h + 1) * lat_width]
    loads[8].wait()
    parted = jnp.dot(split_of(2 * mem_len), memory[...], preferred_element_type=f32).astype(bf16)
    lanes = 2 * span_len
    row_count = head_count * span_len
    lane = lax.broadcasted_iota(jnp.int32, (row_count, lanes), 1)
    own_pos = me * span_len + lax.broadcasted_iota(jnp.int32, (row_count, lanes), 0) % span_len
    along = (((1,), (1,)), ((), ()))
    scale = score_scale * 1.4426950408889634
    for s in range(seqs):
        keys[s, pl.ds(mem_at, mem_len)] = parted[s * mem_len : (s + 1) * mem_len]
        keys[s, pl.ds(mem_at + mem_len, key_total - mem_at - mem_len)] = jnp.zeros(
            (key_total - mem_at - mem_len, lat_width), bf16
        )
        bound[s] = jnp.minimum(own_pos, limit[:, s : s + 1] - 1) - lane

    def wide(x, times):
        return x if times == 1 else jnp.concatenate([x] * times, axis=1)

    def attend(ks, chosen_seqs, opening=False):
        firsts = [pl.multiple_of(device(k, 0) * span_len, lanes) for k in ks]
        for s in chosen_seqs:
            held = [keys[s, pl.ds(first, lanes)] for first in firsts]
            seen_keys = [first <= bound[s] for first in firsts]
            if opening:
                held.append(keys[s, pl.ds(mem_at, lanes)])
                seen_keys.append(lane < mem_len)
            held = held[0] if len(held) == 1 else jnp.concatenate(held, axis=0)
            score = lax.dot_general(heads[s], held, along, preferred_element_type=f32)
            parts = [
                jnp.where(visible, score[:, i * lanes : (i + 1) * lanes], -jnp.inf)
                for i, visible in enumerate(seen_keys)
            ]
            top = functools.reduce(jnp.maximum, parts)
            top = jnp.broadcast_to(jnp.max(top, axis=1, keepdims=True), top.shape)
            if not opening:
                before = peak[s]
                top = jnp.maximum(before, top)
                fade = jnp.exp2((before - top) * scale)
            parts = [jnp.exp2((part - top) * scale) for part in parts]
            added = functools.reduce(jnp.add, parts)
            mass[s] = added if opening else mass[s] * fade + added
            peak[s] = top
            weight = parts[0] if len(parts) == 1 else jnp.concatenate(parts, axis=1)
            more = jnp.dot(weight.astype(bf16), held, preferred_element_type=f32)
            blend[s] = more if opening else blend[s] * wide(fade, lat_width // lanes) + more

    def round_parts(slot, h):
        return [w_out.at[round_piece(far_dp * depth, slot, h)]]

    round_start, round_near_own, round_hop, round_near = gather(
        round_parts, round_send, round_recv, round_swap_send, round_swap_recv
    )
    def steps_at(dist):
        return (last,) if dist == half_ring else (2 * dist - 2, 2 * dist - 1)

    def at_dist(dist):
        return [half_ring] if dist == half_ring else [dist, chips - dist]

    def hop_all(stream, dist):
        for j in steps_at(dist):
            stream[2](j)

    def use_keys(chosen_seqs, dist):
        for s in chosen_seqs:
            for j in steps_at(dist):
                streams[s][3](j)
        attend(at_dist(dist), chosen_seqs)

    rounds = (round_start, round_near_own, round_hop, round_near)
    for h in (0, 1):
        piece = w_out.at[round_piece(far_dp * depth, me, h)]
        across(piece, piece, pieces + 1 + h).wait_recv()
        round_start(h)
    for dist in range(1, half_ring):
        if dist > 1:
            hop_all(rounds, dist - 1)
        for s in range(seqs):
            hop_all(streams[s], dist)
        if dist == 1:
            for s in range(seqs):
                streams[s][1]()
            attend([0], range(seqs), True)
            loads[9].wait()
            parted_hidden[...] = jnp.dot(split, hidden[...], preferred_element_type=f32).astype(bf16)
        else:
            use_keys(range(seqs), dist - 1)
    pass_far(0)
    hop_all(rounds, half_ring - 1)
    use_keys(range(seqs), half_ring - 1)
    for s in range(seqs):
        hop_all(streams[s], half_ring)
    pass_far(1)
    hop_all(rounds, half_ring)
    use_keys([0], half_ring)
    for i in range(2, pieces + 1):
        pass_far(i)

    def row_parts(slot, h):
        return [rows.at[slot, pl.ds(h * span_len + i * sub, sub)] for i in (0, 1)]

    row_start, row_near_own, row_hop, row_near = gather(row_parts, row_send, row_recv, row_swap_send, row_swap_recv)
    await_near(0)
    near_cols = pl.ds(pl.multiple_of(own_dp * depth, depth), depth)
    far_cols = pl.ds(pl.multiple_of(far_dp * depth, depth), depth)
    for s in range(seqs):
        if s == 1:
            use_keys([1], half_ring)
        total = jnp.sum(mass[s], axis=1, keepdims=True)
        attended[...] = (blend[s] / total).astype(bf16)
        for h in range(head_count):
            values[spans[s], pl.ds(h * value_dim, value_dim)] = jnp.dot(
                attended[pl.ds(h * span_len, span_len)], w_uv[h], preferred_element_type=f32
            ).astype(bf16)
        residual = parted_hidden[spans[s]].astype(f32) + jnp.dot(
            values[spans[s], near_cols], w_out[near_cols], preferred_element_type=f32
        )
        if s == 0:
            round_near_own()
            for i in range(last + 1):
                round_near(i)
            for i in range(1, pieces + 1):
                await_near(i)
        residual = residual + jnp.dot(values[spans[s], far_cols], w_out[far_cols], preferred_element_type=f32)
        mean_square = jnp.mean(residual * residual, axis=1, keepdims=True)
        normed = residual * lax.rsqrt(mean_square + norm_eps) * gain[...].astype(f32)
        rows[me, spans[s]] = normed.astype(bf16)
        row_start(s)

    woven = jnp.dot(weave, values[...], preferred_element_type=f32).astype(bf16)
    kept[...] = (
        hidden[...].astype(f32)
        + jnp.dot(woven[:, :depth], w_out[pl.ds(0, depth)], preferred_element_type=f32)
        + jnp.dot(woven[:, depth:], w_out[pl.ds(depth, depth)], preferred_element_type=f32)
    )
    hits, scales = [], []
    own_id = me.astype(f32)
    for c in range(chips):
        pair = jnp.concatenate([tables[2 * c], tables[2 * c + 1]], axis=1).astype(f32)
        matches = pair[:8] == own_id
        hits.append(jnp.max(jnp.where(matches, 1.0, 0.0), axis=0, keepdims=True))
        scales.append(jnp.sum(jnp.where(matches, pair[8:], 0.0), axis=0, keepdims=True))
    hits = jnp.concatenate(hits, axis=0)
    to = lax.broadcasted_iota(jnp.int32, (2 * count, 2 * count), 0)
    at = lax.broadcasted_iota(jnp.int32, (2 * count, 2 * count), 1)
    earlier = (to < at).astype(f32).astype(bf16)
    ranks = jnp.dot(hits.astype(bf16), earlier, preferred_element_type=f32)
    ranks = jnp.where(hits > 0.5, ranks, -1.0)
    slot_id = lax.broadcasted_iota(jnp.int32, (slots, 2 * count), 0).astype(f32)
    for c in range(chips):
        chosen = slot_id == ranks[c : c + 1]
        place[c] = jnp.where(chosen, 1.0, 0.0).astype(bf16)
        weighed = jnp.where(chosen, scales[c], 0.0).astype(bf16)
        for i in (0, 1):
            own_part = weighed[:, i * count : (i + 1) * count]
            mix[2 * c + i] = jnp.dot(own_part, split, preferred_element_type=f32).astype(bf16)

    def start_experts(ks):
        picked = []
        for k in ks:
            first = device(k, 0)
            held = rows[pl.ds(first, 2)].reshape(2 * count, width)
            picked.append(jnp.dot(place[first // 2], held, preferred_element_type=f32).astype(bf16))
        picked = picked[0] if len(ks) == 1 else jnp.concatenate(picked, axis=0)
        gate_h = lax.dot_general(picked, w_gate[...], along, preferred_element_type=f32)
        up_h = lax.dot_general(picked, w_up[...], along, preferred_element_type=f32)
        act[pl.ds(0, len(ks) * slots)] = (gate_h / (1.0 + jnp.exp(-gate_h)) * up_h).astype(bf16)

    shares = {}
    down = (((0,), (0,)), ((), ()))

    def end_experts(ks):
        made = jnp.dot(act[pl.ds(0, len(ks) * slots)], w_down[...], preferred_element_type=f32).astype(bf16)
        for i, k in enumerate(ks):
            part = made[i * slots : (i + 1) * slots]
            give[k] = lax.dot_general(mix[device(k, 1 - core)], part, down, preferred_element_type=f32).astype(bf16)
            shares[k] = remote(give.at[k], paired.at[k], pair_send.at[k], pair_recv.at[k], partner)
            send(shares[k])
            mine[k] = lax.dot_general(mix[device(k, core)], part, down, preferred_element_type=f32).astype(bf16)

    seen = set()

    def bring(k):
        if k not in seen:
            seen.add(k)
            shares[k].wait_recv()

    def index_of(dist, h):
        return 0 if dist == half_ring else 1 + 2 * (half_ring - 1 - dist) + h

    def await_ring(way, j, u):
        piece = arrived.at[way, j, pl.ds(u * sub, sub)]
        remote(piece, piece, ring_send.at[u, way, j], ring_recv.at[u, way, j], ahead[way]).wait_recv()

    def advance(dist, chain):
        for u in (0, 1):
            for way in (0, 1):
                h = way if chain == 0 else 1 - way
                k = offset(way, dist)
                bring(k)
                part, within = pl.ds(h * span_len + u * sub, sub), pl.ds(u * sub, sub)
                total = mine[k, part].astype(f32) + paired[k, part].astype(f32)
                if dist < half_ring - chain:
                    j = index_of(dist + 1, h)
                    await_ring(way, j, u)
                    total = total + arrived[way, j, within].astype(f32)
                mine[k, part] = total.astype(bf16)
                j = index_of(dist, h)
                send(remote(
                    mine.at[k, part], arrived.at[way, j, within],
                    ring_send.at[u, way, j], ring_recv.at[u, way, j], ahead[way],
                ))

    row_near_own()
    for load in loads[10:]:
        load.wait()
    start_experts([0])
    end_experts([0])

    tasks = []
    for j in range(last + 1):
        if j < last:
            row_hop(j)
        if j % 2 == 1 or j == last:
            for i in (j - 1, j) if j % 2 == 1 else (j,):
                row_near(i)
            dist = step_of(0, j)[0]
            ks = [half_ring] if j == last else [dist, chips - dist]
            tasks += [functools.partial(start_experts, ks), functools.partial(end_experts, ks)]
        for _ in range(min(len(tasks), 1 if j < last - 1 else len(tasks))):
            tasks.pop(0)()
        if j == last - 1:
            row_hop(last)
            advance(half_ring - 1, 1)

    advance(half_ring, 0)
    for dist in range(half_ring - 2, 0, -1):
        advance(dist, 1)
        advance(dist + 1, 0)
    advance(1, 0)

    bring(0)
    for u, h in ((0, 0), (0, 1), (1, 0), (1, 1)):
        part, within = pl.ds(h * span_len + u * sub, sub), pl.ds(u * sub, sub)
        total = kept[part] + mine[0, part].astype(f32) + paired[0, part].astype(f32)
        for way in (0, 1):
            j = index_of(1, h)
            await_ring(way, j, u)
            total = total + arrived[way, j, within].astype(f32)
        out_ref[part] = total.astype(bf16)
    for copy in waits:
        copy.wait_send()


def fused_layer(
    ids, gates, lengths, gain, latents, queries, memory, hidden, w_uv, w_out, w_gate_t, w_up_t, w_down, n, slots, collective_id
):
    span_len, seqs, width = hidden.shape
    count = span_len * seqs
    lat_width = latents.shape[2]
    head_count = queries.shape[2] // lat_width
    here, _, value_dim = w_uv.shape
    mem_len = memory.shape[0]
    chips = n // 2
    steps = chips - 1
    inner = w_down.shape[0]
    key_total = n * span_len + count
    bf16, f32 = jnp.bfloat16, jnp.float32
    dma, vmem = pltpu.SemaphoreType.DMA, pltpu.VMEM
    row_count = head_count * span_len
    pieces = 2
    return pl.pallas_call(
        functools.partial(layer_kernel, n),
        out_shape=pltpu.VMEM((count, width), bf16),
        in_specs=[pl.BlockSpec(memory_space=pl.ANY)] * 13,
        out_specs=pl.BlockSpec(memory_space=pltpu.VMEM),
        scratch_shapes=[
            vmem(ids.shape, jnp.int32),
            vmem(gates.shape, bf16),
            vmem(lengths.shape, jnp.int32),
            vmem(gain.shape, bf16),
            vmem((count, lat_width), bf16),
            vmem((count, head_count * lat_width), bf16),
            vmem((seqs * mem_len, lat_width), bf16),
            vmem((count, width), bf16),
            vmem((count, width), bf16),
            vmem((seqs, key_total, lat_width), bf16),
            vmem((n, 16, count), bf16),
            vmem((seqs, row_count, lat_width), bf16),
            vmem((seqs, row_count, count), jnp.int32),
            vmem((seqs, row_count, count), f32),
            vmem((seqs, row_count, count), f32),
            vmem((seqs, row_count, lat_width), f32),
            vmem((row_count, lat_width), bf16),
            vmem((count, head_count * value_dim), bf16),
            vmem((head_count, lat_width, value_dim), bf16),
            vmem((head_count * value_dim, width), bf16),
            vmem((count, width), f32),
            vmem((chips, slots, 2 * count), bf16),
            vmem((n, slots, count), bf16),
            vmem((n, count, width), bf16),
            vmem((inner, width), bf16),
            vmem((inner, width), bf16),
            vmem((inner, width), bf16),
            vmem((2 * slots, inner), bf16),
            vmem((chips, count, width), bf16),
            vmem((chips, count, width), bf16),
            vmem((chips, count, width), bf16),
            vmem((2, steps, count // 2, width), bf16),
            dma((13,)),
            dma((pieces + 3,)),
            dma((pieces + 3,)),
            dma((pieces + 1,)),
            dma((pieces + 1,)),
            dma((2, 2, 2, steps)),
            dma((2, 2, 2, steps)),
            dma((2, 2, 2 * steps + 2)),
            dma((2, 2, 2 * steps + 2)),
            dma((2, 2, steps)),
            dma((2, 2, steps)),
            dma((2, 2 * steps + 2)),
            dma((2, 2 * steps + 2)),
            dma((1, 2, steps)),
            dma((1, 2, steps)),
            dma((1, 2 * steps + 2)),
            dma((1, 2 * steps + 2)),
            dma((2, 2, steps)),
            dma((2, 2, steps)),
            dma((chips,)),
            dma((chips,)),
        ],
        compiler_params=pltpu.CompilerParams(
            collective_id=collective_id, has_side_effects=True, vmem_limit_bytes=61000000
        ),
        cost_estimate=pl.CostEstimate(
            flops=6 * chips * slots * width * inner, bytes_accessed=32 * n * count * width, transcendentals=0
        ),
        name="layer_%d" % collective_id,
    )(ids, gates, lengths, gain, latents, queries, memory, hidden, w_uv, w_out, w_gate_t, w_up_t, w_down)


def round_share(depth, n):
    return depth // (2 * n) // 16 * 16


def layer_bytes(n, count, width, inner, slots, lat_width, head_count, value_dim):
    chips = n // 2
    key_total = (n + 2) * count // 2
    row_count = head_count * count // 2
    front = count * (1 + head_count) * lat_width + 2 * key_total * lat_width + 3 * row_count * lat_width
    front += 4 * row_count * lat_width + 12 * row_count * count + head_count * value_dim * (lat_width + width + count)
    back = n * count * width + 3 * width * inner + (4 * chips - 1) * count * width + 5 * count * width
    back += 4 * chips * slots * count + 2 * slots * inner
    return 2 * (front + back) + 8 * slots * inner * 2


def shards(
    hidden,
    queries,
    latents,
    mem_latents,
    lengths,
    ids,
    gates,
    norm_gain,
    w_uv,
    w_out,
    w_gate,
    w_up,
    w_down,
):
    f32, bf16 = jnp.float32, jnp.bfloat16
    local_len, seq_count, model_width = hidden.shape[1:]
    latent_dim = latents.shape[3]
    head_count = queries.shape[3] // latent_dim
    row_count = local_len * seq_count
    n = lax.axis_size("expert")
    dp_size = lax.axis_size("dp")
    me = lax.axis_index("expert")
    core = me % 2
    own_dp = lax.axis_index("dp")
    heads_here, _, value_dim = w_uv.shape
    top_count = ids.shape[3]
    ids_t = jnp.transpose(ids[0], (2, 1, 0)).reshape(top_count, row_count).astype(bf16)
    gates_t = jnp.transpose(gates[0], (2, 1, 0)).reshape(top_count, row_count)
    capacity = min(row_count, row_count * top_count // (n * w_gate.shape[0]) + 2)
    slots = -(-2 * capacity // 128) * 128
    fits = (
        dp_size == 2
        and w_gate.shape[0] == 1
        and n >= 8
        and top_count <= 8
        and seq_count == 2
        and row_count % 128 == 0
        and heads_here % 2 == 0
        and heads_here * value_dim % (64 * n // 4) == 0
        and round_share(heads_here * value_dim, n) >= 16
        and mem_latents.shape[1] <= row_count
        and layer_bytes(n, row_count, model_width, w_down.shape[1], slots, latent_dim, head_count, value_dim)
        < 60 * 1024 * 1024
    )
    if fits:
        out = fused_layer(
            jnp.transpose(ids[0], (2, 1, 0)), jnp.transpose(gates[0], (2, 1, 0)), lengths, norm_gain,
            latents[0], queries[0], mem_latents[0], hidden[0], w_uv, w_out,
            jnp.transpose(w_gate[0]), jnp.transpose(w_up[0]), w_down[0], n, slots, 4,
        )
        return out.reshape(1, local_len, seq_count, model_width)

    half_heads = heads_here // 2
    uv_half = lax.dynamic_slice_in_dim(w_uv, core * half_heads, half_heads, 0)
    out_half = lax.dynamic_slice_in_dim(
        w_out, core * half_heads * value_dim, half_heads * value_dim, 0
    )
    uv_groups, out_groups, starts = [w_uv], [w_out], [own_dp * heads_here]
    swap = [(i, i ^ 1) for i in range(n)]
    sizes = [heads_here]
    for shift in range(1, dp_size):
        turn = [(i, (i + shift) % dp_size) for i in range(dp_size)]
        source = (own_dp - shift + dp_size) % dp_size
        uv_far = lax.ppermute(uv_half, "dp", turn)
        out_far = lax.ppermute(out_half, "dp", turn)
        uv_near = lax.ppermute(uv_far, "expert", swap)
        out_near = lax.ppermute(out_far, "expert", swap)
        uv_groups += [uv_far, uv_near]
        out_groups += [out_far, out_near]
        starts += [
            source * heads_here + core * half_heads,
            source * heads_here + (1 - core) * half_heads,
        ]
        sizes += [half_heads, half_heads]

    latent_rows = jnp.transpose(latents[0], (1, 0, 2)).reshape(row_count, latent_dim)
    table = jnp.concatenate([ids_t, gates_t], axis=0).reshape(-1)
    table_rows = -(-table.shape[0] // (16 * latent_dim)) * 16
    table = jnp.pad(table, (0, table_rows * latent_dim - table.shape[0]))
    packed = jnp.concatenate([latent_rows, table.reshape(table_rows, latent_dim)], axis=0)
    all_rows = row_count + table_rows
    cut = (all_rows // 2 + 15) // 16 * 16
    gathered = ring_gather(packed, n, cut, 0)

    segment = gathered[:, :row_count].reshape(n, seq_count, local_len, latent_dim)
    segment = jnp.transpose(segment, (1, 0, 2, 3)).reshape(seq_count, n * local_len, latent_dim)
    memory = jnp.transpose(mem_latents[0], (1, 0, 2))
    mem_count = memory.shape[1]
    keys = jnp.concatenate([memory, segment], axis=1)
    query_rows = jnp.transpose(
        queries[0].reshape(local_len, seq_count, head_count, latent_dim), (1, 2, 0, 3)
    ).reshape(seq_count, head_count * local_len, latent_dim)
    scores = jnp.einsum("sql,sjl->sqj", query_rows, keys, preferred_element_type=f32) * score_scale
    key_pos = lax.broadcasted_iota(jnp.int32, scores.shape, 2) - mem_count
    own_pos = me * local_len + lax.broadcasted_iota(jnp.int32, scores.shape, 1) % local_len
    visible = (key_pos <= own_pos) & (key_pos < lengths[0][:, None, None])
    scores = jnp.where(visible | (key_pos < 0), scores, -jnp.inf)
    weights = jnp.exp(scores - jnp.max(scores, axis=2, keepdims=True))
    total = jnp.sum(weights, axis=2, keepdims=True)
    attended = jnp.einsum("sqj,sjl->sql", weights.astype(bf16), keys, preferred_element_type=f32)
    attended = (attended / total).astype(bf16)
    attended = attended.reshape(seq_count, head_count, local_len, latent_dim)

    attn_out = jnp.zeros((row_count, model_width), f32)
    for uv, out, start, size in zip(uv_groups, out_groups, starts, sizes):
        heads = lax.dynamic_slice_in_dim(attended, start, size, 1)
        values = jnp.einsum("shtl,hlv->sthv", heads, uv, preferred_element_type=f32).astype(bf16)
        attn_out = attn_out + jnp.dot(
            values.reshape(row_count, size * value_dim), out, preferred_element_type=f32
        )

    hidden_rows = jnp.transpose(hidden[0], (1, 0, 2)).reshape(row_count, model_width)
    residual = lax.optimization_barrier(hidden_rows).astype(f32) + attn_out
    mean_square = jnp.mean(residual * residual, axis=-1, keepdims=True)
    normed = (residual * lax.rsqrt(mean_square + norm_eps) * norm_gain.astype(f32)).astype(bf16)

    rows_all = ring_gather(normed, n, row_count // 2, 1)
    experts_here = w_gate.shape[0]
    expert_count = n * experts_here
    groups = n // 2
    wide = 2 * row_count
    slots = -(-2 * capacity // 16) * 16
    tables = gathered[:, row_count:].reshape(n, -1)[:, : 2 * top_count * row_count]
    tables = tables.reshape(groups, 2, 2, top_count, row_count)
    named = jnp.transpose(tables[:, :, 0], (2, 0, 1, 3)).reshape(top_count, groups, wide)
    scale = jnp.transpose(tables[:, :, 1], (2, 0, 1, 3)).reshape(top_count, groups, wide)
    rows_all = rows_all.reshape(groups, wide, model_width)
    steps = jnp.arange(wide, dtype=jnp.int32)
    earlier = (steps[:, None] < steps[None, :]).astype(bf16)
    made_rows, mixes = [], []
    for e in range(experts_here):
        matches = named == (me * experts_here + e).astype(bf16)
        hit = jnp.any(matches, axis=0)
        gate = jnp.sum(jnp.where(matches, scale.astype(f32), 0.0), axis=0)
        slot = jnp.dot(hit.astype(bf16), earlier, preferred_element_type=f32).astype(jnp.int32)
        slot = jnp.where(hit, slot, -1)
        chosen = slot[:, None, :] == jnp.arange(slots, dtype=jnp.int32)[None, :, None]
        placing = chosen.astype(bf16)
        slot_t = jnp.where(hit, slot, -1).reshape(n, row_count)
        chosen_t = slot_t[:, :, None] == jnp.arange(slots, dtype=jnp.int32)[None, None, :]
        mixes.append(jnp.where(chosen_t, gate.reshape(n, row_count)[:, :, None], 0.0).astype(bf16))
        picked = jnp.einsum("gct,gtd->gcd", placing, rows_all, preferred_element_type=f32)
        picked = picked.astype(bf16).reshape(groups * slots, model_width)
        gate_h = jnp.dot(picked, w_gate[e], preferred_element_type=f32)
        up_h = jnp.dot(picked, w_up[e], preferred_element_type=f32)
        act = (jax.nn.silu(gate_h) * up_h).astype(bf16)
        produced = jnp.dot(act, w_down[e], preferred_element_type=f32).astype(bf16)
        made_rows.append(produced.reshape(groups, slots, model_width))
    made_rows = made_rows[0] if experts_here == 1 else jnp.concatenate(made_rows, axis=1)
    mixing = mixes[0] if experts_here == 1 else jnp.concatenate(mixes, axis=2)
    routed = ring_reduce(made_rows, mixing, n, 2)
    layer_out = (residual + routed).astype(bf16).reshape(seq_count, local_len, model_width)
    return jnp.transpose(layer_out, (1, 0, 2))[None]


def solution(mesh):
    return jax.shard_map(
        shards,
        mesh=mesh,
        in_specs=(
            P("dp", "expert", None, None),
            P("dp", "expert", None, None),
            P("dp", "expert", None, None),
            P("dp", None, None, None),
            P("dp", None),
            P("dp", "expert", None, None),
            P("dp", "expert", None, None),
            P(),
            P("dp", None, None),
            P("dp", None),
            P("expert", None, None),
            P("expert", None, None),
            P("expert", None, None),
        ),
        out_specs=P("dp", "expert", None, None),
        check_vma=False,
    )
```

```python
import functools

import jax
import jax.numpy as jnp
from jax import lax
from jax.experimental import pallas as pl
from jax.experimental.pallas import tpu as pltpu
from jax.sharding import PartitionSpec as P

score_scale = 192.0 ** (-0.5)
norm_eps = 1e-06
MESH = pl.DeviceIdType.MESH


def ring_place(n):
    chips = n // 2
    depth = chips // 2
    me = lax.axis_index("expert")
    core = me % 2
    chip = me // 2
    row, col = chip // 2, chip % 2
    pos = col * row + (1 - col) * (chips - 1 - row)

    def device(offset, core_of):
        p = (pos + offset + chips) % chips
        q = p // depth
        r = (1 - q) * p + q * (chips - 1 - p)
        return (2 * r + 1 - q) * 2 + core_of

    return me, core, device


def greet(targets):
    barrier = pltpu.get_barrier_semaphore()
    for target in targets:
        pl.semaphore_signal(barrier, inc=1, device_id={"expert": target}, device_id_type=MESH)
    pl.semaphore_wait(barrier, len(targets))


def remote(src, dst, send_sem, recv_sem, target):
    return pltpu.make_async_remote_copy(
        src_ref=src,
        dst_ref=dst,
        send_sem=send_sem,
        recv_sem=recv_sem,
        device_id={"expert": target},
        device_id_type=MESH,
    )


def gather_kernel(n, cut, x_ref, out_ref, ring_send, ring_recv, pair_send, pair_recv, own_sem):
    chips = n // 2
    half_ring = chips // 2
    rows = x_ref.shape[0]
    last = chips - 2
    me, core, device = ring_place(n)
    partner = device(0, 1 - core)
    ahead = (device(1, core), device(-1, core))
    spans = (pl.ds(0, cut), pl.ds(cut, rows - cut))
    greet((ahead[0], ahead[1], partner))

    def arrival(way, j):
        dist, half = (half_ring, way) if j == last else (j // 2 + 1, j % 2)
        return device(-dist if way == 0 else dist, core), spans[half]

    waits = []
    for way in (0, 1):
        for j in (0, 1):
            if j > last:
                continue
            if j == last and half_ring == 1:
                span = spans[way]
            else:
                span = spans[j]
            copy = remote(
                x_ref.at[span], out_ref.at[me, span],
                ring_send.at[way, j], ring_recv.at[way, j], ahead[way],
            )
            copy.start()
            waits.append(copy)
    share = remote(x_ref, out_ref.at[me], pair_send.at[2 * last + 2], pair_recv.at[2 * last + 2], partner)
    share.start()
    waits.append(share)
    keep = pltpu.make_async_copy(x_ref, out_ref.at[me], own_sem)
    keep.start()

    for j in range(last + 1):
        for way in (0, 1):
            slot, span = arrival(way, j)
            piece = out_ref.at[slot, span]
            remote(piece, piece, ring_send.at[way, j], ring_recv.at[way, j], ahead[way]).wait_recv()
            onward = j + 2
            if j >= last - 2 and j < last:
                onward = last if j == last - 2 + way else None
            if j == last:
                onward = None
            if onward is not None:
                copy = remote(piece, piece, ring_send.at[way, onward], ring_recv.at[way, onward], ahead[way])
                copy.start()
                waits.append(copy)
            index = 2 * j + way
            copy = remote(piece, piece, pair_send.at[index], pair_recv.at[index], partner)
            copy.start()
            waits.append(copy)

    for j in range(last + 1):
        for way in (0, 1):
            dist, half = (half_ring, way) if j == last else (j // 2 + 1, j % 2)
            slot = device(-dist if way == 0 else dist, 1 - core)
            piece = out_ref.at[slot, spans[half]]
            index = 2 * j + way
            remote(piece, piece, pair_send.at[index], pair_recv.at[index], partner).wait_recv()
    other = out_ref.at[partner]
    remote(other, other, pair_send.at[2 * last + 2], pair_recv.at[2 * last + 2], partner).wait_recv()
    for copy in waits:
        copy.wait_send()
    keep.wait()


def ring_gather(x, n, cut, collective_id):
    rows, cols = x.shape
    steps = n // 2 - 1
    return pl.pallas_call(
        functools.partial(gather_kernel, n, cut),
        out_shape=jax.ShapeDtypeStruct((n, rows, cols), x.dtype),
        in_specs=[pl.BlockSpec(memory_space=pltpu.VMEM)],
        out_specs=pl.BlockSpec(memory_space=pl.ANY),
        scratch_shapes=[
            pltpu.SemaphoreType.DMA((2, steps)),
            pltpu.SemaphoreType.DMA((2, steps)),
            pltpu.SemaphoreType.DMA((2 * steps + 1,)),
            pltpu.SemaphoreType.DMA((2 * steps + 1,)),
            pltpu.SemaphoreType.DMA,
        ],
        compiler_params=pltpu.CompilerParams(collective_id=collective_id, has_side_effects=True),
        cost_estimate=pl.CostEstimate(flops=0, bytes_accessed=16 * n * rows * cols, transcendentals=0),
        name="ring_gather_%d" % collective_id,
    )(x)


def reduce_kernel(
    n, rows_ref, mix_ref, out_ref, mine, paired, give, arrived, ring_send, ring_recv, pair_send, pair_recv
):
    chips = n // 2
    half_ring = chips // 2
    half = mine.shape[1] // 2
    last = chips - 2
    me, core, device = ring_place(n)
    partner = device(0, 1 - core)
    ahead = (device(1, core), device(-1, core))
    greet((ahead[0], ahead[1], partner))

    order = [half_ring]
    for k in range(half_ring - 1, 0, -1):
        order += [k, chips - k]
    order.append(0)
    depth = give.shape[0]
    shares, made, seen = {}, [], set()

    def weigh(k, core_of):
        dest = device(k, core_of)
        return jnp.dot(
            mix_ref[dest], rows_ref[dest // 2], preferred_element_type=jnp.float32
        ).astype(mine.dtype)

    def make():
        k = order[len(made)]
        slot = len(made) % depth
        if len(made) >= depth:
            shares[order[len(made) - depth]].wait_send()
        give[slot] = weigh(k, 1 - core)
        shares[k] = remote(give.at[slot], paired.at[k], pair_send.at[k], pair_recv.at[k], partner)
        shares[k].start()
        mine[k] = weigh(k, core)
        made.append(k)

    def bring(k):
        while k not in made or (len(made) < chips and len(made) < order.index(k) + 3):
            make()
        if k not in seen:
            seen.add(k)
            shares[k].wait_recv()

    def index_of(dist, h):
        return 0 if dist == half_ring else 1 + 2 * (half_ring - 1 - dist) + h

    def await_ring(way, j):
        piece = arrived.at[way, j]
        remote(piece, piece, ring_send.at[way, j], ring_recv.at[way, j], ahead[way]).wait_recv()

    sends = []
    for dist in range(half_ring, 0, -1):
        for turn in (0, 1):
            for way in (0, 1):
                if dist == half_ring:
                    if turn == 1:
                        continue
                    h = way
                elif dist == half_ring - 1:
                    h = 1 - way if turn == 0 else way
                else:
                    h = turn
                k = dist if way == 0 else chips - dist
                bring(k)
                span = pl.ds(h * half, half)
                total = mine[k, span].astype(jnp.float32) + paired[k, span].astype(jnp.float32)
                has_prior = dist < half_ring - 1 or (dist == half_ring - 1 and h == way)
                if has_prior:
                    j = index_of(dist + 1, h)
                    await_ring(way, j)
                    total = total + arrived[way, j].astype(jnp.float32)
                mine[k, span] = total.astype(mine.dtype)
                j = index_of(dist, h)
                copy = remote(
                    mine.at[k, span], arrived.at[way, j],
                    ring_send.at[way, j], ring_recv.at[way, j], ahead[way],
                )
                copy.start()
                sends.append(copy)
    bring(0)
    for h in (0, 1):
        span = pl.ds(h * half, half)
        total = mine[0, span].astype(jnp.float32) + paired[0, span].astype(jnp.float32)
        for way in (0, 1):
            j = index_of(1, h)
            await_ring(way, j)
            total = total + arrived[way, j].astype(jnp.float32)
        out_ref[span] = total
    for copy in sends:
        copy.wait_send()
    for k in order[chips - min(depth, chips) :]:
        shares[k].wait_send()


def ring_reduce(rows_in, mix, n, collective_id):
    rows = mix.shape[1]
    cols = rows_in.shape[2]
    chips = n // 2
    dtype = rows_in.dtype
    return pl.pallas_call(
        functools.partial(reduce_kernel, n),
        out_shape=jax.ShapeDtypeStruct((rows, cols), jnp.float32),
        in_specs=[pl.BlockSpec(memory_space=pltpu.VMEM)] * 2,
        out_specs=pl.BlockSpec(memory_space=pltpu.VMEM),
        scratch_shapes=[
            pltpu.VMEM((chips, rows, cols), dtype),
            pltpu.VMEM((chips, rows, cols), dtype),
            pltpu.VMEM((min(4, chips), rows, cols), dtype),
            pltpu.VMEM((2, chips - 1, rows // 2, cols), dtype),
            pltpu.SemaphoreType.DMA((2, chips - 1)),
            pltpu.SemaphoreType.DMA((2, chips - 1)),
            pltpu.SemaphoreType.DMA((chips,)),
            pltpu.SemaphoreType.DMA((chips,)),
        ],
        compiler_params=pltpu.CompilerParams(
            collective_id=collective_id, has_side_effects=True, vmem_limit_bytes=62 * 1024 * 1024
        ),
        cost_estimate=pl.CostEstimate(
            flops=2 * mix.size * cols, bytes_accessed=16 * n * rows * cols, transcendentals=0
        ),
        name="ring_reduce_%d" % collective_id,
    )(rows_in, mix)


def layer_kernel(
    n,
    ids_hbm, gates_hbm, limit_hbm, gain_hbm,
    latent_hbm, query_hbm, memory_hbm, hidden_hbm, uv_hbm, wout_hbm, gate_hbm, up_hbm, down_hbm,
    out_ref,
    ids, gates, limit, gain,
    latent, query, memory, hidden, parted_hidden, keys, tables, heads, bound, peak, mass, blend,
    attended, values, w_uv, w_out, kept,
    place, mix, rows, w_gate, w_up, w_down, act, mine, paired, give, arrived,
    load_sem, far_send, far_recv, near_send, near_recv,
    key_send, key_recv, key_swap_send, key_swap_recv,
    row_send, row_recv, row_swap_send, row_swap_recv,
    round_send, round_recv, round_swap_send, round_swap_recv,
    ring_send, ring_recv, pair_send, pair_recv,
):
    f32, bf16 = jnp.float32, jnp.bfloat16
    chips = n // 2
    half_ring = chips // 2
    last = chips - 2
    count, width = kept.shape
    seqs, span_len = 2, count // 2
    lat_width = latent.shape[1]
    mem_len = memory.shape[0] // 2
    head_count = query.shape[1] // lat_width
    mem_at = n * span_len
    key_total = keys.shape[1]
    top_count = ids.shape[0]
    here = uv_hbm.shape[0]
    value_dim = uv_hbm.shape[2]
    half_here = here // 2
    slots = place.shape[1]
    me, core, device = ring_place(n)
    own_dp = lax.axis_index("dp")
    far_dp = 1 - own_dp
    partner = device(0, 1 - core)
    ahead = (device(1, core), device(-1, core))
    spans = (pl.ds(0, span_len), pl.ds(span_len, span_len))

    loads = [
        pltpu.make_async_copy(src, dst, load_sem.at[i])
        for i, (src, dst) in enumerate((
            (latent_hbm.reshape(count, lat_width), latent),
            (ids_hbm, ids),
            (gates_hbm, gates),
            (limit_hbm, limit),
            (gain_hbm, gain),
            (wout_hbm, w_out.at[pl.ds(own_dp * here * value_dim, here * value_dim)]),
            (uv_hbm, w_uv.at[pl.ds(own_dp * here, here)]),
            (query_hbm.reshape(query.shape), query),
            (memory_hbm.reshape(memory.shape), memory),
            (hidden_hbm.reshape(count, width), hidden),
            (gate_hbm, w_gate),
            (up_hbm, w_up),
            (down_hbm, w_down),
        ))
    ]
    for load in loads:
        load.start()
    waits = []

    def send(copy):
        copy.start()
        waits.append(copy)

    barrier = pltpu.get_barrier_semaphore()
    for target in (ahead[0], ahead[1], partner):
        pl.semaphore_signal(barrier, inc=1, device_id={"expert": target}, device_id_type=MESH)
    pl.semaphore_signal(barrier, inc=1, device_id={"dp": far_dp}, device_id_type=MESH)
    def uv_piece(owner, of_core):
        return pl.ds(owner * here + of_core * half_here, half_here)

    depth = here * value_dim
    round_rows = round_share(depth, n)
    pieces = far_send.shape[0] - 3
    out_rows = (depth - n * round_rows) // (2 * pieces)

    def out_piece(first, of_core, i):
        at = first + n * round_rows + (of_core * pieces + i) * out_rows
        return pl.ds(pl.multiple_of(at, 8), out_rows)

    def round_piece(first, slot, h):
        size = -(-round_rows // 16) * 8
        return pl.ds(pl.multiple_of(first + slot * round_rows + h * size, 8), size if h == 0 else round_rows - size)

    def across(src, dst, i):
        return pltpu.make_async_remote_copy(
            src_ref=src, dst_ref=dst, send_sem=far_send.at[i], recv_sem=far_recv.at[i],
            device_id={"dp": far_dp}, device_id_type=MESH,
        )

    def far_ref(i, of_core):
        return w_uv.at[uv_piece(far_dp, of_core)] if i == 0 else w_out.at[out_piece(far_dp * depth, of_core, i - 1)]

    def pass_far(i):
        piece = far_ref(i, core)
        across(piece, piece, i).wait_recv()
        send(remote(piece, piece, near_send.at[i], near_recv.at[i], partner))

    def await_near(i):
        piece = far_ref(i, 1 - core)
        remote(piece, piece, near_send.at[i], near_recv.at[i], partner).wait_recv()

    def step_of(way, j):
        return (half_ring, way) if j == last else (j // 2 + 1, j % 2)

    def offset(way, dist):
        return dist if way == 0 else chips - dist

    def gather(parts, sends, recvs, swap_sends, swap_recvs, base=0):
        own = 2 * last + 2

        def start(h):
            for way in (0, 1):
                for i, ref in enumerate(parts(me, h)):
                    send(remote(ref, ref, sends.at[base + i, way, h], recvs.at[base + i, way, h], ahead[way]))
            for i, ref in enumerate(parts(me, h)):
                send(remote(ref, ref, swap_sends.at[base + i, own + h], swap_recvs.at[base + i, own + h], partner))

        def near_own():
            for h in (0, 1):
                for i, ref in enumerate(parts(partner, h)):
                    remote(ref, ref, swap_sends.at[base + i, own + h], swap_recvs.at[base + i, own + h], partner).wait_recv()

        def hop(j):
            onward = [j + 2, j + 2]
            if last - 2 <= j < last:
                onward = [last if j == last - 2 + way else None for way in (0, 1)]
            if j == last:
                onward = [None, None]
            found = []
            for way in (0, 1):
                dist, h = step_of(way, j)
                found += [(i, way, ref) for i, ref in enumerate(parts(device(-dist if way == 0 else dist, core), h))]
            for i, way, ref in sorted(found, key=lambda piece: piece[:2]):
                remote(ref, ref, sends.at[base + i, way, j], recvs.at[base + i, way, j], ahead[way]).wait_recv()
                if onward[way] is not None:
                    k = onward[way]
                    send(remote(ref, ref, sends.at[base + i, way, k], recvs.at[base + i, way, k], ahead[way]))
                k = 2 * j + way
                send(remote(ref, ref, swap_sends.at[base + i, k], swap_recvs.at[base + i, k], partner))

        def near(j):
            for way in (0, 1):
                dist, h = step_of(way, j)
                k = 2 * j + way
                for i, ref in enumerate(parts(device(-dist if way == 0 else dist, 1 - core), h)):
                    remote(ref, ref, swap_sends.at[base + i, k], swap_recvs.at[base + i, k], partner).wait_recv()

        return start, near_own, hop, near

    def split_of(total):
        to = lax.broadcasted_iota(jnp.int32, (total, total), 0)
        at = lax.broadcasted_iota(jnp.int32, (total, total), 1)
        return (to == at % 2 * (total // 2) + at // 2).astype(f32).astype(bf16)

    split = split_of(count)
    to = lax.broadcasted_iota(jnp.int32, (count, count), 0)
    at = lax.broadcasted_iota(jnp.int32, (count, count), 1)
    weave = (at == to % 2 * span_len + to // 2).astype(f32).astype(bf16)

    def place_of(slot, first, size):
        return pl.ds(pl.multiple_of(slot * span_len + first, size), size)

    sub = span_len // 2

    def key_parts(s):
        def parts(slot, h):
            found = [keys.at[s, place_of(slot, h * sub, sub)]]
            return found + ([tables.at[slot]] if s == 0 and h == 0 else [])

        return gather(parts, key_send, key_recv, key_swap_send, key_swap_recv, 2 * s)

    streams = [key_parts(s) for s in range(seqs)]
    for load in loads[:5]:
        load.wait()
    lines = []
    for source, filler in ((ids, 255.0), (gates, 0.0)):
        taken = source[...].astype(f32)
        lines.append(jnp.concatenate([taken[:, s, :] for s in range(seqs)], axis=1))
        if top_count < 8:
            lines.append(jnp.full((8 - top_count, count), filler, f32))
    tables[me] = jnp.concatenate(lines, axis=0).astype(bf16)
    for s in range(seqs):
        keys[s, place_of(me, 0, span_len)] = jnp.dot(
            split[s * span_len : (s + 1) * span_len], latent[...], preferred_element_type=f32
        ).astype(bf16)
    pl.semaphore_wait(barrier, 4)
    loads[5].wait()
    for h in (0, 1):
        piece = w_out.at[round_piece(own_dp * depth, me, h)]
        send(across(piece, piece, pieces + 1 + h))
    loads[6].wait()
    piece = w_uv.at[uv_piece(own_dp, core)]
    send(across(piece, piece, 0))
    for i in range(pieces):
        piece = w_out.at[out_piece(own_dp * depth, core, i)]
        send(across(piece, piece, i + 1))
    for s in range(seqs):
        for h in (0, 1):
            streams[s][0](h)

    loads[7].wait()
    for s in range(seqs):
        parted = jnp.dot(
            split[s * span_len : (s + 1) * span_len], query[...], preferred_element_type=f32
        ).astype(bf16)
        for h in range(head_count):
            heads[s, pl.ds(h * span_len, span_len)] = parted[:, h * lat_width : (h + 1) * lat_width]
    loads[8].wait()
    parted = jnp.dot(split_of(2 * mem_len), memory[...], preferred_element_type=f32).astype(bf16)
    lanes = 2 * span_len
    row_count = head_count * span_len
    lane = lax.broadcasted_iota(jnp.int32, (row_count, lanes), 1)
    own_pos = me * span_len + lax.broadcasted_iota(jnp.int32, (row_count, lanes), 0) % span_len
    along = (((1,), (1,)), ((), ()))
    scale = score_scale * 1.4426950408889634
    for s in range(seqs):
        keys[s, pl.ds(mem_at, mem_len)] = parted[s * mem_len : (s + 1) * mem_len]
        keys[s, pl.ds(mem_at + mem_len, key_total - mem_at - mem_len)] = jnp.zeros(
            (key_total - mem_at - mem_len, lat_width), bf16
        )
        bound[s] = jnp.minimum(own_pos, limit[:, s : s + 1] - 1) - lane

    def wide(x, times):
        return x if times == 1 else jnp.concatenate([x] * times, axis=1)

    def attend(ks, chosen_seqs, opening=False):
        firsts = [pl.multiple_of(device(k, 0) * span_len, lanes) for k in ks]
        for s in chosen_seqs:
            held = [keys[s, pl.ds(first, lanes)] for first in firsts]
            seen_keys = [first <= bound[s] for first in firsts]
            if opening:
                held.append(keys[s, pl.ds(mem_at, lanes)])
                seen_keys.append(lane < mem_len)
            held = held[0] if len(held) == 1 else jnp.concatenate(held, axis=0)
            score = lax.dot_general(heads[s], held, along, preferred_element_type=f32)
            parts = [
                jnp.where(visible, score[:, i * lanes : (i + 1) * lanes], -jnp.inf)
                for i, visible in enumerate(seen_keys)
            ]
            top = functools.reduce(jnp.maximum, parts)
            top = jnp.broadcast_to(jnp.max(top, axis=1, keepdims=True), top.shape)
            if not opening:
                before = peak[s]
                top = jnp.maximum(before, top)
                fade = jnp.exp2((before - top) * scale)
            parts = [jnp.exp2((part - top) * scale) for part in parts]
            added = functools.reduce(jnp.add, parts)
            mass[s] = added if opening else mass[s] * fade + added
            peak[s] = top
            weight = parts[0] if len(parts) == 1 else jnp.concatenate(parts, axis=1)
            more = jnp.dot(weight.astype(bf16), held, preferred_element_type=f32)
            blend[s] = more if opening else blend[s] * wide(fade, lat_width // lanes) + more

    def round_parts(slot, h):
        return [w_out.at[round_piece(far_dp * depth, slot, h)]]

    round_start, round_near_own, round_hop, round_near = gather(
        round_parts, round_send, round_recv, round_swap_send, round_swap_recv
    )
    def steps_at(dist):
        return (last,) if dist == half_ring else (2 * dist - 2, 2 * dist - 1)

    def at_dist(dist):
        return [half_ring] if dist == half_ring else [dist, chips - dist]

    def hop_all(stream, dist):
        for j in steps_at(dist):
            stream[2](j)

    def use_keys(chosen_seqs, dist):
        for s in chosen_seqs:
            for j in steps_at(dist):
                streams[s][3](j)
        attend(at_dist(dist), chosen_seqs)

    rounds = (round_start, round_near_own, round_hop, round_near)
    for h in (0, 1):
        piece = w_out.at[round_piece(far_dp * depth, me, h)]
        across(piece, piece, pieces + 1 + h).wait_recv()
        round_start(h)
    for dist in range(1, half_ring):
        if dist > 1:
            hop_all(rounds, dist - 1)
        for s in range(seqs):
            hop_all(streams[s], dist)
        if dist == 1:
            for s in range(seqs):
                streams[s][1]()
            attend([0], range(seqs), True)
            loads[9].wait()
            parted_hidden[...] = jnp.dot(split, hidden[...], preferred_element_type=f32).astype(bf16)
        else:
            use_keys(range(seqs), dist - 1)
    pass_far(0)
    hop_all(rounds, half_ring - 1)
    use_keys(range(seqs), half_ring - 1)
    for s in range(seqs):
        hop_all(streams[s], half_ring)
    pass_far(1)
    hop_all(rounds, half_ring)
    use_keys([0], half_ring)
    for i in range(2, pieces + 1):
        pass_far(i)

    def row_parts(slot, h):
        return [rows.at[slot, pl.ds(h * span_len + i * sub, sub)] for i in (0, 1)]

    row_start, row_near_own, row_hop, row_near = gather(row_parts, row_send, row_recv, row_swap_send, row_swap_recv)
    await_near(0)
    near_cols = pl.ds(pl.multiple_of(own_dp * depth, depth), depth)
    far_cols = pl.ds(pl.multiple_of(far_dp * depth, depth), depth)
    for s in range(seqs):
        if s == 1:
            use_keys([1], half_ring)
        total = jnp.sum(mass[s], axis=1, keepdims=True)
        attended[...] = (blend[s] / total).astype(bf16)
        for h in range(head_count):
            values[spans[s], pl.ds(h * value_dim, value_dim)] = jnp.dot(
                attended[pl.ds(h * span_len, span_len)], w_uv[h], preferred_element_type=f32
            ).astype(bf16)
        residual = parted_hidden[spans[s]].astype(f32) + jnp.dot(
            values[spans[s], near_cols], w_out[near_cols], preferred_element_type=f32
        )
        if s == 0:
            round_near_own()
            for i in range(last + 1):
                round_near(i)
            for i in range(1, pieces + 1):
                await_near(i)
        residual = residual + jnp.dot(values[spans[s], far_cols], w_out[far_cols], preferred_element_type=f32)
        mean_square = jnp.mean(residual * residual, axis=1, keepdims=True)
        normed = residual * lax.rsqrt(mean_square + norm_eps) * gain[...].astype(f32)
        rows[me, spans[s]] = normed.astype(bf16)
        row_start(s)

    woven = jnp.dot(weave, values[...], preferred_element_type=f32).astype(bf16)
    kept[...] = (
        hidden[...].astype(f32)
        + jnp.dot(woven[:, :depth], w_out[pl.ds(0, depth)], preferred_element_type=f32)
        + jnp.dot(woven[:, depth:], w_out[pl.ds(depth, depth)], preferred_element_type=f32)
    )
    hits, scales = [], []
    own_id = me.astype(f32)
    for c in range(chips):
        pair = jnp.concatenate([tables[2 * c], tables[2 * c + 1]], axis=1).astype(f32)
        matches = pair[:8] == own_id
        hits.append(jnp.max(jnp.where(matches, 1.0, 0.0), axis=0, keepdims=True))
        scales.append(jnp.sum(jnp.where(matches, pair[8:], 0.0), axis=0, keepdims=True))
    hits = jnp.concatenate(hits, axis=0)
    to = lax.broadcasted_iota(jnp.int32, (2 * count, 2 * count), 0)
    at = lax.broadcasted_iota(jnp.int32, (2 * count, 2 * count), 1)
    earlier = (to < at).astype(f32).astype(bf16)
    ranks = jnp.dot(hits.astype(bf16), earlier, preferred_element_type=f32)
    ranks = jnp.where(hits > 0.5, ranks, -1.0)
    slot_id = lax.broadcasted_iota(jnp.int32, (slots, 2 * count), 0).astype(f32)
    for c in range(chips):
        chosen = slot_id == ranks[c : c + 1]
        place[c] = jnp.where(chosen, 1.0, 0.0).astype(bf16)
        weighed = jnp.where(chosen, scales[c], 0.0).astype(bf16)
        for i in (0, 1):
            own_part = weighed[:, i * count : (i + 1) * count]
            mix[2 * c + i] = jnp.dot(own_part, split, preferred_element_type=f32).astype(bf16)

    def start_experts(ks):
        picked = []
        for k in ks:
            first = device(k, 0)
            held = rows[pl.ds(first, 2)].reshape(2 * count, width)
            picked.append(jnp.dot(place[first // 2], held, preferred_element_type=f32).astype(bf16))
        picked = picked[0] if len(ks) == 1 else jnp.concatenate(picked, axis=0)
        gate_h = lax.dot_general(picked, w_gate[...], along, preferred_element_type=f32)
        up_h = lax.dot_general(picked, w_up[...], along, preferred_element_type=f32)
        act[pl.ds(0, len(ks) * slots)] = (gate_h / (1.0 + jnp.exp(-gate_h)) * up_h).astype(bf16)

    shares = {}
    down = (((0,), (0,)), ((), ()))

    def end_experts(ks):
        made = jnp.dot(act[pl.ds(0, len(ks) * slots)], w_down[...], preferred_element_type=f32).astype(bf16)
        for i, k in enumerate(ks):
            part = made[i * slots : (i + 1) * slots]
            give[k] = lax.dot_general(mix[device(k, 1 - core)], part, down, preferred_element_type=f32).astype(bf16)
            shares[k] = remote(give.at[k], paired.at[k], pair_send.at[k], pair_recv.at[k], partner)
            send(shares[k])
            mine[k] = lax.dot_general(mix[device(k, core)], part, down, preferred_element_type=f32).astype(bf16)

    seen = set()

    def bring(k):
        if k not in seen:
            seen.add(k)
            shares[k].wait_recv()

    def index_of(dist, h):
        return 0 if dist == half_ring else 1 + 2 * (half_ring - 1 - dist) + h

    def await_ring(way, j, u):
        piece = arrived.at[way, j, pl.ds(u * sub, sub)]
        remote(piece, piece, ring_send.at[u, way, j], ring_recv.at[u, way, j], ahead[way]).wait_recv()

    def advance(dist, chain):
        for u in (0, 1):
            for way in (0, 1):
                h = way if chain == 0 else 1 - way
                k = offset(way, dist)
                bring(k)
                part, within = pl.ds(h * span_len + u * sub, sub), pl.ds(u * sub, sub)
                total = mine[k, part].astype(f32) + paired[k, part].astype(f32)
                if dist < half_ring - chain:
                    j = index_of(dist + 1, h)
                    await_ring(way, j, u)
                    total = total + arrived[way, j, within].astype(f32)
                mine[k, part] = total.astype(bf16)
                j = index_of(dist, h)
                send(remote(
                    mine.at[k, part], arrived.at[way, j, within],
                    ring_send.at[u, way, j], ring_recv.at[u, way, j], ahead[way],
                ))

    row_near_own()
    for load in loads[10:]:
        load.wait()
    start_experts([0])
    end_experts([0])

    tasks = []
    for j in range(last + 1):
        if j < last:
            row_hop(j)
        if j % 2 == 1 or j == last:
            for i in (j - 1, j) if j % 2 == 1 else (j,):
                row_near(i)
            dist = step_of(0, j)[0]
            ks = [half_ring] if j == last else [dist, chips - dist]
            tasks += [functools.partial(start_experts, ks), functools.partial(end_experts, ks)]
        for _ in range(min(len(tasks), 1 if j < last - 1 else len(tasks))):
            tasks.pop(0)()
        if j == last - 1:
            row_hop(last)
            advance(half_ring - 1, 1)

    advance(half_ring, 0)
    for dist in range(half_ring - 2, 0, -1):
        advance(dist, 1)
        advance(dist + 1, 0)
    advance(1, 0)

    bring(0)
    for u, h in ((0, 0), (0, 1), (1, 0), (1, 1)):
        part, within = pl.ds(h * span_len + u * sub, sub), pl.ds(u * sub, sub)
        total = kept[part] + mine[0, part].astype(f32) + paired[0, part].astype(f32)
        for way in (0, 1):
            j = index_of(1, h)
            await_ring(way, j, u)
            total = total + arrived[way, j, within].astype(f32)
        out_ref[part] = total.astype(bf16)
    for copy in waits:
        copy.wait_send()


def fused_layer(
    ids, gates, lengths, gain, latents, queries, memory, hidden, w_uv, w_out, w_gate_t, w_up_t, w_down, n, slots, collective_id
):
    span_len, seqs, width = hidden.shape
    count = span_len * seqs
    lat_width = latents.shape[2]
    head_count = queries.shape[2] // lat_width
    here, _, value_dim = w_uv.shape
    mem_len = memory.shape[0]
    chips = n // 2
    steps = chips - 1
    inner = w_down.shape[0]
    key_total = n * span_len + count
    bf16, f32 = jnp.bfloat16, jnp.float32
    dma, vmem = pltpu.SemaphoreType.DMA, pltpu.VMEM
    row_count = head_count * span_len
    pieces = 2
    return pl.pallas_call(
        functools.partial(layer_kernel, n),
        out_shape=pltpu.VMEM((count, width), bf16),
        in_specs=[pl.BlockSpec(memory_space=pl.ANY)] * 13,
        out_specs=pl.BlockSpec(memory_space=pltpu.VMEM),
        scratch_shapes=[
            vmem(ids.shape, jnp.int32),
            vmem(gates.shape, bf16),
            vmem(lengths.shape, jnp.int32),
            vmem(gain.shape, bf16),
            vmem((count, lat_width), bf16),
            vmem((count, head_count * lat_width), bf16),
            vmem((seqs * mem_len, lat_width), bf16),
            vmem((count, width), bf16),
            vmem((count, width), bf16),
            vmem((seqs, key_total, lat_width), bf16),
            vmem((n, 16, count), bf16),
            vmem((seqs, row_count, lat_width), bf16),
            vmem((seqs, row_count, count), jnp.int32),
            vmem((seqs, row_count, count), f32),
            vmem((seqs, row_count, count), f32),
            vmem((seqs, row_count, lat_width), f32),
            vmem((row_count, lat_width), bf16),
            vmem((count, head_count * value_dim), bf16),
            vmem((head_count, lat_width, value_dim), bf16),
            vmem((head_count * value_dim, width), bf16),
            vmem((count, width), f32),
            vmem((chips, slots, 2 * count), bf16),
            vmem((n, slots, count), bf16),
            vmem((n, count, width), bf16),
            vmem((inner, width), bf16),
            vmem((inner, width), bf16),
            vmem((inner, width), bf16),
            vmem((2 * slots, inner), bf16),
            vmem((chips, count, width), bf16),
            vmem((chips, count, width), bf16),
            vmem((chips, count, width), bf16),
            vmem((2, steps, count // 2, width), bf16),
            dma((13,)),
            dma((pieces + 3,)),
            dma((pieces + 3,)),
            dma((pieces + 1,)),
            dma((pieces + 1,)),
            dma((3, 2, steps)),
            dma((3, 2, steps)),
            dma((3, 2 * steps + 2)),
            dma((3, 2 * steps + 2)),
            dma((2, 2, steps)),
            dma((2, 2, steps)),
            dma((2, 2 * steps + 2)),
            dma((2, 2 * steps + 2)),
            dma((1, 2, steps)),
            dma((1, 2, steps)),
            dma((1, 2 * steps + 2)),
            dma((1, 2 * steps + 2)),
            dma((2, 2, steps)),
            dma((2, 2, steps)),
            dma((chips,)),
            dma((chips,)),
        ],
        compiler_params=pltpu.CompilerParams(
            collective_id=collective_id, has_side_effects=True, vmem_limit_bytes=61000000
        ),
        cost_estimate=pl.CostEstimate(
            flops=6 * chips * slots * width * inner, bytes_accessed=32 * n * count * width, transcendentals=0
        ),
        name="layer_%d" % collective_id,
    )(ids, gates, lengths, gain, latents, queries, memory, hidden, w_uv, w_out, w_gate_t, w_up_t, w_down)


def round_share(depth, n):
    return depth // (2 * n) // 16 * 16


def layer_bytes(n, count, width, inner, slots, lat_width, head_count, value_dim):
    chips = n // 2
    key_total = (n + 2) * count // 2
    row_count = head_count * count // 2
    front = count * (1 + head_count) * lat_width + 2 * key_total * lat_width + 3 * row_count * lat_width
    front += 4 * row_count * lat_width + 12 * row_count * count + head_count * value_dim * (lat_width + width + count)
    back = n * count * width + 3 * width * inner + (4 * chips - 1) * count * width + 5 * count * width
    back += 4 * chips * slots * count + 2 * slots * inner
    return 2 * (front + back) + 8 * slots * inner * 2


def shards(
    hidden,
    queries,
    latents,
    mem_latents,
    lengths,
    ids,
    gates,
    norm_gain,
    w_uv,
    w_out,
    w_gate,
    w_up,
    w_down,
):
    f32, bf16 = jnp.float32, jnp.bfloat16
    local_len, seq_count, model_width = hidden.shape[1:]
    latent_dim = latents.shape[3]
    head_count = queries.shape[3] // latent_dim
    row_count = local_len * seq_count
    n = lax.axis_size("expert")
    dp_size = lax.axis_size("dp")
    me = lax.axis_index("expert")
    core = me % 2
    own_dp = lax.axis_index("dp")
    heads_here, _, value_dim = w_uv.shape
    top_count = ids.shape[3]
    ids_t = jnp.transpose(ids[0], (2, 1, 0)).reshape(top_count, row_count).astype(bf16)
    gates_t = jnp.transpose(gates[0], (2, 1, 0)).reshape(top_count, row_count)
    capacity = min(row_count, row_count * top_count // (n * w_gate.shape[0]) + 2)
    slots = -(-2 * capacity // 128) * 128
    fits = (
        dp_size == 2
        and w_gate.shape[0] == 1
        and n >= 8
        and top_count <= 8
        and seq_count == 2
        and row_count % 128 == 0
        and heads_here % 2 == 0
        and heads_here * value_dim % (64 * n // 4) == 0
        and round_share(heads_here * value_dim, n) >= 16
        and mem_latents.shape[1] <= row_count
        and layer_bytes(n, row_count, model_width, w_down.shape[1], slots, latent_dim, head_count, value_dim)
        < 60 * 1024 * 1024
    )
    if fits:
        out = fused_layer(
            jnp.transpose(ids[0], (2, 1, 0)), jnp.transpose(gates[0], (2, 1, 0)), lengths, norm_gain,
            latents[0], queries[0], mem_latents[0], hidden[0], w_uv, w_out,
            jnp.transpose(w_gate[0]), jnp.transpose(w_up[0]), w_down[0], n, slots, 4,
        )
        return out.reshape(1, local_len, seq_count, model_width)

    half_heads = heads_here // 2
    uv_half = lax.dynamic_slice_in_dim(w_uv, core * half_heads, half_heads, 0)
    out_half = lax.dynamic_slice_in_dim(
        w_out, core * half_heads * value_dim, half_heads * value_dim, 0
    )
    uv_groups, out_groups, starts = [w_uv], [w_out], [own_dp * heads_here]
    swap = [(i, i ^ 1) for i in range(n)]
    sizes = [heads_here]
    for shift in range(1, dp_size):
        turn = [(i, (i + shift) % dp_size) for i in range(dp_size)]
        source = (own_dp - shift + dp_size) % dp_size
        uv_far = lax.ppermute(uv_half, "dp", turn)
        out_far = lax.ppermute(out_half, "dp", turn)
        uv_near = lax.ppermute(uv_far, "expert", swap)
        out_near = lax.ppermute(out_far, "expert", swap)
        uv_groups += [uv_far, uv_near]
        out_groups += [out_far, out_near]
        starts += [
            source * heads_here + core * half_heads,
            source * heads_here + (1 - core) * half_heads,
        ]
        sizes += [half_heads, half_heads]

    latent_rows = jnp.transpose(latents[0], (1, 0, 2)).reshape(row_count, latent_dim)
    table = jnp.concatenate([ids_t, gates_t], axis=0).reshape(-1)
    table_rows = -(-table.shape[0] // (16 * latent_dim)) * 16
    table = jnp.pad(table, (0, table_rows * latent_dim - table.shape[0]))
    packed = jnp.concatenate([latent_rows, table.reshape(table_rows, latent_dim)], axis=0)
    all_rows = row_count + table_rows
    cut = (all_rows // 2 + 15) // 16 * 16
    gathered = ring_gather(packed, n, cut, 0)

    segment = gathered[:, :row_count].reshape(n, seq_count, local_len, latent_dim)
    segment = jnp.transpose(segment, (1, 0, 2, 3)).reshape(seq_count, n * local_len, latent_dim)
    memory = jnp.transpose(mem_latents[0], (1, 0, 2))
    mem_count = memory.shape[1]
    keys = jnp.concatenate([memory, segment], axis=1)
    query_rows = jnp.transpose(
        queries[0].reshape(local_len, seq_count, head_count, latent_dim), (1, 2, 0, 3)
    ).reshape(seq_count, head_count * local_len, latent_dim)
    scores = jnp.einsum("sql,sjl->sqj", query_rows, keys, preferred_element_type=f32) * score_scale
    key_pos = lax.broadcasted_iota(jnp.int32, scores.shape, 2) - mem_count
    own_pos = me * local_len + lax.broadcasted_iota(jnp.int32, scores.shape, 1) % local_len
    visible = (key_pos <= own_pos) & (key_pos < lengths[0][:, None, None])
    scores = jnp.where(visible | (key_pos < 0), scores, -jnp.inf)
    weights = jnp.exp(scores - jnp.max(scores, axis=2, keepdims=True))
    total = jnp.sum(weights, axis=2, keepdims=True)
    attended = jnp.einsum("sqj,sjl->sql", weights.astype(bf16), keys, preferred_element_type=f32)
    attended = (attended / total).astype(bf16)
    attended = attended.reshape(seq_count, head_count, local_len, latent_dim)

    attn_out = jnp.zeros((row_count, model_width), f32)
    for uv, out, start, size in zip(uv_groups, out_groups, starts, sizes):
        heads = lax.dynamic_slice_in_dim(attended, start, size, 1)
        values = jnp.einsum("shtl,hlv->sthv", heads, uv, preferred_element_type=f32).astype(bf16)
        attn_out = attn_out + jnp.dot(
            values.reshape(row_count, size * value_dim), out, preferred_element_type=f32
        )

    hidden_rows = jnp.transpose(hidden[0], (1, 0, 2)).reshape(row_count, model_width)
    residual = lax.optimization_barrier(hidden_rows).astype(f32) + attn_out
    mean_square = jnp.mean(residual * residual, axis=-1, keepdims=True)
    normed = (residual * lax.rsqrt(mean_square + norm_eps) * norm_gain.astype(f32)).astype(bf16)

    rows_all = ring_gather(normed, n, row_count // 2, 1)
    experts_here = w_gate.shape[0]
    expert_count = n * experts_here
    groups = n // 2
    wide = 2 * row_count
    slots = -(-2 * capacity // 16) * 16
    tables = gathered[:, row_count:].reshape(n, -1)[:, : 2 * top_count * row_count]
    tables = tables.reshape(groups, 2, 2, top_count, row_count)
    named = jnp.transpose(tables[:, :, 0], (2, 0, 1, 3)).reshape(top_count, groups, wide)
    scale = jnp.transpose(tables[:, :, 1], (2, 0, 1, 3)).reshape(top_count, groups, wide)
    rows_all = rows_all.reshape(groups, wide, model_width)
    steps = jnp.arange(wide, dtype=jnp.int32)
    earlier = (steps[:, None] < steps[None, :]).astype(bf16)
    made_rows, mixes = [], []
    for e in range(experts_here):
        matches = named == (me * experts_here + e).astype(bf16)
        hit = jnp.any(matches, axis=0)
        gate = jnp.sum(jnp.where(matches, scale.astype(f32), 0.0), axis=0)
        slot = jnp.dot(hit.astype(bf16), earlier, preferred_element_type=f32).astype(jnp.int32)
        slot = jnp.where(hit, slot, -1)
        chosen = slot[:, None, :] == jnp.arange(slots, dtype=jnp.int32)[None, :, None]
        placing = chosen.astype(bf16)
        slot_t = jnp.where(hit, slot, -1).reshape(n, row_count)
        chosen_t = slot_t[:, :, None] == jnp.arange(slots, dtype=jnp.int32)[None, None, :]
        mixes.append(jnp.where(chosen_t, gate.reshape(n, row_count)[:, :, None], 0.0).astype(bf16))
        picked = jnp.einsum("gct,gtd->gcd", placing, rows_all, preferred_element_type=f32)
        picked = picked.astype(bf16).reshape(groups * slots, model_width)
        gate_h = jnp.dot(picked, w_gate[e], preferred_element_type=f32)
        up_h = jnp.dot(picked, w_up[e], preferred_element_type=f32)
        act = (jax.nn.silu(gate_h) * up_h).astype(bf16)
        produced = jnp.dot(act, w_down[e], preferred_element_type=f32).astype(bf16)
        made_rows.append(produced.reshape(groups, slots, model_width))
    made_rows = made_rows[0] if experts_here == 1 else jnp.concatenate(made_rows, axis=1)
    mixing = mixes[0] if experts_here == 1 else jnp.concatenate(mixes, axis=2)
    routed = ring_reduce(made_rows, mixing, n, 2)
    layer_out = (residual + routed).astype(bf16).reshape(seq_count, local_len, model_width)
    return jnp.transpose(layer_out, (1, 0, 2))[None]


def solution(mesh):
    return jax.shard_map(
        shards,
        mesh=mesh,
        in_specs=(
            P("dp", "expert", None, None),
            P("dp", "expert", None, None),
            P("dp", "expert", None, None),
            P("dp", None, None, None),
            P("dp", None),
            P("dp", "expert", None, None),
            P("dp", "expert", None, None),
            P(),
            P("dp", None, None),
            P("dp", None),
            P("expert", None, None),
            P("expert", None, None),
            P("expert", None, None),
        ),
        out_specs=P("dp", "expert", None, None),
        check_vma=False,
    )
```
